32 devices in a mesh: gx: 2 (over x), gy: 4 (over z), gz: 4 (over y, core).
Axes of the slice: x: 2, y: 2, z: 4, core: 2. Of those that a mesh axis runs over, the one named last changes fastest.
Arguments:
- conductivity: float32 [16, 32, 1024], P('gx', 'gy', 'gz'), may hold values from 0.1 to 10
- source: float32 [16, 32, 1024], P('gx', 'gy', 'gz'), may hold values from -5 to 5
Outputs:
- solution: float32 [16, 32, 1024], P('gx', 'gy', 'gz')
- residual: float32 [16, 32, 1024], P('gx', 'gy', 'gz')
The draws below stay inside these ranges and needn't reach their ends.
All inputs are finite; a program needn't handle non-finite values.
Results may differ from the reference program's by a relative error of at most 0.0003.
Values sent between devices are 32-bit elements; how exact they have to be, the bound alone decides.
No kernel may reach another device: no remote copies, remote signals or barrier semaphores. Data moves between devices by JAX's collectives and lax.ppermute only.
A program may use at most 64 MiB of HBM per device.

```python
import math
import jax
import jax.numpy as jnp

LEVELS = 3
DEGREE = 4
COARSE_DEGREE = 8
NX = 16
NY = 32
NZ = 1024


def draw_source(key, part):
    rough = jnp.clip(jax.random.normal(key, (NX, NY, NZ), jnp.float32), -5.0, 5.0)
    return rough


def levels(stream_key, dims, cuts, smallest, largest):
    def one(position, parts):
        steps = jax.random.uniform(jax.random.fold_in(jax.random.fold_in(stream_key, 6), position), (parts,), jnp.float32, smallest / len(cuts), largest / len(cuts))
        return jnp.repeat(jnp.exp(steps), dims[position] // parts).reshape((-1,) + (1,) * (len(dims) - position - 1))

    factor_of = one(*cuts[0])
    for cut in cuts[1:]:
        factor_of = factor_of * one(*cut)
    return factor_of


def setup_inputs(seed: int = 0) -> dict:
    seeds = jax.random.split(jax.random.key(seed), 3)
    return {
        "conductivity": jnp.clip(jnp.exp(math.log(10.0) - 4.6051702 * jax.random.uniform(seeds[0], (NX, NY, NZ), jnp.float32) ** levels(seeds[0], (NX, NY, NZ), ((0, 2), (1, 4), (2, 4)), -0.2, 0.2)), 0.1, 10.0),
        "source": draw_source(jax.random.fold_in(seeds[2], 71), 0),
    }


weight_table = {1: 14.0 / 30.0, 2: 3.0 / 30.0, 3: 1.0 / 30.0}
neighbour_offsets = [(along_one, along_two, along_three) for along_one in (-1, 0, 1) for along_two in (-1, 0, 1) for along_three in (-1, 0, 1) if (along_one, along_two, along_three) != (0, 0, 0)]
smooth_low = 0.5
coarse_low = 0.03
upper_bound = 2.0


def shifted(padded, offset):
    return padded[1 + offset[0]:padded.shape[0] - 1 + offset[0], 1 + offset[1]:padded.shape[1] - 1 + offset[1], 1 + offset[2]:padded.shape[2] - 1 + offset[2]]


def stencil(field_pad, coeff_pad, spacing):
    centre_field = shifted(field_pad, (0, 0, 0))
    centre_coeff = shifted(coeff_pad, (0, 0, 0))
    total = jnp.zeros(centre_field.shape, jnp.float32)
    for offset in neighbour_offsets:
        weight = weight_table[abs(offset[0]) + abs(offset[1]) + abs(offset[2])]
        total = total + weight * (centre_coeff + shifted(coeff_pad, offset)) * (centre_field - shifted(field_pad, offset))
    return total * (0.5 / spacing)


def diagonal_of(coeff_pad, spacing):
    centre_coeff = shifted(coeff_pad, (0, 0, 0))
    total = jnp.zeros(centre_coeff.shape, jnp.float32)
    for offset in neighbour_offsets:
        weight = weight_table[abs(offset[0]) + abs(offset[1]) + abs(offset[2])]
        total = total + weight * (centre_coeff + shifted(coeff_pad, offset))
    return total * (0.5 / spacing)


def coarsen(values):
    extent = values.shape
    return values.reshape(extent[0] // 2, 2, extent[1] // 2, 2, extent[2] // 2, 2).mean(axis=(1, 3, 5))


def refine(values):
    return jnp.repeat(jnp.repeat(jnp.repeat(values, 2, axis=0), 2, axis=1), 2, axis=2)


def chebyshev_coefs(degree, lower):
    centre = (upper_bound + lower) / 2.0
    half_width = (upper_bound - lower) / 2.0
    ratio_term = centre / half_width
    rho_prev = 1.0 / ratio_term
    weights = []
    for number in range(1, degree):
        rho_next = 1.0 / (2.0 * ratio_term - rho_prev)
        weights.append((rho_next * rho_prev, 2.0 * rho_next / half_width))
        rho_prev = rho_next
    return centre, weights


def smooth(operate, diagonal, right_side, start, degree, lower, final):
    centre, weights = chebyshev_coefs(degree, lower)
    if start is None:
        residual = right_side
    else:
        residual = right_side - operate(start)
    update = residual / (centre * diagonal)
    solution = update if start is None else start + update
    for pair in weights:
        residual = residual - operate(update)
        update = pair[0] * update + pair[1] * residual / diagonal
        solution = solution + update
    if final:
        residual = residual - operate(update)
    return solution, residual


def reference(conductivity, source):
    coeffs = [conductivity]
    for number in range(1, LEVELS):
        coeffs.append(coarsen(coeffs[-1]))

    def cycle(grid_level, right_side):
        spacing = float(4 ** grid_level)
        coeff_pad = jnp.pad(coeffs[grid_level], 1)
        diagonal = diagonal_of(coeff_pad, spacing)

        def operate(field):
            return stencil(jnp.pad(field, 1), coeff_pad, spacing)

        if grid_level == LEVELS - 1:
            return smooth(operate, diagonal, right_side, None, COARSE_DEGREE, coarse_low, False)
        solution, residual = smooth(operate, diagonal, right_side, None, DEGREE, smooth_low, True)
        correction, ignored = cycle(grid_level + 1, coarsen(residual))
        solution = solution + refine(correction)
        return smooth(operate, diagonal, right_side, solution, DEGREE, smooth_low, grid_level == 0)

    return cycle(0, source)
```

```python
import jax
import jax.numpy as jnp
from jax import lax
from jax.experimental import pallas as pl
from jax.experimental.pallas import tpu as pltpu
from jax.sharding import PartitionSpec as P

DEGREE = 4
COARSE_DEGREE = 8
smooth_low = 0.5
coarse_low = 0.03
upper_bound = 2.0

F32 = jnp.float32
LANES = 128
PAD = 8
HALO = 5
COARSE_PAD = 4
FACE = 14.0 / 3.0
CORNER = 1.0 / 3.0
TOTAL = 128.0 / 3.0
SCALE = 0.05


def chebyshev_coefs(degree, lower):
    centre = (upper_bound + lower) / 2.0
    half_width = (upper_bound - lower) / 2.0
    ratio_term = centre / half_width
    rho_prev = 1.0 / ratio_term
    weights = []
    for number in range(1, degree):
        rho_next = 1.0 / (2.0 * ratio_term - rho_prev)
        weights.append((rho_next * rho_prev, 2.0 * rho_next / half_width))
        rho_prev = rho_next
    return centre, weights


def loop(start, stop, body, unroll=1):
    def step(i, carry):
        body(i)
        return carry

    lax.fori_loop(start, stop, step, 0, unroll=unroll)


def third_pairs(values):
    tiles, rows, _ = values.shape
    flat = values.reshape(tiles * rows, LANES)
    up = pltpu.roll(flat, 1, 1).reshape(tiles, rows, LANES)
    down = pltpu.roll(flat, LANES - 1, 1).reshape(tiles, rows, LANES)
    if tiles > 1:
        lane = lax.broadcasted_iota(jnp.int32, (tiles, rows, LANES), 2)
        up_other = jnp.concatenate([up[tiles - 1 :], up[: tiles - 1]], axis=0)
        down_other = jnp.concatenate([down[1:], down[:1]], axis=0)
        up = jnp.where(lane == 0, up_other, up)
        down = jnp.where(lane == LANES - 1, down_other, down)
    return up + down


def neighbour_sum(ref, y, row):
    centre = ref[y, :, row : row + 8, :]
    before = ref[y - 1, :, row : row + 8, :]
    after = ref[y + 1, :, row : row + 8, :]
    side = ref[y, :, row - 1 : row + 7, :] + ref[y, :, row + 1 : row + 9, :]
    corner = (ref[y - 1, :, row - 1 : row + 7, :] + ref[y - 1, :, row + 1 : row + 9, :]) + (
        ref[y + 1, :, row - 1 : row + 7, :] + ref[y + 1, :, row + 1 : row + 9, :]
    )
    face = (before + after) + side
    plane = FACE * face + corner
    beside = FACE * centre + face + CORNER * corner
    return plane + third_pairs(beside), centre


def zero_pads(refs):
    for ref in refs:
        count, tiles, rows, _ = ref.shape
        zero = jnp.zeros((tiles, PAD, LANES), F32)

        def body(y, ref=ref, rows=rows, zero=zero):
            ref[y, :, 0:PAD, :] = zero
            ref[y, :, rows - PAD : rows, :] = zero

        loop(0, count, body, 2)


def zero_rows(ref, rows):
    zero = jnp.zeros(ref.shape[1:], F32)
    for y in rows:
        ref[y] = zero


def tiles_of(ref):
    return range(0, ref.shape[2], 8)


def make_diagonal(kap, diag, inv, lo, hi, unroll=1):
    def body(y):
        for x in tiles_of(diag):
            total, centre = neighbour_sum(kap, y, PAD + x)
            value = TOTAL * centre + total
            diag[y, :, x : x + 8, :] = value
            inv[y, :, x : x + 8, :] = jnp.where(centre > 0.0, 1.0 / value, 0.0)

    loop(lo, hi, body, unroll)


def first_update(kap, inv, res, v, w, acc, lo, hi, scale, add, unroll=1):
    def body(y):
        for x in tiles_of(inv):
            step = (inv[y, :, x : x + 8, :] * scale) * res[y, :, x : x + 8, :]
            v[y, :, PAD + x : PAD + x + 8, :] = step
            w[y, :, PAD + x : PAD + x + 8, :] = kap[y, :, PAD + x : PAD + x + 8, :] * step
            acc[y, :, x : x + 8, :] = acc[y, :, x : x + 8, :] + step if add else step

    loop(lo, hi, body, unroll)


def times(kap, v, w, lo, hi, unroll=1):
    def body(y):
        w[y] = kap[y] * v[y]

    loop(lo, hi, body, unroll)


def new_residual(kap, diag, res, v, w, y, x):
    total, centre = neighbour_sum(v, y, PAD + x)
    weighted, _ = neighbour_sum(w, y, PAD + x)
    return (
        res[y, :, x : x + 8, :]
        - diag[y, :, x : x + 8, :] * centre
        + (kap[y, :, PAD + x : PAD + x + 8, :] * total + weighted)
    ), centre


def residual_only(kap, diag, res, v, w, lo, hi, unroll=1):
    def body(y):
        for x in tiles_of(diag):
            value, _ = new_residual(kap, diag, res, v, w, y, x)
            res[y, :, x : x + 8, :] = value

    loop(lo, hi, body, unroll)


def smoothing_step(kap, diag, inv, res, old, new, acc, lo, hi, pair, unroll=1):
    def body(y):
        for x in tiles_of(diag):
            value, centre = new_residual(kap, diag, res, old[0], old[1], y, x)
            res[y, :, x : x + 8, :] = value
            step = pair[0] * centre + (pair[1] * inv[y, :, x : x + 8, :]) * value
            new[0][y, :, PAD + x : PAD + x + 8, :] = step
            new[1][y, :, PAD + x : PAD + x + 8, :] = (
                kap[y, :, PAD + x : PAD + x + 8, :] * step
            )
            acc[y, :, x : x + 8, :] = acc[y, :, x : x + 8, :] + step

    loop(lo, hi, body, unroll)


def halving(rows):
    row = lax.broadcasted_iota(jnp.int32, (rows, rows // 2), 0)
    col = lax.broadcasted_iota(jnp.int32, (rows, rows // 2), 1)
    return jnp.where(row // 2 == col, 0.125, 0.0).astype(F32)


def doubling(cols):
    row = lax.broadcasted_iota(jnp.int32, (cols // 2, cols), 0)
    col = lax.broadcasted_iota(jnp.int32, (cols // 2, cols), 1)
    return jnp.where(col // 2 == row, 1.0, 0.0).astype(F32)


def halo_doubling():
    row = lax.broadcasted_iota(jnp.int32, (LANES, LANES), 0)
    col = lax.broadcasted_iota(jnp.int32, (LANES, LANES), 1)
    source = col // 2 + jnp.where(col < LANES // 2, 0, LANES // 2)
    return jnp.where(source == row, 1.0, 0.0).astype(F32)


def product(left, right):
    return jnp.dot(left, right, precision=lax.Precision.HIGHEST, preferred_element_type=F32)


def along_lanes(values):
    return jnp.concatenate([values[t] for t in range(values.shape[0])], axis=-1)


def before_kernel(flags, own, ylo, yhi, kap, diag, inv, xout, rout, coarse, va, wa, vb, wb, res, acc, flat):
    rows = own.shape[1]
    x_count = own.shape[3]
    inner = slice(PAD, PAD + x_count)
    last = HALO + rows
    has_lo = flags[2] > 0
    has_hi = flags[3] > 0
    zero_pads((kap, va, wa, vb, wb))

    def fill(y):
        kap[HALO + y, :, inner, :] = SCALE * own[0, y]
        res[HALO + y] = own[1, y]

    loop(0, rows, fill)
    for j in range(HALO):
        kap[j, :, inner, :] = jnp.where(has_lo, SCALE * ylo[j], 0.0)
        kap[last + j, :, inner, :] = jnp.where(has_hi, SCALE * yhi[j], 0.0)
    for j in range(HALO - 1):
        res[1 + j] = ylo[HALO + j]
        res[last + j] = yhi[HALO + j]
    make_diagonal(kap, diag, inv, 1, last + HALO - 1)
    centre, weights = chebyshev_coefs(DEGREE, smooth_low)
    first_update(kap, inv, res, va, wa, acc, 1, last + HALO - 1, 1.0 / centre, False)
    old, new = (va, wa), (vb, wb)
    lo, hi = 2, last + HALO - 2
    for pair in weights:
        smoothing_step(kap, diag, inv, res, old, new, acc, lo, hi, pair)
        old, new = new, old
        lo, hi = lo + 1, hi - 1
    residual_only(kap, diag, res, old[0], old[1], HALO, last)
    tiles = rout.shape[1]

    def emit(y):
        xout[y] = acc[HALO + y, 0:tiles]
        rout[y] = res[HALO + y, 0:tiles]

    loop(0, rows, emit)
    pieces = []
    for source, offset in ((kap, PAD), (res, 0)):
        for y in range(0, rows, 2):
            both = (
                source[HALO + y, 0:tiles, offset : offset + x_count, :]
                + source[HALO + y + 1, 0:tiles, offset : offset + x_count, :]
            )
            pieces.append(along_lanes(both))
    flat[...] = product(jnp.concatenate(pieces, axis=0), halving(tiles * LANES))
    total = flat.shape[0]
    coarse[...] = flat[pl.ds(0, total // 2, stride=2), :] + flat[pl.ds(1, total // 2, stride=2), :]


def after_kernel(flags, *refs, count, offsets):
    blocks = refs[:count]
    (kap, diag, inv, xpre, rown, rlo, rhi, sol, resid) = refs[count : count + 9]
    (k1, d1, i1, r1, x1, va1, wa1, vb1, wb1, k2, d2, i2, r2, x2, va2, wa2, vb2, wb2, flat, va, wa, vb, wb, res, acc) = refs[count + 9 :]
    me_x, me_y = flags[4], flags[5]
    zero_pads((k1, va1, wa1, vb1, wb1, k2, va2, wa2, vb2, wb2, va, wa, vb, wb))
    each = blocks[0].shape[1]
    xc = blocks[0].shape[3]
    yc = each * count
    lo1, hi1 = COARSE_PAD, COARSE_PAD + yc
    edge = [lo1 - 1, hi1]
    for ref in (k1, va1, wa1, vb1, wb1):
        zero_rows(ref, edge)
    zero_rows(x1, list(range(lo1)) + list(range(hi1, hi1 + COARSE_PAD)))
    for block, offset in zip(blocks, offsets):
        at = lax.rem(me_y - offset + count, count) * each + COARSE_PAD
        for y in range(each):
            k1[at + y, :, PAD : PAD + xc, :] = block[0, y] * 0.25
            r1[at + y] = block[1, y]
    make_diagonal(k1, d1, i1, lo1, hi1)
    centre, weights = chebyshev_coefs(DEGREE, smooth_low)
    first_update(k1, i1, r1, va1, wa1, x1, lo1, hi1, 1.0 / centre, False)
    old, new = (va1, wa1), (vb1, wb1)
    for pair in weights:
        smoothing_step(k1, d1, i1, r1, old, new, x1, lo1, hi1, pair)
        old, new = new, old
    residual_only(k1, d1, r1, old[0], old[1], lo1, hi1)
    tiles1 = k1.shape[1]
    y2 = yc // 2
    half = xc // 2
    for target, source, offset, factor in ((k2, k1, PAD, 0.25), (r2, r1, 0, 1.0)):
        pieces = []
        for y in range(y2):
            a = lo1 + 2 * y
            both = source[a, :, offset : offset + xc, :] + source[a + 1, :, offset : offset + xc, :]
            pieces.append(along_lanes(both))
        flat[0 : y2 * xc, :] = product(jnp.concatenate(pieces, axis=0), halving(tiles1 * LANES))[:, 0:LANES]
        if target is k2:
            zero_rows(k2, range(y2 + 2))
        for y in range(y2):
            value = flat[pl.ds(y * xc, half, stride=2), :] + flat[pl.ds(y * xc + 1, half, stride=2), :]
            if target is k2:
                k2[1 + y, 0, PAD : PAD + half, :] = value * factor
            else:
                r2[1 + y] = jnp.zeros(r2.shape[1:], F32)
                r2[1 + y, 0, 0:half, :] = value
    for ref in (va2, wa2, vb2, wb2):
        zero_rows(ref, [0, y2 + 1])
    make_diagonal(k2, d2, i2, 1, 1 + y2, y2)
    centre, weights = chebyshev_coefs(COARSE_DEGREE, coarse_low)
    first_update(k2, i2, r2, va2, wa2, x2, 1, 1 + y2, 1.0 / centre, False, y2)
    old, new = (va2, wa2), (vb2, wb2)
    for pair in weights:
        smoothing_step(k2, d2, i2, r2, old, new, x2, 1, 1 + y2, pair, y2)
        old, new = new, old
    for y in range(y2):
        value = x2[1 + y, 0, 0:half, :]
        flat[pl.ds(y * xc, half, stride=2), :] = value
        flat[pl.ds(y * xc + 1, half, stride=2), :] = value
    wide = product(flat[0 : y2 * xc, :], doubling(2 * LANES))
    for y in range(y2):
        for t in range(tiles1):
            value = wide[y * xc : (y + 1) * xc, t * LANES : (t + 1) * LANES]
            for s in (0, 1):
                at = lo1 + 2 * y + s
                va1[at, t, PAD : PAD + xc, :] = value
                x1[at, t] = x1[at, t] + value
    times(k1, va1, wa1, lo1, hi1)
    centre, weights = chebyshev_coefs(DEGREE, smooth_low)
    residual_only(k1, d1, r1, va1, wa1, lo1, hi1)
    first_update(k1, i1, r1, va1, wa1, x1, lo1, hi1, 1.0 / centre, True)
    old, new = (va1, wa1), (vb1, wb1)
    for pair in weights:
        smoothing_step(k1, d1, i1, r1, old, new, x1, lo1, hi1, pair)
        old, new = new, old
    rows = rown.shape[0]
    last = HALO + rows
    x_count = rown.shape[2]
    wide_rows = (rows + 2 * HALO) // 2 + 1
    start = COARSE_PAD - (HALO + 1) // 2 + each * me_y
    for t in range(tiles1):
        for y in range(wide_rows):
            value = x1[start + y, t]
            base = (t * wide_rows + y) * x_count
            flat[pl.ds(base, xc, stride=2), :] = value
            flat[pl.ds(base + 1, xc, stride=2), :] = value
    n = wide_rows * x_count
    parts = []
    for t in range(tiles1 - 1):
        both = product(flat[t * n : (t + 1) * n, :], doubling(2 * LANES))
        parts += [both[:, 0:LANES], both[:, LANES:]]
    parts.append(product(flat[(tiles1 - 1) * n : tiles1 * n, :], halo_doubling()))
    own_tiles = len(parts) - 1
    for j in range(rows + 2 * HALO):
        y = (j + 1) // 2
        for t, part in enumerate(parts):
            value = part[y * x_count : (y + 1) * x_count, :]
            va[j, t, PAD : PAD + x_count, :] = value
            if HALO <= j < last and t < own_tiles:
                acc[j, t] = xpre[j - HALO, t] + value
    times(kap, va, wa, 0, rows + 2 * HALO)

    def fill(y):
        res[HALO + y] = rown[y]

    loop(0, rows, fill)
    for j in range(HALO - 1):
        res[1 + j] = rlo[j]
        res[last + j] = rhi[j]
    residual_only(kap, diag, res, va, wa, 1, last + HALO - 1)
    first_update(kap, inv, res, va, wa, acc, 1, last + HALO - 1, 1.0 / centre, True)
    old, new = (va, wa), (vb, wb)
    lo, hi = 2, last + HALO - 2
    for pair in weights:
        smoothing_step(kap, diag, inv, res, old, new, acc, lo, hi, pair)
        old, new = new, old
        lo, hi = lo + 1, hi - 1
    residual_only(kap, diag, res, old[0], old[1], HALO, last)
    block_x = sol.shape[0]
    first = pl.multiple_of(me_x * block_x, 8)
    for y in range(rows):
        for t in range(own_tiles):
            lanes = slice(t * LANES, (t + 1) * LANES)
            sol[:, y, lanes] = acc[HALO + y, t, pl.ds(first, block_x), :]
            resid[:, y, lanes] = res[HALO + y, t, pl.ds(first, block_x), :]


def ring(values, axis, step):
    count = lax.axis_size(axis)
    return lax.ppermute(values, axis, [(i, (i + step) % count) for i in range(count)])


def gather_first(values, axis, dim):
    count = lax.axis_size(axis)
    if count == 1:
        return values
    if count == 2:
        other = lax.ppermute(values, axis, [(0, 1), (1, 0)])
        first = lax.axis_index(axis) == 0
        return jnp.concatenate(
            [jnp.where(first, values, other), jnp.where(first, other, values)], axis=dim
        )
    every = lax.all_gather(values, axis)
    return jnp.concatenate([every[i] for i in range(count)], axis=dim)


def halo_tile(from_low, from_high, has_low, has_high):
    lane = lax.broadcasted_iota(jnp.int32, from_low.shape, from_low.ndim - 1)
    low = jnp.where(has_low, from_low, 0.0)
    high = jnp.where(has_high, from_high, 0.0)
    return jnp.where(lane < LANES // 2, high, low)


def vmem(shape):
    return pltpu.VMEM(shape, F32)


def call(kernel, out_shapes, scratch, inputs):
    limit = 4 * 2**20
    for s in scratch:
        size = 4
        for n in s.shape:
            size *= n
        limit += size
    for a in list(inputs) + list(out_shapes):
        limit += 4 * a.size if hasattr(a, "size") else 0
    limit = min(limit + 8 * 2**20, 60 * 2**20)
    whole = pl.BlockSpec(memory_space=pltpu.VMEM)
    return pl.pallas_call(
        kernel,
        out_shape=out_shapes,
        in_specs=[pl.BlockSpec(memory_space=pltpu.SMEM)] + [whole] * (len(inputs) - 1),
        out_specs=[whole] * len(out_shapes),
        scratch_shapes=scratch,
        compiler_params=pltpu.CompilerParams(vmem_limit_bytes=limit),
    )(*inputs)


def body(conductivity, source):
    bx, by, bz = conductivity.shape
    tiles = bz // LANES
    nx, ny, nz = (lax.axis_size(a) for a in ("gx", "gy", "gz"))
    ix, iy, iz = (lax.axis_index(a) for a in ("gx", "gy", "gz"))
    flags = jnp.stack([iz > 0, iz < nz - 1, iy > 0, iy < ny - 1, ix, iy]).astype(jnp.int32)
    has_left, has_right = iz > 0, iz < nz - 1
    x_count = bx * nx

    def shape(*dims):
        return jax.ShapeDtypeStruct(dims, F32)

    both = jnp.stack([conductivity, source]).reshape(2, bx, by, tiles, LANES)
    both = gather_first(both.transpose(0, 2, 3, 1, 4), "gx", 3)
    left = ring(both[:, :, tiles - 1], "gz", 1)
    right = ring(both[:, :, 0], "gz", -1)
    halo = halo_tile(left, right, has_left, has_right)
    own = jnp.concatenate([both, halo[:, :, None]], axis=2)
    ylo = ring(jnp.concatenate([own[0, by - HALO :], own[1, by - HALO + 1 :]], axis=0), "gy", 1)
    yhi = ring(jnp.concatenate([own[0, :HALO], own[1, : HALO - 1]], axis=0), "gy", -1)

    ext = by + 2 * HALO
    padded = x_count + 2 * PAD
    wide = (ext, tiles + 1, padded, LANES)
    plain = (ext, tiles + 1, x_count, LANES)
    each = by // 2
    xc = x_count // 2
    kap, diag, inv, xpre, rpre, coarse = call(
        before_kernel,
        [
            shape(*wide),
            shape(*plain),
            shape(*plain),
            shape(by, tiles, x_count, LANES),
            shape(by, tiles, x_count, LANES),
            shape(2 * each * xc, LANES),
        ],
        [vmem(wide)] * 4 + [vmem(plain)] * 2 + [vmem((2 * each * x_count, LANES))],
        [flags, own, ylo, yhi],
    )

    small = coarse.reshape(2 * each * xc, LANES)

    def with_tile(t):
        return jnp.concatenate([small, rpre[:, t].reshape(by * x_count, LANES)], axis=0)

    left = ring(with_tile(tiles - 1), "gz", 1)
    right = ring(with_tile(0), "gz", -1)
    halo = halo_tile(left, right, has_left, has_right)
    cut = 2 * each * xc
    coarse_halo = halo[:cut].reshape(2, each, 1, xc, LANES)
    coarse_own = jnp.concatenate([coarse.reshape(2, each, 1, xc, LANES), coarse_halo], axis=2)
    rown = jnp.concatenate([rpre, halo[cut:].reshape(by, 1, x_count, LANES)], axis=1)
    flat_coarse = coarse_own.reshape(-1, LANES)
    edge = HALO - 1
    n_flat = flat_coarse.shape[0]
    blocks, offsets = [coarse_own], [0]
    rlo = rhi = rown[:edge]
    for step in range(1, ny):
        parts = [flat_coarse]
        if step == 1:
            parts.append(rown[by - edge :].reshape(-1, LANES))
        if step == ny - 1:
            parts.append(rown[:edge].reshape(-1, LANES))
        got = ring(jnp.concatenate(parts, axis=0), "gy", step)
        blocks.append(got[:n_flat].reshape(coarse_own.shape))
        offsets.append(step)
        rest = got[n_flat:]
        size = edge * (tiles + 1) * x_count
        if step == 1:
            rlo = rest[:size].reshape(edge, tiles + 1, x_count, LANES)
            rest = rest[size:]
        if step == ny - 1:
            rhi = rest[:size].reshape(edge, tiles + 1, x_count, LANES)

    yc = each * ny
    tiles1 = tiles // 2 + 1
    wide1 = (yc + 2 * COARSE_PAD, tiles1, xc + 2 * PAD, LANES)
    plain1 = (yc + 2 * COARSE_PAD, tiles1, xc, LANES)
    y2 = yc // 2
    x2 = max(xc // 2, 8)
    wide2 = (y2 + 2, 1, x2 + 2 * PAD, LANES)
    plain2 = (y2 + 2, 1, x2, LANES)
    flat_rows = max(y2 * xc, tiles1 * (ext // 2 + 1) * x_count)

    def kernel(*refs):
        after_kernel(*refs, count=len(blocks), offsets=offsets)

    sol, resid = call(
        kernel,
        [shape(bx, by, bz), shape(bx, by, bz)],
        [vmem(wide1)] + [vmem(plain1)] * 4 + [vmem(wide1)] * 4
        + [vmem(wide2)] + [vmem(plain2)] * 4 + [vmem(wide2)] * 4
        + [vmem((flat_rows, LANES))] + [vmem(wide)] * 4 + [vmem(plain)] * 2,
        [flags] + blocks + [kap, diag, inv, xpre, rown, rlo, rhi],
    )
    return sol, resid


def solution(mesh):
    spec = P("gx", "gy", "gz")
    return jax.shard_map(body, mesh=mesh, in_specs=(spec, spec), out_specs=(spec, spec), check_vma=False)
```

```python
import jax
import jax.numpy as jnp
from jax import lax
from jax.experimental import pallas as pl
from jax.experimental.pallas import tpu as pltpu
from jax.sharding import PartitionSpec as P

DEGREE = 4
COARSE_DEGREE = 8
smooth_low = 0.5
coarse_low = 0.03
upper_bound = 2.0

F32 = jnp.float32
LANES = 128
PAD = 8
HALO = 5
COARSE_PAD = 4
FACE = 14.0 / 3.0
CORNER = 1.0 / 3.0
TOTAL = 128.0 / 3.0
SCALE = 0.05


def chebyshev_coefs(degree, lower):
    centre = (upper_bound + lower) / 2.0
    half_width = (upper_bound - lower) / 2.0
    ratio_term = centre / half_width
    rho_prev = 1.0 / ratio_term
    weights = []
    for number in range(1, degree):
        rho_next = 1.0 / (2.0 * ratio_term - rho_prev)
        weights.append((rho_next * rho_prev, 2.0 * rho_next / half_width))
        rho_prev = rho_next
    return centre, weights


CHUNK = 16


def chunks(start, stop, body):
    count = stop - start
    full = count // CHUNK
    if full == 1:
        body(start, CHUNK)
    elif full > 1:

        def step(i, carry):
            body(start + i * CHUNK, CHUNK)
            return carry

        lax.fori_loop(0, full, step, 0)
    if count % CHUNK:
        body(start + full * CHUNK, count % CHUNK)


def loop(start, stop, body):
    def group(first, rows):
        for i in range(rows):
            body(first + i)

    chunks(start, stop, group)


def third_pairs(values):
    tiles, rows, _ = values.shape
    flat = values.reshape(tiles * rows, LANES)
    up = pltpu.roll(flat, 1, 1).reshape(tiles, rows, LANES)
    down = pltpu.roll(flat, LANES - 1, 1).reshape(tiles, rows, LANES)
    if tiles > 1:
        lane = lax.broadcasted_iota(jnp.int32, (tiles, rows, LANES), 2)
        up_other = jnp.concatenate([up[tiles - 1 :], up[: tiles - 1]], axis=0)
        down_other = jnp.concatenate([down[1:], down[:1]], axis=0)
        up = jnp.where(lane == 0, up_other, up)
        down = jnp.where(lane == LANES - 1, down_other, down)
    return up + down


def neighbour_sums(ref, first, rows, row):
    at = range(first - 1, first + rows + 1) if isinstance(first, int) else [first + i for i in range(-1, rows + 1)]
    centre = [ref[y, :, row : row + 8, :] for y in at]
    side = [ref[y, :, row - 1 : row + 7, :] + ref[y, :, row + 1 : row + 9, :] for y in at]
    out = []
    for i in range(1, rows + 1):
        corner = side[i - 1] + side[i + 1]
        face = (centre[i - 1] + centre[i + 1]) + side[i]
        plane = FACE * face + corner
        beside = FACE * centre[i] + face + CORNER * corner
        out.append((plane + third_pairs(beside), centre[i]))
    return out


def zero_pads(refs):
    for ref in refs:
        count, tiles, rows, _ = ref.shape
        zero = jnp.zeros((tiles, PAD, LANES), F32)

        def body(y, ref=ref, rows=rows, zero=zero):
            ref[y, :, 0:PAD, :] = zero
            ref[y, :, rows - PAD : rows, :] = zero

        loop(0, count, body)


def zero_rows(ref, rows):
    zero = jnp.zeros(ref.shape[1:], F32)
    for y in rows:
        ref[y] = zero


def tiles_of(ref):
    return range(0, ref.shape[2], 8)


def make_diagonal(kap, diag, inv, lo, hi):
    def body(first, rows):
        for x in tiles_of(diag):
            for i, (total, centre) in enumerate(neighbour_sums(kap, first, rows, PAD + x)):
                value = TOTAL * centre + total
                diag[first + i, :, x : x + 8, :] = value
                inv[first + i, :, x : x + 8, :] = jnp.where(centre > 0.0, 1.0 / value, 0.0)

    chunks(lo, hi, body)


def first_update(kap, inv, res, v, w, acc, lo, hi, scale, add):
    def body(y):
        for x in tiles_of(inv):
            step = (inv[y, :, x : x + 8, :] * scale) * res[y, :, x : x + 8, :]
            v[y, :, PAD + x : PAD + x + 8, :] = step
            w[y, :, PAD + x : PAD + x + 8, :] = kap[y, :, PAD + x : PAD + x + 8, :] * step
            acc[y, :, x : x + 8, :] = acc[y, :, x : x + 8, :] + step if add else step

    loop(lo, hi, body)


def times(kap, v, w, lo, hi):
    def body(y):
        w[y] = kap[y] * v[y]

    loop(lo, hi, body)


def new_residuals(kap, diag, res, v, w, first, rows, x):
    total = neighbour_sums(v, first, rows, PAD + x)
    weighted = neighbour_sums(w, first, rows, PAD + x)
    for i in range(rows):
        y = first + i
        k = kap[y, :, PAD + x : PAD + x + 8, :]
        centre = total[i][1]
        value = (
            res[y, :, x : x + 8, :]
            - diag[y, :, x : x + 8, :] * centre
            + (k * total[i][0] + weighted[i][0])
        )
        res[y, :, x : x + 8, :] = value
        yield y, k, centre, value


def residual_only(kap, diag, res, v, w, lo, hi):
    def body(first, rows):
        for x in tiles_of(diag):
            for _ in new_residuals(kap, diag, res, v, w, first, rows, x):
                pass

    chunks(lo, hi, body)


def smoothing_step(kap, diag, inv, res, old, new, acc, lo, hi, pair):
    def body(first, rows):
        for x in tiles_of(diag):
            for y, k, centre, value in new_residuals(kap, diag, res, old[0], old[1], first, rows, x):
                step = pair[0] * centre + (pair[1] * inv[y, :, x : x + 8, :]) * value
                new[0][y, :, PAD + x : PAD + x + 8, :] = step
                new[1][y, :, PAD + x : PAD + x + 8, :] = k * step
                acc[y, :, x : x + 8, :] = acc[y, :, x : x + 8, :] + step

    chunks(lo, hi, body)


def halving(rows):
    row = lax.broadcasted_iota(jnp.int32, (rows, rows // 2), 0)
    col = lax.broadcasted_iota(jnp.int32, (rows, rows // 2), 1)
    return jnp.where(row // 2 == col, 0.125, 0.0).astype(F32)


def doubling(cols):
    row = lax.broadcasted_iota(jnp.int32, (cols // 2, cols), 0)
    col = lax.broadcasted_iota(jnp.int32, (cols // 2, cols), 1)
    return jnp.where(col // 2 == row, 1.0, 0.0).astype(F32)


def halo_doubling():
    row = lax.broadcasted_iota(jnp.int32, (LANES, LANES), 0)
    col = lax.broadcasted_iota(jnp.int32, (LANES, LANES), 1)
    source = col // 2 + jnp.where(col < LANES // 2, 0, LANES // 2)
    return jnp.where(source == row, 1.0, 0.0).astype(F32)


def product(left, right):
    return jnp.dot(left, right, precision=lax.Precision.HIGHEST, preferred_element_type=F32)


def along_lanes(values):
    return jnp.concatenate([values[t] for t in range(values.shape[0])], axis=-1)


def before_kernel(flags, own, ylo, yhi, kap, diag, inv, xout, rout, coarse, va, wa, vb, wb, res, acc, flat):
    rows = own.shape[1]
    x_count = own.shape[3]
    inner = slice(PAD, PAD + x_count)
    last = HALO + rows
    has_lo = flags[2] > 0
    has_hi = flags[3] > 0
    zero_pads((kap, va, wa, vb, wb))

    def fill(y):
        kap[HALO + y, :, inner, :] = SCALE * own[0, y]
        res[HALO + y] = own[1, y]

    loop(0, rows, fill)
    for j in range(HALO):
        kap[j, :, inner, :] = jnp.where(has_lo, SCALE * ylo[j], 0.0)
        kap[last + j, :, inner, :] = jnp.where(has_hi, SCALE * yhi[j], 0.0)
    for j in range(HALO - 1):
        res[1 + j] = ylo[HALO + j]
        res[last + j] = yhi[HALO + j]
    make_diagonal(kap, diag, inv, 1, last + HALO - 1)
    centre, weights = chebyshev_coefs(DEGREE, smooth_low)
    first_update(kap, inv, res, va, wa, acc, 1, last + HALO - 1, 1.0 / centre, False)
    old, new = (va, wa), (vb, wb)
    lo, hi = 2, last + HALO - 2
    for pair in weights:
        smoothing_step(kap, diag, inv, res, old, new, acc, lo, hi, pair)
        old, new = new, old
        lo, hi = lo + 1, hi - 1
    residual_only(kap, diag, res, old[0], old[1], HALO, last)
    tiles = rout.shape[1]

    def emit(y):
        xout[y] = acc[HALO + y, 0:tiles]
        rout[y] = res[HALO + y, 0:tiles]

    loop(0, rows, emit)
    pieces = []
    for source, offset in ((kap, PAD), (res, 0)):
        for y in range(0, rows, 2):
            both = (
                source[HALO + y, 0:tiles, offset : offset + x_count, :]
                + source[HALO + y + 1, 0:tiles, offset : offset + x_count, :]
            )
            pieces.append(along_lanes(both))
    flat[...] = product(jnp.concatenate(pieces, axis=0), halving(tiles * LANES))
    total = flat.shape[0]
    coarse[...] = flat[pl.ds(0, total // 2, stride=2), :] + flat[pl.ds(1, total // 2, stride=2), :]


def after_kernel(flags, *refs, count, offsets):
    blocks = refs[:count]
    (kap, diag, inv, xpre, rown, rlo, rhi, sol, resid) = refs[count : count + 9]
    (k1, d1, i1, r1, x1, va1, wa1, vb1, wb1, k2, d2, i2, r2, x2, va2, wa2, vb2, wb2, flat, va, wa, vb, wb, res, acc) = refs[count + 9 :]
    me_x, me_y = flags[4], flags[5]
    zero_pads((k1, va1, wa1, vb1, wb1, k2, va2, wa2, vb2, wb2, va, wa, vb, wb))
    each = blocks[0].shape[1]
    xc = blocks[0].shape[3]
    yc = each * count
    lo1, hi1 = COARSE_PAD, COARSE_PAD + yc
    edge = [lo1 - 1, hi1]
    for ref in (k1, va1, wa1, vb1, wb1):
        zero_rows(ref, edge)
    zero_rows(x1, list(range(lo1)) + list(range(hi1, hi1 + COARSE_PAD)))
    for block, offset in zip(blocks, offsets):
        at = lax.rem(me_y - offset + count, count) * each + COARSE_PAD
        for y in range(each):
            k1[at + y, :, PAD : PAD + xc, :] = block[0, y] * 0.25
            r1[at + y] = block[1, y]
    make_diagonal(k1, d1, i1, lo1, hi1)
    centre, weights = chebyshev_coefs(DEGREE, smooth_low)
    first_update(k1, i1, r1, va1, wa1, x1, lo1, hi1, 1.0 / centre, False)
    old, new = (va1, wa1), (vb1, wb1)
    for pair in weights:
        smoothing_step(k1, d1, i1, r1, old, new, x1, lo1, hi1, pair)
        old, new = new, old
    residual_only(k1, d1, r1, old[0], old[1], lo1, hi1)
    tiles1 = k1.shape[1]
    y2 = yc // 2
    half = xc // 2
    for target, source, offset, factor in ((k2, k1, PAD, 0.25), (r2, r1, 0, 1.0)):
        pieces = []
        for y in range(y2):
            a = lo1 + 2 * y
            both = source[a, :, offset : offset + xc, :] + source[a + 1, :, offset : offset + xc, :]
            pieces.append(along_lanes(both))
        flat[0 : y2 * xc, :] = product(jnp.concatenate(pieces, axis=0), halving(tiles1 * LANES))[:, 0:LANES]
        if target is k2:
            zero_rows(k2, range(y2 + 2))
        for y in range(y2):
            value = flat[pl.ds(y * xc, half, stride=2), :] + flat[pl.ds(y * xc + 1, half, stride=2), :]
            if target is k2:
                k2[1 + y, 0, PAD : PAD + half, :] = value * factor
            else:
                r2[1 + y] = jnp.zeros(r2.shape[1:], F32)
                r2[1 + y, 0, 0:half, :] = value
    for ref in (va2, wa2, vb2, wb2):
        zero_rows(ref, [0, y2 + 1])
    make_diagonal(k2, d2, i2, 1, 1 + y2)
    centre, weights = chebyshev_coefs(COARSE_DEGREE, coarse_low)
    first_update(k2, i2, r2, va2, wa2, x2, 1, 1 + y2, 1.0 / centre, False)
    old, new = (va2, wa2), (vb2, wb2)
    for pair in weights:
        smoothing_step(k2, d2, i2, r2, old, new, x2, 1, 1 + y2, pair)
        old, new = new, old
    for y in range(y2):
        value = x2[1 + y, 0, 0:half, :]
        flat[pl.ds(y * xc, half, stride=2), :] = value
        flat[pl.ds(y * xc + 1, half, stride=2), :] = value
    wide = product(flat[0 : y2 * xc, :], doubling(2 * LANES))
    for y in range(y2):
        for t in range(tiles1):
            value = wide[y * xc : (y + 1) * xc, t * LANES : (t + 1) * LANES]
            for s in (0, 1):
                at = lo1 + 2 * y + s
                va1[at, t, PAD : PAD + xc, :] = value
                x1[at, t] = x1[at, t] + value
    times(k1, va1, wa1, lo1, hi1)
    centre, weights = chebyshev_coefs(DEGREE, smooth_low)
    residual_only(k1, d1, r1, va1, wa1, lo1, hi1)
    first_update(k1, i1, r1, va1, wa1, x1, lo1, hi1, 1.0 / centre, True)
    old, new = (va1, wa1), (vb1, wb1)
    for pair in weights:
        smoothing_step(k1, d1, i1, r1, old, new, x1, lo1, hi1, pair)
        old, new = new, old
    rows = rown.shape[0]
    last = HALO + rows
    x_count = rown.shape[2]
    wide_rows = (rows + 2 * HALO) // 2 + 1
    start = COARSE_PAD - (HALO + 1) // 2 + each * me_y
    for t in range(tiles1):
        for y in range(wide_rows):
            value = x1[start + y, t]
            base = (t * wide_rows + y) * x_count
            flat[pl.ds(base, xc, stride=2), :] = value
            flat[pl.ds(base + 1, xc, stride=2), :] = value
    n = wide_rows * x_count
    parts = []
    for t in range(tiles1 - 1):
        both = product(flat[t * n : (t + 1) * n, :], doubling(2 * LANES))
        parts += [both[:, 0:LANES], both[:, LANES:]]
    parts.append(product(flat[(tiles1 - 1) * n : tiles1 * n, :], halo_doubling()))
    own_tiles = len(parts) - 1
    for j in range(rows + 2 * HALO):
        y = (j + 1) // 2
        for t, part in enumerate(parts):
            value = part[y * x_count : (y + 1) * x_count, :]
            va[j, t, PAD : PAD + x_count, :] = value
            if HALO <= j < last and t < own_tiles:
                acc[j, t] = xpre[j - HALO, t] + value
    times(kap, va, wa, 0, rows + 2 * HALO)

    def fill(y):
        res[HALO + y] = rown[y]

    loop(0, rows, fill)
    for j in range(HALO - 1):
        res[1 + j] = rlo[j]
        res[last + j] = rhi[j]
    residual_only(kap, diag, res, va, wa, 1, last + HALO - 1)
    first_update(kap, inv, res, va, wa, acc, 1, last + HALO - 1, 1.0 / centre, True)
    old, new = (va, wa), (vb, wb)
    lo, hi = 2, last + HALO - 2
    for pair in weights:
        smoothing_step(kap, diag, inv, res, old, new, acc, lo, hi, pair)
        old, new = new, old
        lo, hi = lo + 1, hi - 1
    residual_only(kap, diag, res, old[0], old[1], HALO, last)
    block_x = sol.shape[0]
    first = pl.multiple_of(me_x * block_x, 8)
    for y in range(rows):
        for t in range(own_tiles):
            lanes = slice(t * LANES, (t + 1) * LANES)
            sol[:, y, lanes] = acc[HALO + y, t, pl.ds(first, block_x), :]
            resid[:, y, lanes] = res[HALO + y, t, pl.ds(first, block_x), :]


def ring(values, axis, step):
    count = lax.axis_size(axis)
    return lax.ppermute(values, axis, [(i, (i + step) % count) for i in range(count)])


def gather_first(values, axis, dim):
    count = lax.axis_size(axis)
    if count == 1:
        return values
    if count == 2:
        other = lax.ppermute(values, axis, [(0, 1), (1, 0)])
        first = lax.axis_index(axis) == 0
        return jnp.concatenate(
            [jnp.where(first, values, other), jnp.where(first, other, values)], axis=dim
        )
    every = lax.all_gather(values, axis)
    return jnp.concatenate([every[i] for i in range(count)], axis=dim)


def halo_tile(from_low, from_high, has_low, has_high):
    lane = lax.broadcasted_iota(jnp.int32, from_low.shape, from_low.ndim - 1)
    low = jnp.where(has_low, from_low, 0.0)
    high = jnp.where(has_high, from_high, 0.0)
    return jnp.where(lane < LANES // 2, high, low)


def vmem(shape):
    return pltpu.VMEM(shape, F32)


def call(kernel, out_shapes, scratch, inputs):
    limit = 4 * 2**20
    for s in scratch:
        size = 4
        for n in s.shape:
            size *= n
        limit += size
    for a in list(inputs) + list(out_shapes):
        limit += 4 * a.size if hasattr(a, "size") else 0
    limit = min(limit + 8 * 2**20, 60 * 2**20)
    whole = pl.BlockSpec(memory_space=pltpu.VMEM)
    return pl.pallas_call(
        kernel,
        out_shape=out_shapes,
        in_specs=[pl.BlockSpec(memory_space=pltpu.SMEM)] + [whole] * (len(inputs) - 1),
        out_specs=[whole] * len(out_shapes),
        scratch_shapes=scratch,
        compiler_params=pltpu.CompilerParams(vmem_limit_bytes=limit),
    )(*inputs)


def body(conductivity, source):
    bx, by, bz = conductivity.shape
    tiles = bz // LANES
    nx, ny, nz = (lax.axis_size(a) for a in ("gx", "gy", "gz"))
    ix, iy, iz = (lax.axis_index(a) for a in ("gx", "gy", "gz"))
    flags = jnp.stack([iz > 0, iz < nz - 1, iy > 0, iy < ny - 1, ix, iy]).astype(jnp.int32)
    has_left, has_right = iz > 0, iz < nz - 1
    x_count = bx * nx

    def shape(*dims):
        return jax.ShapeDtypeStruct(dims, F32)

    both = jnp.stack([conductivity, source]).reshape(2, bx, by, tiles, LANES)
    both = gather_first(both.transpose(0, 2, 3, 1, 4), "gx", 3)
    left = ring(both[:, :, tiles - 1], "gz", 1)
    right = ring(both[:, :, 0], "gz", -1)
    halo = halo_tile(left, right, has_left, has_right)
    own = jnp.concatenate([both, halo[:, :, None]], axis=2)
    ylo = ring(jnp.concatenate([own[0, by - HALO :], own[1, by - HALO + 1 :]], axis=0), "gy", 1)
    yhi = ring(jnp.concatenate([own[0, :HALO], own[1, : HALO - 1]], axis=0), "gy", -1)

    ext = by + 2 * HALO
    padded = x_count + 2 * PAD
    wide = (ext, tiles + 1, padded, LANES)
    plain = (ext, tiles + 1, x_count, LANES)
    each = by // 2
    xc = x_count // 2
    kap, diag, inv, xpre, rpre, coarse = call(
        before_kernel,
        [
            shape(*wide),
            shape(*plain),
            shape(*plain),
            shape(by, tiles, x_count, LANES),
            shape(by, tiles, x_count, LANES),
            shape(2 * each * xc, LANES),
        ],
        [vmem(wide)] * 4 + [vmem(plain)] * 2 + [vmem((2 * each * x_count, LANES))],
        [flags, own, ylo, yhi],
    )

    small = coarse.reshape(2 * each * xc, LANES)

    def with_tile(t):
        return jnp.concatenate([small, rpre[:, t].reshape(by * x_count, LANES)], axis=0)

    left = ring(with_tile(tiles - 1), "gz", 1)
    right = ring(with_tile(0), "gz", -1)
    halo = halo_tile(left, right, has_left, has_right)
    cut = 2 * each * xc
    coarse_halo = halo[:cut].reshape(2, each, 1, xc, LANES)
    coarse_own = jnp.concatenate([coarse.reshape(2, each, 1, xc, LANES), coarse_halo], axis=2)
    rown = jnp.concatenate([rpre, halo[cut:].reshape(by, 1, x_count, LANES)], axis=1)
    flat_coarse = coarse_own.reshape(-1, LANES)
    edge = HALO - 1
    n_flat = flat_coarse.shape[0]
    blocks, offsets = [coarse_own], [0]
    rlo = rhi = rown[:edge]
    for step in range(1, ny):
        parts = [flat_coarse]
        if step == 1:
            parts.append(rown[by - edge :].reshape(-1, LANES))
        if step == ny - 1:
            parts.append(rown[:edge].reshape(-1, LANES))
        got = ring(jnp.concatenate(parts, axis=0), "gy", step)
        blocks.append(got[:n_flat].reshape(coarse_own.shape))
        offsets.append(step)
        rest = got[n_flat:]
        size = edge * (tiles + 1) * x_count
        if step == 1:
            rlo = rest[:size].reshape(edge, tiles + 1, x_count, LANES)
            rest = rest[size:]
        if step == ny - 1:
            rhi = rest[:size].reshape(edge, tiles + 1, x_count, LANES)

    yc = each * ny
    tiles1 = tiles // 2 + 1
    wide1 = (yc + 2 * COARSE_PAD, tiles1, xc + 2 * PAD, LANES)
    plain1 = (yc + 2 * COARSE_PAD, tiles1, xc, LANES)
    y2 = yc // 2
    x2 = max(xc // 2, 8)
    wide2 = (y2 + 2, 1, x2 + 2 * PAD, LANES)
    plain2 = (y2 + 2, 1, x2, LANES)
    flat_rows = max(y2 * xc, tiles1 * (ext // 2 + 1) * x_count)

    def kernel(*refs):
        after_kernel(*refs, count=len(blocks), offsets=offsets)

    sol, resid = call(
        kernel,
        [shape(bx, by, bz), shape(bx, by, bz)],
        [vmem(wide1)] + [vmem(plain1)] * 4 + [vmem(wide1)] * 4
        + [vmem(wide2)] + [vmem(plain2)] * 4 + [vmem(wide2)] * 4
        + [vmem((flat_rows, LANES))] + [vmem(wide)] * 4 + [vmem(plain)] * 2,
        [flags] + blocks + [kap, diag, inv, xpre, rown, rlo, rhi],
    )
    return sol, resid


def solution(mesh):
    spec = P("gx", "gy", "gz")
    return jax.shard_map(body, mesh=mesh, in_specs=(spec, spec), out_specs=(spec, spec), check_vma=False)
```

```python
import jax
import jax.numpy as jnp
from jax import lax
from jax.experimental import pallas as pl
from jax.experimental.pallas import tpu as pltpu
from jax.sharding import PartitionSpec as P

DEGREE = 4
COARSE_DEGREE = 8
smooth_low = 0.5
coarse_low = 0.03
upper_bound = 2.0

F32 = jnp.float32
LANES = 128
PAD = 8
HALO = 5
COARSE_PAD = 4
FACE = 14.0 / 3.0
CORNER = 1.0 / 3.0
TOTAL = 128.0 / 3.0
SCALE = 0.05


def chebyshev_coefs(degree, lower):
    centre = (upper_bound + lower) / 2.0
    half_width = (upper_bound - lower) / 2.0
    ratio_term = centre / half_width
    rho_prev = 1.0 / ratio_term
    weights = []
    for number in range(1, degree):
        rho_next = 1.0 / (2.0 * ratio_term - rho_prev)
        weights.append((rho_next * rho_prev, 2.0 * rho_next / half_width))
        rho_prev = rho_next
    return centre, weights


CHUNK = 16


def chunks(start, stop, body):
    count = stop - start
    full = count // CHUNK
    if full == 1:
        body(start, CHUNK)
    elif full > 1:

        def step(i, carry):
            body(start + i * CHUNK, CHUNK)
            return carry

        lax.fori_loop(0, full, step, 0)
    if count % CHUNK:
        body(start + full * CHUNK, count % CHUNK)


def loop(start, stop, body):
    def group(first, rows):
        for i in range(rows):
            body(first + i)

    chunks(start, stop, group)


def third_pairs(values):
    tiles, rows, _ = values.shape
    flat = values.reshape(tiles * rows, LANES)
    up = pltpu.roll(flat, 1, 1).reshape(tiles, rows, LANES)
    down = pltpu.roll(flat, LANES - 1, 1).reshape(tiles, rows, LANES)
    if tiles > 1:
        lane = lax.broadcasted_iota(jnp.int32, (tiles, rows, LANES), 2)
        up_other = jnp.concatenate([up[tiles - 1 :], up[: tiles - 1]], axis=0)
        down_other = jnp.concatenate([down[1:], down[:1]], axis=0)
        up = jnp.where(lane == 0, up_other, up)
        down = jnp.where(lane == LANES - 1, down_other, down)
    return up + down


def neighbour_sums(ref, first, rows, row):
    at = range(first - 1, first + rows + 1) if isinstance(first, int) else [first + i for i in range(-1, rows + 1)]
    centre = [ref[y, :, row : row + 8, :] for y in at]
    side = [ref[y, :, row - 1 : row + 7, :] + ref[y, :, row + 1 : row + 9, :] for y in at]
    out = []
    for i in range(1, rows + 1):
        corner = side[i - 1] + side[i + 1]
        face = (centre[i - 1] + centre[i + 1]) + side[i]
        plane = FACE * face + corner
        beside = FACE * centre[i] + face + CORNER * corner
        out.append((plane + third_pairs(beside), centre[i]))
    return out


def zero_pads(refs):
    for ref in refs:
        count, tiles, rows, _ = ref.shape
        zero = jnp.zeros((tiles, PAD, LANES), F32)

        def body(y, ref=ref, rows=rows, zero=zero):
            ref[y, :, 0:PAD, :] = zero
            ref[y, :, rows - PAD : rows, :] = zero

        loop(0, count, body)


def zero_rows(ref, rows):
    zero = jnp.zeros(ref.shape[1:], F32)
    for y in rows:
        ref[y] = zero


def tiles_of(ref):
    return range(0, ref.shape[2], 8)


def make_diagonal(kap, diag, inv, lo, hi):
    def body(first, rows):
        for x in tiles_of(diag):
            for i, (total, centre) in enumerate(neighbour_sums(kap, first, rows, PAD + x)):
                value = TOTAL * centre + total
                diag[first + i, :, x : x + 8, :] = value
                inv[first + i, :, x : x + 8, :] = jnp.where(centre > 0.0, 1.0 / value, 0.0)

    chunks(lo, hi, body)


def first_update(kap, inv, res, v, w, acc, lo, hi, scale, add):
    def body(y):
        for x in tiles_of(inv):
            step = (inv[y, :, x : x + 8, :] * scale) * res[y, :, x : x + 8, :]
            v[y, :, PAD + x : PAD + x + 8, :] = step
            w[y, :, PAD + x : PAD + x + 8, :] = kap[y, :, PAD + x : PAD + x + 8, :] * step
            acc[y, :, x : x + 8, :] = acc[y, :, x : x + 8, :] + step if add else step

    loop(lo, hi, body)


def times(kap, v, w, lo, hi):
    def body(y):
        w[y] = kap[y] * v[y]

    loop(lo, hi, body)


def new_residuals(kap, diag, res, v, w, first, rows, x):
    total = neighbour_sums(v, first, rows, PAD + x)
    weighted = neighbour_sums(w, first, rows, PAD + x)
    for i in range(rows):
        y = first + i
        k = kap[y, :, PAD + x : PAD + x + 8, :]
        centre = total[i][1]
        value = (
            res[y, :, x : x + 8, :]
            - diag[y, :, x : x + 8, :] * centre
            + (k * total[i][0] + weighted[i][0])
        )
        res[y, :, x : x + 8, :] = value
        yield y, k, centre, value


def residual_only(kap, diag, res, v, w, lo, hi):
    def body(first, rows):
        for x in tiles_of(diag):
            for _ in new_residuals(kap, diag, res, v, w, first, rows, x):
                pass

    chunks(lo, hi, body)


def smoothing_step(kap, diag, inv, res, old, new, acc, lo, hi, pair):
    def body(first, rows):
        for x in tiles_of(diag):
            for y, k, centre, value in new_residuals(kap, diag, res, old[0], old[1], first, rows, x):
                step = pair[0] * centre + (pair[1] * inv[y, :, x : x + 8, :]) * value
                new[0][y, :, PAD + x : PAD + x + 8, :] = step
                new[1][y, :, PAD + x : PAD + x + 8, :] = k * step
                acc[y, :, x : x + 8, :] = acc[y, :, x : x + 8, :] + step

    chunks(lo, hi, body)


def halving(rows):
    row = lax.broadcasted_iota(jnp.int32, (rows, rows // 2), 0)
    col = lax.broadcasted_iota(jnp.int32, (rows, rows // 2), 1)
    return jnp.where(row // 2 == col, 0.125, 0.0).astype(F32)


def doubling(cols):
    row = lax.broadcasted_iota(jnp.int32, (cols // 2, cols), 0)
    col = lax.broadcasted_iota(jnp.int32, (cols // 2, cols), 1)
    return jnp.where(col // 2 == row, 1.0, 0.0).astype(F32)


def halo_doubling():
    row = lax.broadcasted_iota(jnp.int32, (LANES, LANES), 0)
    col = lax.broadcasted_iota(jnp.int32, (LANES, LANES), 1)
    source = col // 2 + jnp.where(col < LANES // 2, 0, LANES // 2)
    return jnp.where(source == row, 1.0, 0.0).astype(F32)


def product(left, right):
    return jnp.dot(left, right, precision=lax.Precision.HIGHEST, preferred_element_type=F32)


def along_lanes(values):
    return jnp.concatenate([values[t] for t in range(values.shape[0])], axis=-1)


def before_kernel(flags, own, ylo, yhi, kap, diag, inv, xout, rout, coarse, va, wa, vb, wb, res, acc, flat):
    rows = own.shape[1]
    x_count = own.shape[3]
    inner = slice(PAD, PAD + x_count)
    last = HALO + rows
    has_lo = flags[2] > 0
    has_hi = flags[3] > 0
    zero_pads((kap, va, wa, vb, wb))

    def fill(y):
        kap[HALO + y, :, inner, :] = SCALE * own[0, y]
        res[HALO + y] = own[1, y]

    loop(0, rows, fill)
    for j in range(HALO):
        kap[j, :, inner, :] = jnp.where(has_lo, SCALE * ylo[j], 0.0)
        kap[last + j, :, inner, :] = jnp.where(has_hi, SCALE * yhi[j], 0.0)
    for j in range(HALO - 1):
        res[1 + j] = ylo[HALO + j]
        res[last + j] = yhi[HALO + j]
    make_diagonal(kap, diag, inv, 1, last + HALO - 1)
    centre, weights = chebyshev_coefs(DEGREE, smooth_low)
    first_update(kap, inv, res, va, wa, acc, 1, last + HALO - 1, 1.0 / centre, False)
    old, new = (va, wa), (vb, wb)
    lo, hi = 2, last + HALO - 2
    for pair in weights:
        smoothing_step(kap, diag, inv, res, old, new, acc, lo, hi, pair)
        old, new = new, old
        lo, hi = lo + 1, hi - 1
    residual_only(kap, diag, res, old[0], old[1], HALO, last)
    tiles = rout.shape[1]

    def emit(y):
        xout[y] = acc[HALO + y, 0:tiles]
        rout[y] = res[HALO + y, 0:tiles]

    loop(0, rows, emit)
    pieces = []
    for source, offset in ((kap, PAD), (res, 0)):
        for y in range(0, rows, 2):
            both = (
                source[HALO + y, 0:tiles, offset : offset + x_count, :]
                + source[HALO + y + 1, 0:tiles, offset : offset + x_count, :]
            )
            pieces.append(along_lanes(both))
    flat[...] = product(jnp.concatenate(pieces, axis=0), halving(tiles * LANES))
    total = flat.shape[0]
    coarse[...] = flat[pl.ds(0, total // 2, stride=2), :] + flat[pl.ds(1, total // 2, stride=2), :]


def after_kernel(places, *refs, count):
    blocks = refs[:count]
    (kap, diag, inv, xpre, rown, rlo, rhi, sol, resid) = refs[count : count + 9]
    (k1, d1, i1, r1, x1, va1, wa1, vb1, wb1, k2, d2, i2, r2, x2, va2, wa2, vb2, wb2, flat, va, wa, vb, wb, res, acc) = refs[count + 9 :]
    me_x, me_y = places[0], places[1]
    zero_pads((k1, va1, wa1, vb1, wb1, k2, va2, wa2, vb2, wb2, va, wa, vb, wb))
    each = blocks[0].shape[1]
    xc = blocks[0].shape[3]
    yc = each * count
    lo1, hi1 = COARSE_PAD, COARSE_PAD + yc
    edge = [lo1 - 1, hi1]
    for ref in (k1, va1, wa1, vb1, wb1):
        zero_rows(ref, edge)
    zero_rows(x1, list(range(lo1)) + list(range(hi1, hi1 + COARSE_PAD)))
    for number, block in enumerate(blocks):
        at = places[2 + number] * each + COARSE_PAD
        for y in range(each):
            k1[at + y, :, PAD : PAD + xc, :] = block[0, y] * 0.25
            r1[at + y] = block[1, y]
    make_diagonal(k1, d1, i1, lo1, hi1)
    centre, weights = chebyshev_coefs(DEGREE, smooth_low)
    first_update(k1, i1, r1, va1, wa1, x1, lo1, hi1, 1.0 / centre, False)
    old, new = (va1, wa1), (vb1, wb1)
    for pair in weights:
        smoothing_step(k1, d1, i1, r1, old, new, x1, lo1, hi1, pair)
        old, new = new, old
    residual_only(k1, d1, r1, old[0], old[1], lo1, hi1)
    tiles1 = k1.shape[1]
    y2 = yc // 2
    half = xc // 2
    for target, source, offset, factor in ((k2, k1, PAD, 0.25), (r2, r1, 0, 1.0)):
        pieces = []
        for y in range(y2):
            a = lo1 + 2 * y
            both = source[a, :, offset : offset + xc, :] + source[a + 1, :, offset : offset + xc, :]
            pieces.append(along_lanes(both))
        flat[0 : y2 * xc, :] = product(jnp.concatenate(pieces, axis=0), halving(tiles1 * LANES))[:, 0:LANES]
        if target is k2:
            zero_rows(k2, range(y2 + 2))
        for y in range(y2):
            value = flat[pl.ds(y * xc, half, stride=2), :] + flat[pl.ds(y * xc + 1, half, stride=2), :]
            if target is k2:
                k2[1 + y, 0, PAD : PAD + half, :] = value * factor
            else:
                r2[1 + y] = jnp.zeros(r2.shape[1:], F32)
                r2[1 + y, 0, 0:half, :] = value
    for ref in (va2, wa2, vb2, wb2):
        zero_rows(ref, [0, y2 + 1])
    make_diagonal(k2, d2, i2, 1, 1 + y2)
    centre, weights = chebyshev_coefs(COARSE_DEGREE, coarse_low)
    first_update(k2, i2, r2, va2, wa2, x2, 1, 1 + y2, 1.0 / centre, False)
    old, new = (va2, wa2), (vb2, wb2)
    for pair in weights:
        smoothing_step(k2, d2, i2, r2, old, new, x2, 1, 1 + y2, pair)
        old, new = new, old
    for y in range(y2):
        value = x2[1 + y, 0, 0:half, :]
        flat[pl.ds(y * xc, half, stride=2), :] = value
        flat[pl.ds(y * xc + 1, half, stride=2), :] = value
    wide = product(flat[0 : y2 * xc, :], doubling(2 * LANES))
    for y in range(y2):
        for t in range(tiles1):
            value = wide[y * xc : (y + 1) * xc, t * LANES : (t + 1) * LANES]
            for s in (0, 1):
                at = lo1 + 2 * y + s
                va1[at, t, PAD : PAD + xc, :] = value
                x1[at, t] = x1[at, t] + value
    times(k1, va1, wa1, lo1, hi1)
    centre, weights = chebyshev_coefs(DEGREE, smooth_low)
    residual_only(k1, d1, r1, va1, wa1, lo1, hi1)
    first_update(k1, i1, r1, va1, wa1, x1, lo1, hi1, 1.0 / centre, True)
    old, new = (va1, wa1), (vb1, wb1)
    for pair in weights:
        smoothing_step(k1, d1, i1, r1, old, new, x1, lo1, hi1, pair)
        old, new = new, old
    rows = rown.shape[0]
    last = HALO + rows
    x_count = rown.shape[2]
    wide_rows = (rows + 2 * HALO) // 2 + 1
    start = COARSE_PAD - (HALO + 1) // 2 + each * me_y
    for t in range(tiles1):
        for y in range(wide_rows):
            value = x1[start + y, t]
            base = (t * wide_rows + y) * x_count
            flat[pl.ds(base, xc, stride=2), :] = value
            flat[pl.ds(base + 1, xc, stride=2), :] = value
    n = wide_rows * x_count
    parts = []
    for t in range(tiles1 - 1):
        both = product(flat[t * n : (t + 1) * n, :], doubling(2 * LANES))
        parts += [both[:, 0:LANES], both[:, LANES:]]
    parts.append(product(flat[(tiles1 - 1) * n : tiles1 * n, :], halo_doubling()))
    own_tiles = len(parts) - 1
    for j in range(rows + 2 * HALO):
        y = (j + 1) // 2
        for t, part in enumerate(parts):
            value = part[y * x_count : (y + 1) * x_count, :]
            va[j, t, PAD : PAD + x_count, :] = value
            if HALO <= j < last and t < own_tiles:
                acc[j, t] = xpre[j - HALO, t] + value
    times(kap, va, wa, 0, rows + 2 * HALO)

    def fill(y):
        res[HALO + y] = rown[y]

    loop(0, rows, fill)
    for j in range(HALO - 1):
        res[1 + j] = rlo[j]
        res[last + j] = rhi[j]
    residual_only(kap, diag, res, va, wa, 1, last + HALO - 1)
    first_update(kap, inv, res, va, wa, acc, 1, last + HALO - 1, 1.0 / centre, True)
    old, new = (va, wa), (vb, wb)
    lo, hi = 2, last + HALO - 2
    for pair in weights:
        smoothing_step(kap, diag, inv, res, old, new, acc, lo, hi, pair)
        old, new = new, old
        lo, hi = lo + 1, hi - 1
    residual_only(kap, diag, res, old[0], old[1], HALO, last)
    block_x = sol.shape[0]
    first = pl.multiple_of(me_x * block_x, 8)
    for y in range(rows):
        for t in range(own_tiles):
            lanes = slice(t * LANES, (t + 1) * LANES)
            sol[:, y, lanes] = acc[HALO + y, t, pl.ds(first, block_x), :]
            resid[:, y, lanes] = res[HALO + y, t, pl.ds(first, block_x), :]


def ring(values, axis, step):
    count = lax.axis_size(axis)
    return lax.ppermute(values, axis, [(i, (i + step) % count) for i in range(count)])


def exchange(to_low, to_high, axis, across=None):
    count = lax.axis_size(axis)
    if count % 2:
        return ring(to_high, axis, 1), ring(to_low, axis, -1)
    odd = lax.axis_index(axis) % 2 == 1
    inner = [i + 1 if i % 2 else i - 1 for i in range(count)]
    one = lax.ppermute(jnp.where(odd, to_low, to_high), axis, [(i, i ^ 1) for i in range(count)])
    names, pairs = axis, [(i, t % count) for i, t in enumerate(inner)]
    if across is not None and lax.axis_size(across) % 2 == 0:
        names = (across, axis)
        pairs = [
            (x * count + i, x * count + t if 0 <= t < count else (x ^ 1) * count + i)
            for x in range(lax.axis_size(across))
            for i, t in enumerate(inner)
        ]
    two = lax.ppermute(jnp.where(odd, to_high, to_low), names, pairs)
    return jnp.where(odd, one, two), jnp.where(odd, two, one)


def gather_first(values, axis, dim):
    count = lax.axis_size(axis)
    if count == 1:
        return values
    if count == 2:
        other = lax.ppermute(values, axis, [(0, 1), (1, 0)])
        first = lax.axis_index(axis) == 0
        return jnp.concatenate(
            [jnp.where(first, values, other), jnp.where(first, other, values)], axis=dim
        )
    every = lax.all_gather(values, axis)
    return jnp.concatenate([every[i] for i in range(count)], axis=dim)


def gather_second(block, low_edge, high_edge, me, count):
    size = block.size // LANES
    shape = block.shape
    low_edge = low_edge.reshape(-1, LANES)
    high_edge = high_edge.reshape(-1, LANES)
    block_rows = block.reshape(size, LANES)
    blocks, sources = [block], [me]
    low = high = low_edge
    if count == 4:
        odd = me % 2 == 1
        got = []
        for step in (1, 2, 3):
            payload = block_rows
            if step != 2:
                edge = jnp.where(odd == (step == 1), low_edge, high_edge)
                payload = jnp.concatenate([block_rows, edge], axis=0)
            got.append(lax.ppermute(payload, "gy", [(i, i ^ step) for i in range(count)]))
            blocks.append(got[-1][:size].reshape(shape))
            sources.append(me ^ step)
        low = jnp.where(odd, got[0][size:], got[2][size:])
        high = jnp.where(odd, got[2][size:], got[0][size:])
    else:
        for step in range(1, count):
            parts = [block_rows]
            if step == 1:
                parts.append(high_edge)
            if step == count - 1:
                parts.append(low_edge)
            got = ring(jnp.concatenate(parts, axis=0), "gy", step)
            blocks.append(got[:size].reshape(shape))
            sources.append((me - step) % count)
            if step == 1:
                low = got[size : size + high_edge.shape[0]]
            if step == count - 1:
                high = got[got.shape[0] - low_edge.shape[0] :]
    return blocks, sources, low, high


def halo_tile(from_low, from_high, has_low, has_high):
    lane = lax.broadcasted_iota(jnp.int32, from_low.shape, from_low.ndim - 1)
    low = jnp.where(has_low, from_low, 0.0)
    high = jnp.where(has_high, from_high, 0.0)
    return jnp.where(lane < LANES // 2, high, low)


def vmem(shape):
    return pltpu.VMEM(shape, F32)


def call(kernel, out_shapes, scratch, inputs):
    limit = 4 * 2**20
    for s in scratch:
        size = 4
        for n in s.shape:
            size *= n
        limit += size
    for a in list(inputs) + list(out_shapes):
        limit += 4 * a.size if hasattr(a, "size") else 0
    limit = min(limit + 8 * 2**20, 60 * 2**20)
    whole = pl.BlockSpec(memory_space=pltpu.VMEM)
    return pl.pallas_call(
        kernel,
        out_shape=out_shapes,
        in_specs=[pl.BlockSpec(memory_space=pltpu.SMEM)] + [whole] * (len(inputs) - 1),
        out_specs=[whole] * len(out_shapes),
        scratch_shapes=scratch,
        compiler_params=pltpu.CompilerParams(vmem_limit_bytes=limit),
    )(*inputs)


def body(conductivity, source):
    bx, by, bz = conductivity.shape
    tiles = bz // LANES
    nx, ny, nz = (lax.axis_size(a) for a in ("gx", "gy", "gz"))
    ix, iy, iz = (lax.axis_index(a) for a in ("gx", "gy", "gz"))
    flags = jnp.stack([iz > 0, iz < nz - 1, iy > 0, iy < ny - 1]).astype(jnp.int32)
    has_left, has_right = iz > 0, iz < nz - 1
    x_count = bx * nx

    def shape(*dims):
        return jax.ShapeDtypeStruct(dims, F32)

    both = jnp.stack([conductivity, source]).reshape(2, bx, by, tiles, LANES)
    both = gather_first(both.transpose(0, 2, 3, 1, 4), "gx", 3)
    left, right = exchange(both[:, :, 0], both[:, :, tiles - 1], "gz")
    halo = halo_tile(left, right, has_left, has_right)
    own = jnp.concatenate([both, halo[:, :, None]], axis=2)
    ylo, yhi = exchange(
        jnp.concatenate([own[0, :HALO], own[1, : HALO - 1]], axis=0),
        jnp.concatenate([own[0, by - HALO :], own[1, by - HALO + 1 :]], axis=0),
        "gy",
        "gx",
    )

    ext = by + 2 * HALO
    padded = x_count + 2 * PAD
    wide = (ext, tiles + 1, padded, LANES)
    plain = (ext, tiles + 1, x_count, LANES)
    each = by // 2
    xc = x_count // 2
    kap, diag, inv, xpre, rpre, coarse = call(
        before_kernel,
        [
            shape(*wide),
            shape(*plain),
            shape(*plain),
            shape(by, tiles, x_count, LANES),
            shape(by, tiles, x_count, LANES),
            shape(2 * each * xc, LANES),
        ],
        [vmem(wide)] * 4 + [vmem(plain)] * 2 + [vmem((2 * each * x_count, LANES))],
        [flags, own, ylo, yhi],
    )

    small = coarse.reshape(2 * each * xc, LANES)

    def with_tile(t):
        return jnp.concatenate([small, rpre[:, t].reshape(by * x_count, LANES)], axis=0)

    left, right = exchange(with_tile(0), with_tile(tiles - 1), "gz")
    halo = halo_tile(left, right, has_left, has_right)
    cut = 2 * each * xc
    coarse_halo = halo[:cut].reshape(2, each, 1, xc, LANES)
    coarse_own = jnp.concatenate([coarse.reshape(2, each, 1, xc, LANES), coarse_halo], axis=2)
    rown = jnp.concatenate([rpre, halo[cut:].reshape(by, 1, x_count, LANES)], axis=1)
    flat_coarse = coarse_own.reshape(-1, LANES)
    edge = HALO - 1
    blocks, sources, rlo, rhi = gather_second(coarse_own, rown[:edge], rown[by - edge :], iy, ny)

    yc = each * ny
    tiles1 = tiles // 2 + 1
    wide1 = (yc + 2 * COARSE_PAD, tiles1, xc + 2 * PAD, LANES)
    plain1 = (yc + 2 * COARSE_PAD, tiles1, xc, LANES)
    y2 = yc // 2
    x2 = max(xc // 2, 8)
    wide2 = (y2 + 2, 1, x2 + 2 * PAD, LANES)
    plain2 = (y2 + 2, 1, x2, LANES)
    flat_rows = max(y2 * xc, tiles1 * (ext // 2 + 1) * x_count)

    places = jnp.stack([ix, iy] + sources).astype(jnp.int32)

    def kernel(*refs):
        after_kernel(*refs, count=len(blocks))

    sol, resid = call(
        kernel,
        [shape(bx, by, bz), shape(bx, by, bz)],
        [vmem(wide1)] + [vmem(plain1)] * 4 + [vmem(wide1)] * 4
        + [vmem(wide2)] + [vmem(plain2)] * 4 + [vmem(wide2)] * 4
        + [vmem((flat_rows, LANES))] + [vmem(wide)] * 4 + [vmem(plain)] * 2,
        [places] + blocks
        + [kap, diag, inv, xpre, rown]
        + [e.reshape(edge, tiles + 1, x_count, LANES) for e in (rlo, rhi)],
    )
    return sol, resid


def solution(mesh):
    spec = P("gx", "gy", "gz")
    return jax.shard_map(body, mesh=mesh, in_specs=(spec, spec), out_specs=(spec, spec), check_vma=False)
```

```python
import jax
import jax.numpy as jnp
from jax import lax
from jax.experimental import pallas as pl
from jax.experimental.pallas import tpu as pltpu
from jax.sharding import PartitionSpec as P

DEGREE = 4
COARSE_DEGREE = 8
smooth_low = 0.5
coarse_low = 0.03
upper_bound = 2.0

F32 = jnp.float32
LANES = 128
PAD = 8
HALO = 5
COARSE_PAD = 4
FACE = 14.0 / 3.0
CORNER = 1.0 / 3.0
TOTAL = 128.0 / 3.0
SCALE = 0.05


def chebyshev_coefs(degree, lower):
    centre = (upper_bound + lower) / 2.0
    half_width = (upper_bound - lower) / 2.0
    ratio_term = centre / half_width
    rho_prev = 1.0 / ratio_term
    weights = []
    for number in range(1, degree):
        rho_next = 1.0 / (2.0 * ratio_term - rho_prev)
        weights.append((rho_next * rho_prev, 2.0 * rho_next / half_width))
        rho_prev = rho_next
    return centre, weights


EDGE = 8
COARSE_EDGE = 32
CHUNK = 16


def chunks(start, stop, body):
    count = stop - start
    full = count // CHUNK
    if full == 1:
        body(start, CHUNK)
    elif full > 1:

        def step(i, carry):
            body(start + i * CHUNK, CHUNK)
            return carry

        lax.fori_loop(0, full, step, 0)
    if count % CHUNK:
        body(start + full * CHUNK, count % CHUNK)


def loop(start, stop, body):
    def group(first, rows):
        for i in range(rows):
            body(first + i)

    chunks(start, stop, group)


def third_pairs(values):
    tiles, rows, _ = values.shape
    flat = values.reshape(tiles * rows, LANES)
    up = pltpu.roll(flat, 1, 1).reshape(tiles, rows, LANES)
    down = pltpu.roll(flat, LANES - 1, 1).reshape(tiles, rows, LANES)
    if tiles > 1:
        lane = lax.broadcasted_iota(jnp.int32, (tiles, rows, LANES), 2)
        up_other = jnp.concatenate([up[tiles - 1 :], up[: tiles - 1]], axis=0)
        down_other = jnp.concatenate([down[1:], down[:1]], axis=0)
        up = jnp.where(lane == 0, up_other, up)
        down = jnp.where(lane == LANES - 1, down_other, down)
    return up + down


def neighbour_sums(ref, first, rows, row):
    at = range(first - 1, first + rows + 1) if isinstance(first, int) else [first + i for i in range(-1, rows + 1)]
    centre = [ref[y, :, row : row + 8, :] for y in at]
    side = [ref[y, :, row - 1 : row + 7, :] + ref[y, :, row + 1 : row + 9, :] for y in at]
    out = []
    for i in range(1, rows + 1):
        corner = side[i - 1] + side[i + 1]
        face = (centre[i - 1] + centre[i + 1]) + side[i]
        plane = FACE * face + corner
        beside = FACE * centre[i] + face + CORNER * corner
        out.append((plane + third_pairs(beside), centre[i]))
    return out


def zero_pads(refs):
    for ref in refs:
        count, tiles, rows, _ = ref.shape
        zero = jnp.zeros((tiles, PAD, LANES), F32)

        def body(y, ref=ref, rows=rows, zero=zero):
            ref[y, :, 0:PAD, :] = zero
            ref[y, :, rows - PAD : rows, :] = zero

        loop(0, count, body)


def zero_rows(ref, rows):
    zero = jnp.zeros(ref.shape[1:], F32)
    for y in rows:
        ref[y] = zero


def tiles_of(ref):
    return range(0, ref.shape[2], 8)


def make_diagonal(kap, diag, inv, lo, hi):
    def body(first, rows):
        for x in tiles_of(diag):
            for i, (total, centre) in enumerate(neighbour_sums(kap, first, rows, PAD + x)):
                value = TOTAL * centre + total
                diag[first + i, :, x : x + 8, :] = value
                inv[first + i, :, x : x + 8, :] = jnp.where(centre > 0.0, 1.0 / value, 0.0)

    chunks(lo, hi, body)


def accumulate(acc, y, x, step, add, own):
    tiles = step.shape[0]
    if own is not None:
        if isinstance(y, int) and not own[0] <= y < own[1]:
            return
        tiles = own[2]
    step = step[0:tiles]
    acc[y, 0:tiles, x : x + 8, :] = acc[y, 0:tiles, x : x + 8, :] + step if add else step


def first_update(kap, inv, res, v, w, acc, lo, hi, scale, add, own=None):
    def body(y):
        for x in tiles_of(inv):
            step = (inv[y, :, x : x + 8, :] * scale) * res[y, :, x : x + 8, :]
            v[y, :, PAD + x : PAD + x + 8, :] = step
            w[y, :, PAD + x : PAD + x + 8, :] = kap[y, :, PAD + x : PAD + x + 8, :] * step
            accumulate(acc, y, x, step, add, own)

    loop(lo, hi, body)


def times(kap, v, w, lo, hi):
    def body(y):
        w[y] = kap[y] * v[y]

    loop(lo, hi, body)


def new_residuals(kap, diag, res, v, w, first, rows, x):
    total = neighbour_sums(v, first, rows, PAD + x)
    weighted = neighbour_sums(w, first, rows, PAD + x)
    for i in range(rows):
        y = first + i
        k = kap[y, :, PAD + x : PAD + x + 8, :]
        centre = total[i][1]
        value = (
            res[y, :, x : x + 8, :]
            - diag[y, :, x : x + 8, :] * centre
            + (k * total[i][0] + weighted[i][0])
        )
        res[y, :, x : x + 8, :] = value
        yield y, k, centre, value


def residual_only(kap, diag, res, v, w, lo, hi):
    def body(first, rows):
        for x in tiles_of(diag):
            for _ in new_residuals(kap, diag, res, v, w, first, rows, x):
                pass

    chunks(lo, hi, body)


def smoothing_step(kap, diag, inv, res, old, new, acc, lo, hi, pair, own=None):
    def body(first, rows):
        for x in tiles_of(diag):
            for y, k, centre, value in new_residuals(kap, diag, res, old[0], old[1], first, rows, x):
                step = pair[0] * centre + (pair[1] * inv[y, :, x : x + 8, :]) * value
                new[0][y, :, PAD + x : PAD + x + 8, :] = step
                new[1][y, :, PAD + x : PAD + x + 8, :] = k * step
                accumulate(acc, y, x, step, True, own)

    chunks(lo, hi, body)


def halving(rows):
    row = lax.broadcasted_iota(jnp.int32, (rows, rows // 2), 0)
    col = lax.broadcasted_iota(jnp.int32, (rows, rows // 2), 1)
    return jnp.where(row // 2 == col, 0.125, 0.0).astype(F32)


def doubling(cols):
    row = lax.broadcasted_iota(jnp.int32, (cols // 2, cols), 0)
    col = lax.broadcasted_iota(jnp.int32, (cols // 2, cols), 1)
    return jnp.where(col // 2 == row, 1.0, 0.0).astype(F32)


def halo_doubling():
    row = lax.broadcasted_iota(jnp.int32, (LANES, LANES), 0)
    col = lax.broadcasted_iota(jnp.int32, (LANES, LANES), 1)
    source = col // 2 + jnp.where(col < LANES // 2, 0, LANES // 2)
    return jnp.where(source == row, 1.0, 0.0).astype(F32)


def product(left, right):
    return jnp.dot(left, right, precision=lax.Precision.HIGHEST, preferred_element_type=F32)


def along_lanes(values):
    return jnp.concatenate([values[t] for t in range(values.shape[0])], axis=-1)


def pack(pieces, width, from_end):
    lane = lax.broadcasted_iota(jnp.int32, pieces[0].shape, 1)
    out = jnp.zeros(pieces[0].shape, F32)
    for i, piece in enumerate(pieces):
        shift = (width * i + (width if from_end else 0)) % LANES
        moved = pltpu.roll(piece, shift, 1) if shift else piece
        out = jnp.where((lane >= width * i) & (lane < width * (i + 1)), moved, out)
    return out


def unpack(left, right, i, width):
    lane = lax.broadcasted_iota(jnp.int32, left.shape, 1)
    back = (LANES - width * i) % LANES
    end = (LANES - width - width * i) % LANES
    first = pltpu.roll(right, back, 1) if back else right
    last = pltpu.roll(left, end, 1) if end else left
    return jnp.where(lane < width, first, jnp.where(lane >= LANES - width, last, 0.0))


def before_kernel(flags, own, zown, ylo, zlo, yhi, zhi, kap, diag, inv, xout, rout, coarse, to_left, to_right, va, wa, vb, wb, res, acc, flat):
    rows = own.shape[1]
    tiles = own.shape[2]
    x_count = own.shape[3]
    inner = slice(PAD, PAD + x_count)
    last = HALO + rows
    zero_pads((kap, va, wa, vb, wb))

    def fill(j, k, b, z, y, there):
        left = jnp.where((flags[0] > 0) & there, z[0], 0.0)
        right = jnp.where((flags[1] > 0) & there, z[1], 0.0)
        kap[j, 0:tiles, inner, :] = jnp.where(there, SCALE * k, 0.0)
        kap[j, tiles, inner, :] = SCALE * unpack(left, right, y, EDGE)
        if b is not None:
            res[j, 0:tiles] = b
            res[j, tiles] = unpack(z[0], z[1], rows + y, EDGE)

    for y in range(rows):
        fill(HALO + y, own[0, y], own[1, y], zown, y, flags[4] > 0)
    for j in range(HALO):
        b = ylo[HALO + j - 1] if j else None
        fill(j, ylo[j], b, zlo, rows - HALO + j, flags[2] > 0)
        b = yhi[HALO + j] if j < HALO - 1 else None
        fill(last + j, yhi[j], b, zhi, j, flags[3] > 0)
    make_diagonal(kap, diag, inv, 1, last + HALO - 1)
    centre, weights = chebyshev_coefs(DEGREE, smooth_low)
    first_update(kap, inv, res, va, wa, acc, 1, last + HALO - 1, 1.0 / centre, False, (HALO, last, tiles))
    old, new = (va, wa), (vb, wb)
    lo, hi = 2, last + HALO - 2
    for pair in weights:
        smoothing_step(kap, diag, inv, res, old, new, acc, lo, hi, pair, (HALO, last, tiles))
        old, new = new, old
        lo, hi = lo + 1, hi - 1
    residual_only(kap, diag, res, old[0], old[1], HALO, last)
    pieces = []
    for y in range(rows):
        xout[y] = acc[HALO + y, 0:tiles]
        rout[y] = res[HALO + y, 0:tiles]
    for source, offset in ((kap, PAD), (res, 0)):
        for y in range(0, rows, 2):
            both = (
                source[HALO + y, 0:tiles, offset : offset + x_count, :]
                + source[HALO + y + 1, 0:tiles, offset : offset + x_count, :]
            )
            pieces.append(along_lanes(both))
    flat[...] = product(jnp.concatenate(pieces, axis=0), halving(tiles * LANES))
    total = flat.shape[0]
    coarse[...] = flat[pl.ds(0, total // 2, stride=2), :] + flat[pl.ds(1, total // 2, stride=2), :]
    each, xc = rows // 2, x_count // 2
    for out, from_end in ((to_left, False), (to_right, True)):
        for i in range(2):
            value = [coarse[(i * each + y) * xc : (i * each + y + 1) * xc, :] for y in range(each)]
            out[i * xc : (i + 1) * xc, :] = pack(value, COARSE_EDGE, from_end)
        value = [res[HALO + y, tiles - 1 if from_end else 0] for y in range(rows)]
        out[2 * xc : 2 * xc + x_count, :] = pack(value, EDGE, from_end)


def after_kernel(places, *refs, count):
    blocks, zblocks = refs[:count], refs[count : 2 * count]
    refs = refs[2 * count :]
    (kap, diag, inv, xpre, rown, zown, rlo, zlo, rhi, zhi, sol, resid) = refs[:12]
    (k1, d1, i1, r1, x1, va1, wa1, vb1, wb1, k2, d2, i2, r2, x2, va2, wa2, vb2, wb2, flat, va, wa, vb, wb, res, acc) = refs[12:]
    me_x, me_y = places[0], places[1]
    zero_pads((k1, va1, wa1, vb1, wb1, k2, va2, wa2, vb2, wb2, va, wa, vb, wb))
    each = blocks[0].shape[1]
    xc = blocks[0].shape[2]
    tiles = xpre.shape[1]
    yc = each * count
    lo1, hi1 = COARSE_PAD, COARSE_PAD + yc
    edge = [lo1 - 1, hi1]
    for ref in (k1, va1, wa1, vb1, wb1):
        zero_rows(ref, edge)
    zero_rows(x1, list(range(lo1)) + list(range(hi1, hi1 + COARSE_PAD)))
    for number, (block, z) in enumerate(zip(blocks, zblocks)):
        at = places[4 + number] * each + COARSE_PAD
        left = jnp.where(places[2] > 0, z[0, 0], 0.0)
        right = jnp.where(places[3] > 0, z[1, 0], 0.0)
        for y in range(each):
            k1[at + y, 0, PAD : PAD + xc, :] = block[0, y] * 0.25
            k1[at + y, 1, PAD : PAD + xc, :] = unpack(left, right, y, COARSE_EDGE) * 0.25
            r1[at + y, 0] = block[1, y]
            r1[at + y, 1] = unpack(z[0, 1], z[1, 1], y, COARSE_EDGE)
    make_diagonal(k1, d1, i1, lo1, hi1)
    centre, weights = chebyshev_coefs(DEGREE, smooth_low)
    first_update(k1, i1, r1, va1, wa1, x1, lo1, hi1, 1.0 / centre, False)
    old, new = (va1, wa1), (vb1, wb1)
    for pair in weights:
        smoothing_step(k1, d1, i1, r1, old, new, x1, lo1, hi1, pair)
        old, new = new, old
    residual_only(k1, d1, r1, old[0], old[1], lo1, hi1)
    tiles1 = k1.shape[1]
    y2 = yc // 2
    half = xc // 2
    for target, source, offset, factor in ((k2, k1, PAD, 0.25), (r2, r1, 0, 1.0)):
        pieces = []
        for y in range(y2):
            a = lo1 + 2 * y
            both = source[a, :, offset : offset + xc, :] + source[a + 1, :, offset : offset + xc, :]
            pieces.append(along_lanes(both))
        flat[0 : y2 * xc, :] = product(jnp.concatenate(pieces, axis=0), halving(tiles1 * LANES))[:, 0:LANES]
        if target is k2:
            zero_rows(k2, range(y2 + 2))
        for y in range(y2):
            value = flat[pl.ds(y * xc, half, stride=2), :] + flat[pl.ds(y * xc + 1, half, stride=2), :]
            if target is k2:
                k2[1 + y, 0, PAD : PAD + half, :] = value * factor
            else:
                r2[1 + y] = jnp.zeros(r2.shape[1:], F32)
                r2[1 + y, 0, 0:half, :] = value
    for ref in (va2, wa2, vb2, wb2):
        zero_rows(ref, [0, y2 + 1])
    make_diagonal(k2, d2, i2, 1, 1 + y2)
    centre, weights = chebyshev_coefs(COARSE_DEGREE, coarse_low)
    first_update(k2, i2, r2, va2, wa2, x2, 1, 1 + y2, 1.0 / centre, False)
    old, new = (va2, wa2), (vb2, wb2)
    for pair in weights:
        smoothing_step(k2, d2, i2, r2, old, new, x2, 1, 1 + y2, pair)
        old, new = new, old
    for y in range(y2):
        value = x2[1 + y, 0, 0:half, :]
        flat[pl.ds(y * xc, half, stride=2), :] = value
        flat[pl.ds(y * xc + 1, half, stride=2), :] = value
    wide = product(flat[0 : y2 * xc, :], doubling(2 * LANES))
    for y in range(y2):
        for t in range(tiles1):
            value = wide[y * xc : (y + 1) * xc, t * LANES : (t + 1) * LANES]
            for s in (0, 1):
                at = lo1 + 2 * y + s
                va1[at, t, PAD : PAD + xc, :] = value
                x1[at, t] = x1[at, t] + value
    times(k1, va1, wa1, lo1, hi1)
    centre, weights = chebyshev_coefs(DEGREE, smooth_low)
    residual_only(k1, d1, r1, va1, wa1, lo1, hi1)
    first_update(k1, i1, r1, va1, wa1, x1, lo1, hi1, 1.0 / centre, True)
    old, new = (va1, wa1), (vb1, wb1)
    for pair in weights:
        smoothing_step(k1, d1, i1, r1, old, new, x1, lo1, hi1, pair)
        old, new = new, old
    rows = rown.shape[0]
    last = HALO + rows
    x_count = rown.shape[2]
    wide_rows = (rows + 2 * HALO) // 2 + 1
    start = COARSE_PAD - (HALO + 1) // 2 + each * me_y
    for t in range(tiles1):
        for y in range(wide_rows):
            value = x1[start + y, t]
            base = (t * wide_rows + y) * x_count
            flat[pl.ds(base, xc, stride=2), :] = value
            flat[pl.ds(base + 1, xc, stride=2), :] = value
    n = wide_rows * x_count
    parts = []
    for t in range(tiles1 - 1):
        both = product(flat[t * n : (t + 1) * n, :], doubling(2 * LANES))
        parts += [both[:, 0:LANES], both[:, LANES:]]
    parts.append(product(flat[(tiles1 - 1) * n : tiles1 * n, :], halo_doubling()))
    own_tiles = len(parts) - 1
    for j in range(rows + 2 * HALO):
        y = (j + 1) // 2
        for t, part in enumerate(parts):
            value = part[y * x_count : (y + 1) * x_count, :]
            va[j, t, PAD : PAD + x_count, :] = value
            if HALO <= j < last and t < own_tiles:
                acc[j, t] = xpre[j - HALO, t] + value
    times(kap, va, wa, 0, rows + 2 * HALO)

    edge = HALO - 1
    for j in range(-edge, rows + edge):
        if j < 0:
            source, z, i, y = rlo, zlo, edge + j, rows + j
        elif j < rows:
            source, z, i, y = rown, zown, j, j
        else:
            source, z, i, y = rhi, zhi, j - rows, j - rows
        res[HALO + j, 0:tiles] = source[i]
        res[HALO + j, tiles] = unpack(z[0], z[1], y, EDGE)
    residual_only(kap, diag, res, va, wa, 1, last + HALO - 1)
    first_update(kap, inv, res, va, wa, acc, 1, last + HALO - 1, 1.0 / centre, True, (HALO, last, tiles))
    old, new = (va, wa), (vb, wb)
    lo, hi = 2, last + HALO - 2
    for pair in weights:
        smoothing_step(kap, diag, inv, res, old, new, acc, lo, hi, pair, (HALO, last, tiles))
        old, new = new, old
        lo, hi = lo + 1, hi - 1
    residual_only(kap, diag, res, old[0], old[1], HALO, last)
    block_x = sol.shape[0]
    first = pl.multiple_of(me_x * block_x, 8)
    for y in range(rows):
        for t in range(own_tiles):
            lanes = slice(t * LANES, (t + 1) * LANES)
            sol[:, y, lanes] = acc[HALO + y, t, pl.ds(first, block_x), :]
            resid[:, y, lanes] = res[HALO + y, t, pl.ds(first, block_x), :]


def ring(values, axis, step):
    count = lax.axis_size(axis)
    return lax.ppermute(values, axis, [(i, (i + step) % count) for i in range(count)])


def exchange(to_low, to_high, axis, across=None):
    count = lax.axis_size(axis)
    if count % 2:
        return ring(to_high, axis, 1), ring(to_low, axis, -1)
    odd = lax.axis_index(axis) % 2 == 1
    inner = [i + 1 if i % 2 else i - 1 for i in range(count)]
    one = lax.ppermute(jnp.where(odd, to_low, to_high), axis, [(i, i ^ 1) for i in range(count)])
    names, pairs = axis, [(i, t % count) for i, t in enumerate(inner)]
    if across is not None and lax.axis_size(across) % 2 == 0:
        names = (across, axis)
        pairs = [
            (x * count + i, x * count + t if 0 <= t < count else (x ^ 1) * count + i)
            for x in range(lax.axis_size(across))
            for i, t in enumerate(inner)
        ]
    two = lax.ppermute(jnp.where(odd, to_high, to_low), names, pairs)
    return jnp.where(odd, one, two), jnp.where(odd, two, one)


def exchange_and_gather(to_low, to_high):
    nx, nz = lax.axis_size("gx"), lax.axis_size("gz")
    if nx != 2 or nz % 2:
        return gather_first(jnp.stack(exchange(to_low, to_high, "gz")), "gx", 1)
    odd = lax.axis_index("gz") % 2 == 1
    out = []
    for payload, step in (
        (jnp.where(odd, to_low, to_high), [i ^ 1 for i in range(nz)]),
        (jnp.where(odd, to_high, to_low), [(i + 1 if i % 2 else i - 1) % nz for i in range(nz)]),
    ):
        same = lax.ppermute(payload, "gz", list(enumerate(step)))
        pairs = [(x * nz + i, (1 - x) * nz + t) for x in (0, 1) for i, t in enumerate(step)]
        cross = lax.ppermute(payload, ("gx", "gz"), pairs)
        first = lax.axis_index("gx") == 0
        out.append(jnp.concatenate([jnp.where(first, same, cross), jnp.where(first, cross, same)], axis=0))
    one, two = out
    return jnp.stack([jnp.where(odd, one, two), jnp.where(odd, two, one)])


def gather_first(values, axis, dim):
    count = lax.axis_size(axis)
    if count == 1:
        return values
    if count == 2:
        other = lax.ppermute(values, axis, [(0, 1), (1, 0)])
        first = lax.axis_index(axis) == 0
        return jnp.concatenate(
            [jnp.where(first, values, other), jnp.where(first, other, values)], axis=dim
        )
    every = lax.all_gather(values, axis)
    return jnp.concatenate([every[i] for i in range(count)], axis=dim)


def gather_second(block, low_edge, high_edge, me, count):
    size = block.shape[0]
    blocks, sources = [block], [me]
    low = high = low_edge
    if count == 4:
        odd = me % 2 == 1
        got = []
        for step in (1, 2, 3):
            payload = block
            if step != 2:
                edge = jnp.where(odd == (step == 1), low_edge, high_edge)
                payload = jnp.concatenate([block, edge], axis=0)
            got.append(lax.ppermute(payload, "gy", [(i, i ^ step) for i in range(count)]))
            blocks.append(got[-1][:size])
            sources.append(me ^ step)
        low = jnp.where(odd, got[0][size:], got[2][size:])
        high = jnp.where(odd, got[2][size:], got[0][size:])
    else:
        for step in range(1, count):
            parts = [block]
            if step == 1:
                parts.append(high_edge)
            if step == count - 1:
                parts.append(low_edge)
            got = ring(jnp.concatenate(parts, axis=0), "gy", step)
            blocks.append(got[:size])
            sources.append((me - step) % count)
            if step == 1:
                low = got[size : size + high_edge.shape[0]]
            if step == count - 1:
                high = got[got.shape[0] - low_edge.shape[0] :]
    return blocks, sources, low, high


def vmem(shape):
    return pltpu.VMEM(shape, F32)


def call(kernel, out_shapes, scratch, inputs):
    limit = 4 * 2**20
    for s in scratch:
        size = 4
        for n in s.shape:
            size *= n
        limit += size
    for a in list(inputs) + list(out_shapes):
        limit += 4 * a.size if hasattr(a, "size") else 0
    limit = min(limit + 8 * 2**20, 60 * 2**20)
    whole = pl.BlockSpec(memory_space=pltpu.VMEM)
    return pl.pallas_call(
        kernel,
        out_shape=out_shapes,
        in_specs=[pl.BlockSpec(memory_space=pltpu.SMEM)] + [whole] * (len(inputs) - 1),
        out_specs=[whole] * len(out_shapes),
        scratch_shapes=scratch,
        compiler_params=pltpu.CompilerParams(vmem_limit_bytes=limit),
    )(*inputs)


def body(conductivity, source):
    bx, by, bz = conductivity.shape
    tiles = bz // LANES
    nx, ny, nz = (lax.axis_size(a) for a in ("gx", "gy", "gz"))
    ix, iy, iz = (lax.axis_index(a) for a in ("gx", "gy", "gz"))
    yes = ix >= 0
    flags = jnp.stack([iz > 0, iz < nz - 1, iy > 0, iy < ny - 1, yes]).astype(jnp.int32)
    x_count = bx * nx

    def shape(*dims):
        return jax.ShapeDtypeStruct(dims, F32)

    def lines(*arrays):
        return jnp.concatenate([a.reshape(-1, LANES) for a in arrays], axis=0)

    mine = jnp.stack([conductivity, source]).reshape(2, bx, by, tiles, LANES).transpose(0, 2, 3, 1, 4)
    first_edge = jnp.concatenate([mine[a, y, 0, :, :EDGE] for a in (0, 1) for y in range(by)], axis=-1)
    last_edge = jnp.concatenate(
        [mine[a, y, tiles - 1, :, LANES - EDGE :] for a in (0, 1) for y in range(by)], axis=-1
    )
    own = gather_first(mine, "gx", 3)
    zown = exchange_and_gather(first_edge, last_edge)
    edge = HALO - 1
    low_rows = lines(own[0, :HALO], own[1, :edge], zown)
    high_rows = lines(own[0, by - HALO :], own[1, by - edge :], zown)
    from_low, from_high = exchange(low_rows, high_rows, "gy", "gx")
    cut = (HALO + edge) * tiles * x_count
    rows_shape = (HALO + edge, tiles, x_count, LANES)
    ylo, zlo = from_low[:cut].reshape(rows_shape), from_low[cut:].reshape(zown.shape)
    yhi, zhi = from_high[:cut].reshape(rows_shape), from_high[cut:].reshape(zown.shape)

    ext = by + 2 * HALO
    padded = x_count + 2 * PAD
    wide = (ext, tiles + 1, padded, LANES)
    plain = (ext, tiles + 1, x_count, LANES)
    each = by // 2
    xc = x_count // 2
    kap, diag, inv, xpre, rpre, coarse, to_left, to_right = call(
        before_kernel,
        [
            shape(*wide),
            shape(*plain),
            shape(*plain),
            shape(by, tiles, x_count, LANES),
            shape(by, tiles, x_count, LANES),
            shape(2 * each * xc, LANES),
            shape(2 * xc + x_count, LANES),
            shape(2 * xc + x_count, LANES),
        ],
        [vmem(wide)] * 4 + [vmem(plain)] * 2 + [vmem((2 * each * x_count, LANES))],
        [flags, own, zown, ylo, zlo, yhi, zhi],
    )

    left, right = exchange(to_left, to_right, "gz")
    coarse_z = jnp.stack([left[: 2 * xc], right[: 2 * xc]])
    fine_z = jnp.stack([left[2 * xc :], right[2 * xc :]])
    blocks, sources, low, high = gather_second(
        lines(coarse, coarse_z), lines(rpre[:edge], fine_z), lines(rpre[by - edge :], fine_z), iy, ny
    )
    cut = 2 * each * xc
    zblocks = [b[cut:].reshape(2, 2, xc, LANES) for b in blocks]
    blocks = [b[:cut].reshape(2, each, xc, LANES) for b in blocks]
    cut = edge * tiles * x_count
    rows_shape = (edge, tiles, x_count, LANES)
    rlo, zrlo = low[:cut].reshape(rows_shape), low[cut:].reshape(fine_z.shape)
    rhi, zrhi = high[:cut].reshape(rows_shape), high[cut:].reshape(fine_z.shape)

    yc = each * ny
    tiles1 = tiles // 2 + 1
    wide1 = (yc + 2 * COARSE_PAD, tiles1, xc + 2 * PAD, LANES)
    plain1 = (yc + 2 * COARSE_PAD, tiles1, xc, LANES)
    y2 = yc // 2
    x2 = max(xc // 2, 8)
    wide2 = (y2 + 2, 1, x2 + 2 * PAD, LANES)
    plain2 = (y2 + 2, 1, x2, LANES)
    flat_rows = max(y2 * xc, tiles1 * (ext // 2 + 1) * x_count)

    places = jnp.stack([jnp.int32(p) for p in (ix, iy, iz > 0, iz < nz - 1, *sources)])

    def kernel(*refs):
        after_kernel(*refs, count=len(blocks))

    sol, resid = call(
        kernel,
        [shape(bx, by, bz), shape(bx, by, bz)],
        [vmem(wide1)] + [vmem(plain1)] * 4 + [vmem(wide1)] * 4
        + [vmem(wide2)] + [vmem(plain2)] * 4 + [vmem(wide2)] * 4
        + [vmem((flat_rows, LANES))] + [vmem(wide)] * 4 + [vmem(plain)] * 2,
        [places] + blocks + zblocks
        + [kap, diag, inv, xpre, rpre, fine_z, rlo, zrlo, rhi, zrhi],
    )
    return sol, resid


def solution(mesh):
    spec = P("gx", "gy", "gz")
    return jax.shard_map(body, mesh=mesh, in_specs=(spec, spec), out_specs=(spec, spec), check_vma=False)
```

```python
import jax
import jax.numpy as jnp
from jax import lax
from jax.experimental import pallas as pl
from jax.experimental.pallas import tpu as pltpu
from jax.sharding import PartitionSpec as P


DEGREE = 4
COARSE_DEGREE = 8
smooth_low = 0.5
coarse_low = 0.03
upper_bound = 2.0

F32 = jnp.float32
LANES = 128
PAD = 8
HALO = 5
COARSE_PAD = 4
FACE = 14.0 / 3.0
CORNER = 1.0 / 3.0
TOTAL = 128.0 / 3.0
SCALE = 0.05


def chebyshev_coefs(degree, lower):
    centre = (upper_bound + lower) / 2.0
    half_width = (upper_bound - lower) / 2.0
    ratio_term = centre / half_width
    rho_prev = 1.0 / ratio_term
    weights = []
    for _ in range(1, degree):
        rho_next = 1.0 / (2.0 * ratio_term - rho_prev)
        weights.append((rho_next * rho_prev, 2.0 * rho_next / half_width))
        rho_prev = rho_next
    return centre, weights


EDGE = 8
COARSE_EDGE = 32
CHUNK = 16


def chunks(start, stop, body):
    count = stop - start
    full = count // CHUNK
    if full == 1:
        body(start, CHUNK)
    elif full > 1:

        def step(i, carry):
            body(start + i * CHUNK, CHUNK)
            return carry

        lax.fori_loop(0, full, step, 0)
    if count % CHUNK:
        body(start + full * CHUNK, count % CHUNK)


def loop(start, stop, body):
    def group(first, rows):
        for i in range(rows):
            body(first + i)

    chunks(start, stop, group)


def third_pairs(values):
    tiles, rows, _ = values.shape
    flat = values.reshape(tiles * rows, LANES)
    up = pltpu.roll(flat, 1, 1).reshape(tiles, rows, LANES)
    down = pltpu.roll(flat, LANES - 1, 1).reshape(tiles, rows, LANES)
    if tiles > 1:
        lane = lax.broadcasted_iota(jnp.int32, (tiles, rows, LANES), 2)
        up_other = jnp.concatenate([up[tiles - 1 :], up[: tiles - 1]], axis=0)
        down_other = jnp.concatenate([down[1:], down[:1]], axis=0)
        up = jnp.where(lane == 0, up_other, up)
        down = jnp.where(lane == LANES - 1, down_other, down)
    return up + down


def neighbour_sums(ref, first, rows, row):
    at = range(first - 1, first + rows + 1) if isinstance(first, int) else [first + i for i in range(-1, rows + 1)]
    centre = [ref[y, :, row : row + 8, :] for y in at]
    side = [ref[y, :, row - 1 : row + 7, :] + ref[y, :, row + 1 : row + 9, :] for y in at]
    out = []
    for i in range(1, rows + 1):
        corner = side[i - 1] + side[i + 1]
        face = (centre[i - 1] + centre[i + 1]) + side[i]
        plane = FACE * face + corner
        beside = FACE * centre[i] + face + CORNER * corner
        out.append((plane + third_pairs(beside), centre[i]))
    return out


def zero_pads(refs):
    for ref in refs:
        count, tiles, rows, _ = ref.shape
        zero = jnp.zeros((tiles, PAD, LANES), F32)

        def body(y, ref=ref, rows=rows, zero=zero):
            ref[y, :, 0:PAD, :] = zero
            ref[y, :, rows - PAD : rows, :] = zero

        loop(0, count, body)


def zero_rows(ref, rows):
    zero = jnp.zeros(ref.shape[1:], F32)
    for y in rows:
        ref[y] = zero


def tiles_of(ref):
    return range(0, ref.shape[2], 8)


def make_diagonal(kap, diag, inv, lo, hi):
    def body(first, rows):
        for x in tiles_of(diag):
            for i, (total, centre) in enumerate(neighbour_sums(kap, first, rows, PAD + x)):
                value = TOTAL * centre + total
                diag[first + i, :, x : x + 8, :] = value
                inv[first + i, :, x : x + 8, :] = jnp.where(centre > 0.0, 1.0 / value, 0.0)

    chunks(lo, hi, body)


def accumulate(acc, y, x, step, add, own):
    tiles = step.shape[0]
    if own is not None:
        if isinstance(y, int) and not own[0] <= y < own[1]:
            return
        tiles = own[2]
    step = step[0:tiles]
    acc[y, 0:tiles, x : x + 8, :] = acc[y, 0:tiles, x : x + 8, :] + step if add else step


def first_update(kap, inv, res, v, w, acc, lo, hi, scale, add, own=None):
    def body(y):
        for x in tiles_of(inv):
            step = (inv[y, :, x : x + 8, :] * scale) * res[y, :, x : x + 8, :]
            v[y, :, PAD + x : PAD + x + 8, :] = step
            w[y, :, PAD + x : PAD + x + 8, :] = kap[y, :, PAD + x : PAD + x + 8, :] * step
            accumulate(acc, y, x, step, add, own)

    loop(lo, hi, body)


def times(kap, v, w, lo, hi):
    def body(y):
        w[y] = kap[y] * v[y]

    loop(lo, hi, body)


def new_residuals(kap, diag, res, v, w, first, rows, x):
    total = neighbour_sums(v, first, rows, PAD + x)
    weighted = neighbour_sums(w, first, rows, PAD + x)
    for i in range(rows):
        y = first + i
        k = kap[y, :, PAD + x : PAD + x + 8, :]
        centre = total[i][1]
        value = (
            res[y, :, x : x + 8, :]
            - diag[y, :, x : x + 8, :] * centre
            + (k * total[i][0] + weighted[i][0])
        )
        yield y, k, centre, value


def residual_only(kap, diag, res, v, w, lo, hi):
    def body(first, rows):
        for x in tiles_of(diag):
            for y, _, _, value in new_residuals(kap, diag, res, v, w, first, rows, x):
                res[y, :, x : x + 8, :] = value

    chunks(lo, hi, body)


def smoothing_step(kap, diag, inv, res, old, new, acc, lo, hi, pair, own=None):
    def body(first, rows):
        for x in tiles_of(diag):
            for y, k, centre, value in new_residuals(kap, diag, res, old[0], old[1], first, rows, x):
                res[y, :, x : x + 8, :] = value
                step = pair[0] * centre + (pair[1] * inv[y, :, x : x + 8, :]) * value
                new[0][y, :, PAD + x : PAD + x + 8, :] = step
                new[1][y, :, PAD + x : PAD + x + 8, :] = k * step
                accumulate(acc, y, x, step, True, own)

    chunks(lo, hi, body)


def lanes_of(values):
    return lax.broadcasted_iota(jnp.int32, values.shape, 1)


def take(values, index):
    return jnp.take_along_axis(values, index, axis=1, mode="promise_in_bounds")


def halve(first, second):
    lane = lanes_of(first)
    even = (2 * lane) % LANES
    low = take(first + pltpu.roll(first, LANES - 1, 1), even)
    high = take(second + pltpu.roll(second, LANES - 1, 1), even)
    return jnp.where(lane < LANES // 2, low, high) * 0.125


def double(values):
    half = lanes_of(values) // 2
    return take(values, half), take(values, half + LANES // 2)


def double_halo(values):
    lane = lanes_of(values)
    return take(values, lane // 2 + jnp.where(lane < LANES // 2, 0, LANES // 2))


def pack(pieces, width, from_end, start=0):
    lane = lax.broadcasted_iota(jnp.int32, pieces[0].shape, 1)
    out = jnp.zeros(pieces[0].shape, F32)
    for i, piece in enumerate(pieces, start):
        shift = (width * i + (width if from_end else 0)) % LANES
        moved = pltpu.roll(piece, shift, 1) if shift else piece
        out = jnp.where((lane >= width * i) & (lane < width * (i + 1)), moved, out)
    return out


def unpack(left, right, i, width, start=0):
    lane = lax.broadcasted_iota(jnp.int32, left.shape, 1)
    back = (LANES - width * i) % LANES
    end = (LANES - width - width * (i + start)) % LANES
    first = pltpu.roll(right, back, 1) if back else right
    last = pltpu.roll(left, end, 1) if end else left
    return jnp.where(lane < width, first, jnp.where(lane >= LANES - width, last, 0.0))


def before_kernel(flags, own, zown, ylo, zlo, yhi, zhi, kap, diag, inv, xout, rout, coarse, to_left, to_right, va, wa, vb, wb, res, acc, flat):
    rows = own.shape[1]
    tiles = own.shape[2]
    x_count = own.shape[3]
    inner = slice(PAD, PAD + x_count)
    last = HALO + rows
    zero_pads((kap, va, wa, vb, wb))

    def fill(j, k, b, z, y, there):
        left = jnp.where((flags[0] > 0) & there, z[0], 0.0)
        right = jnp.where((flags[1] > 0) & there, z[1], 0.0)
        kap[j, 0:tiles, inner, :] = jnp.where(there, SCALE * k, 0.0)
        kap[j, tiles, inner, :] = SCALE * unpack(left, right, y, EDGE)
        if b is not None:
            res[j, 0:tiles] = b
            res[j, tiles] = unpack(z[0], z[1], rows + y, EDGE)

    for y in range(rows):
        fill(HALO + y, own[0, y], own[1, y], zown, y, flags[4] > 0)
    for j in range(HALO):
        b = ylo[HALO + j - 1] if j else None
        fill(j, ylo[j], b, zlo, rows - HALO + j, flags[2] > 0)
        b = yhi[HALO + j] if j < HALO - 1 else None
        fill(last + j, yhi[j], b, zhi, j, flags[3] > 0)
    make_diagonal(kap, diag, inv, 1, last + HALO - 1)
    centre, weights = chebyshev_coefs(DEGREE, smooth_low)
    first_update(kap, inv, res, va, wa, acc, 1, last + HALO - 1, 1.0 / centre, False, (HALO, last, tiles))
    old, new = (va, wa), (vb, wb)
    lo, hi = 2, last + HALO - 2
    for pair in weights:
        smoothing_step(kap, diag, inv, res, old, new, acc, lo, hi, pair, (HALO, last, tiles))
        old, new = new, old
        lo, hi = lo + 1, hi - 1
    residual_only(kap, diag, res, old[0], old[1], HALO, last)
    at = 0
    for y in range(rows):
        xout[y] = acc[HALO + y, 0:tiles]
        rout[y] = res[HALO + y, 0:tiles]
    for source, offset in ((kap, PAD), (res, 0)):
        for y in range(0, rows, 2):
            both = (
                source[HALO + y, 0:tiles, offset : offset + x_count, :]
                + source[HALO + y + 1, 0:tiles, offset : offset + x_count, :]
            )
            flat[at : at + x_count, :] = halve(both[0], both[1])
            at += x_count
    total = flat.shape[0]
    coarse[...] = flat[pl.ds(0, total // 2, stride=2), :] + flat[pl.ds(1, total // 2, stride=2), :]
    each, xc = rows // 2, x_count // 2
    for out, from_end in ((to_left, False), (to_right, True)):
        for i in range(2):
            value = [coarse[(i * each + y) * xc : (i * each + y + 1) * xc, :] for y in range(each)]
            out[i * xc : (i + 1) * xc, :] = pack(value, COARSE_EDGE, from_end)
        value = [res[HALO + y, tiles - 1 if from_end else 0] for y in range(rows)]
        out[2 * xc : 2 * xc + x_count, :] = pack(value, EDGE, from_end, rows if from_end else 0)


def after_kernel(places, *refs, count):
    blocks, zblocks = refs[:count], refs[count : 2 * count]
    refs = refs[2 * count :]
    (kap, diag, inv, xpre, rown, zown, rlo, zlo, rhi, zhi, sol, resid) = refs[:12]
    (k1, d1, i1, r1, x1, va1, wa1, vb1, wb1, k2, d2, i2, r2, x2, va2, wa2, vb2, wb2, flat, va, wa, vb, wb, res, acc) = refs[12:]
    me_x, me_y = places[0], places[1]
    zero_pads((k1, va1, wa1, vb1, wb1, k2, va2, wa2, vb2, wb2, va, wa, vb, wb))
    each = blocks[0].shape[1]
    xc = blocks[0].shape[2]
    tiles = xpre.shape[1]
    yc = each * count
    lo1, hi1 = COARSE_PAD, COARSE_PAD + yc
    edge = [lo1 - 1, hi1]
    for ref in (k1, va1, wa1, vb1, wb1):
        zero_rows(ref, edge)
    zero_rows(x1, list(range(lo1)) + list(range(hi1, hi1 + COARSE_PAD)))
    for number, (block, z) in enumerate(zip(blocks, zblocks)):
        at = places[4 + number] * each + COARSE_PAD
        left = jnp.where(places[2] > 0, z[0, 0], 0.0)
        right = jnp.where(places[3] > 0, z[1, 0], 0.0)
        for y in range(each):
            k1[at + y, 0, PAD : PAD + xc, :] = block[0, y] * 0.25
            k1[at + y, 1, PAD : PAD + xc, :] = unpack(left, right, y, COARSE_EDGE) * 0.25
            r1[at + y, 0] = block[1, y]
            r1[at + y, 1] = unpack(z[0, 1], z[1, 1], y, COARSE_EDGE)
    make_diagonal(k1, d1, i1, lo1, hi1)
    centre, weights = chebyshev_coefs(DEGREE, smooth_low)
    first_update(k1, i1, r1, va1, wa1, x1, lo1, hi1, 1.0 / centre, False)
    old, new = (va1, wa1), (vb1, wb1)
    for pair in weights:
        smoothing_step(k1, d1, i1, r1, old, new, x1, lo1, hi1, pair)
        old, new = new, old
    residual_only(k1, d1, r1, old[0], old[1], lo1, hi1)
    tiles1 = k1.shape[1]
    y2 = yc // 2
    half = xc // 2
    for target, source, offset, factor in ((k2, k1, PAD, 0.25), (r2, r1, 0, 1.0)):
        for y in range(y2):
            a = lo1 + 2 * y
            both = source[a, :, offset : offset + xc, :] + source[a + 1, :, offset : offset + xc, :]
            flat[y * xc : (y + 1) * xc, :] = halve(both[0], both[1])
        if target is k2:
            zero_rows(k2, range(y2 + 2))
        for y in range(y2):
            value = flat[pl.ds(y * xc, half, stride=2), :] + flat[pl.ds(y * xc + 1, half, stride=2), :]
            if target is k2:
                k2[1 + y, 0, PAD : PAD + half, :] = value * factor
            else:
                r2[1 + y] = jnp.zeros(r2.shape[1:], F32)
                r2[1 + y, 0, 0:half, :] = value
    for ref in (va2, wa2, vb2, wb2):
        zero_rows(ref, [0, y2 + 1])
    make_diagonal(k2, d2, i2, 1, 1 + y2)
    centre, weights = chebyshev_coefs(COARSE_DEGREE, coarse_low)
    first_update(k2, i2, r2, va2, wa2, x2, 1, 1 + y2, 1.0 / centre, False)
    old, new = (va2, wa2), (vb2, wb2)
    for pair in weights:
        smoothing_step(k2, d2, i2, r2, old, new, x2, 1, 1 + y2, pair)
        old, new = new, old
    for y in range(y2):
        value = x2[1 + y, 0, 0:half, :]
        flat[pl.ds(y * xc, half, stride=2), :] = value
        flat[pl.ds(y * xc + 1, half, stride=2), :] = value
    for y in range(y2):
        for t, value in enumerate(double(flat[y * xc : (y + 1) * xc, :])):
            for s in (0, 1):
                at = lo1 + 2 * y + s
                va1[at, t, PAD : PAD + xc, :] = value
                x1[at, t] = x1[at, t] + value
    times(k1, va1, wa1, lo1, hi1)
    centre, weights = chebyshev_coefs(DEGREE, smooth_low)
    residual_only(k1, d1, r1, va1, wa1, lo1, hi1)
    first_update(k1, i1, r1, va1, wa1, x1, lo1, hi1, 1.0 / centre, True)
    old, new = (va1, wa1), (vb1, wb1)
    for pair in weights:
        smoothing_step(k1, d1, i1, r1, old, new, x1, lo1, hi1, pair)
        old, new = new, old
    rows = rown.shape[0]
    last = HALO + rows
    x_count = rown.shape[2]
    wide_rows = (rows + 2 * HALO) // 2 + 1
    start = COARSE_PAD - (HALO + 1) // 2 + each * me_y
    for t in range(tiles1):
        for y in range(wide_rows):
            value = x1[start + y, t]
            base = (t * wide_rows + y) * x_count
            flat[pl.ds(base, xc, stride=2), :] = value
            flat[pl.ds(base + 1, xc, stride=2), :] = value
    inner = slice(PAD, PAD + x_count)
    for y in range(wide_rows):
        parts = []
        for t in range(tiles1):
            at = (t * wide_rows + y) * x_count
            value = flat[at : at + x_count, :]
            parts += double(value) if t < tiles1 - 1 else [double_halo(value)]
        for j in (2 * y - 1, 2 * y):
            if not 0 <= j < rows + 2 * HALO:
                continue
            for t, value in enumerate(parts):
                va[j, t, inner, :] = value
                wa[j, t, inner, :] = kap[j, t, inner, :] * value
                if HALO <= j < last and t < tiles:
                    acc[j, t] = xpre[j - HALO, t] + value

    edge = HALO - 1
    for j in range(-edge, rows + edge):
        if j < 0:
            source, z, i, y = rlo, zlo, edge + j, rows + j
        elif j < rows:
            source, z, i, y = rown, zown, j, j
        else:
            source, z, i, y = rhi, zhi, j - rows, j - rows
        res[HALO + j, 0:tiles] = source[i]
        packed = z[...]
        res[HALO + j, tiles] = unpack(packed, packed, y, EDGE, rows)
    residual_only(kap, diag, res, va, wa, 1, last + HALO - 1)
    first_update(kap, inv, res, va, wa, acc, 1, last + HALO - 1, 1.0 / centre, True, (HALO, last, tiles))
    old, new = (va, wa), (vb, wb)
    lo, hi = 2, last + HALO - 2
    for pair in weights:
        smoothing_step(kap, diag, inv, res, old, new, acc, lo, hi, pair, (HALO, last, tiles))
        old, new = new, old
        lo, hi = lo + 1, hi - 1
    block_x = sol.shape[0]
    for x in range(0, x_count, 8):

        @pl.when(me_x == x // block_x)
        def _(x=x):
            values = new_residuals(kap, diag, res, old[0], old[1], HALO, rows, x)
            for y, (_, _, _, value) in enumerate(values):
                for t in range(tiles):
                    lanes = slice(t * LANES, (t + 1) * LANES)
                    at = slice(x % block_x, x % block_x + 8)
                    sol[at, y, lanes] = acc[HALO + y, t, x : x + 8, :]
                    resid[at, y, lanes] = value[t]


def ring(values, axis, step):
    count = lax.axis_size(axis)
    return lax.ppermute(values, axis, [(i, (i + step) % count) for i in range(count)])


def exchange(to_low, to_high, axis, across=None):
    count = lax.axis_size(axis)
    if count % 2:
        return ring(to_high, axis, 1), ring(to_low, axis, -1)
    odd = lax.axis_index(axis) % 2 == 1
    inner = [i + 1 if i % 2 else i - 1 for i in range(count)]
    one = lax.ppermute(jnp.where(odd, to_low, to_high), axis, [(i, i ^ 1) for i in range(count)])
    names, pairs = axis, [(i, t % count) for i, t in enumerate(inner)]
    if across is not None and lax.axis_size(across) % 2 == 0:
        names = (across, axis)
        pairs = [
            (x * count + i, x * count + t if 0 <= t < count else (x ^ 1) * count + i)
            for x in range(lax.axis_size(across))
            for i, t in enumerate(inner)
        ]
    two = lax.ppermute(jnp.where(odd, to_high, to_low), names, pairs)
    return jnp.where(odd, one, two), jnp.where(odd, two, one)


def exchange_and_gather(to_low, to_high):
    nx, nz = lax.axis_size("gx"), lax.axis_size("gz")
    if nx != 2 or nz % 2:
        return gather_first(jnp.stack(exchange(to_low, to_high, "gz")), "gx", 1)
    odd = lax.axis_index("gz") % 2 == 1
    out = []
    for payload, step in (
        (jnp.where(odd, to_low, to_high), [i ^ 1 for i in range(nz)]),
        (jnp.where(odd, to_high, to_low), [(i + 1 if i % 2 else i - 1) % nz for i in range(nz)]),
    ):
        same = lax.ppermute(payload, "gz", list(enumerate(step)))
        pairs = [(x * nz + i, (1 - x) * nz + t) for x in (0, 1) for i, t in enumerate(step)]
        cross = lax.ppermute(payload, ("gx", "gz"), pairs)
        first = lax.axis_index("gx") == 0
        out.append(jnp.concatenate([jnp.where(first, same, cross), jnp.where(first, cross, same)], axis=0))
    one, two = out
    return jnp.stack([jnp.where(odd, one, two), jnp.where(odd, two, one)])


def gather_first(values, axis, dim):
    count = lax.axis_size(axis)
    if count == 1:
        return values
    if count == 2:
        other = lax.ppermute(values, axis, [(0, 1), (1, 0)])
        first = lax.axis_index(axis) == 0
        return jnp.concatenate(
            [jnp.where(first, values, other), jnp.where(first, other, values)], axis=dim
        )
    every = lax.all_gather(values, axis)
    return jnp.concatenate([every[i] for i in range(count)], axis=dim)


def gather_second(block, low_edge, high_edge, me, count):
    size = block.shape[0]
    blocks, sources = [block], [me]
    low = high = low_edge
    if count == 4:
        odd = me % 2 == 1
        got = []
        for step in (1, 2, 3):
            payload = block
            if step != 2:
                edge = jnp.where(odd == (step == 1), low_edge, high_edge)
                payload = jnp.concatenate([block, edge], axis=0)
            got.append(lax.ppermute(payload, "gy", [(i, i ^ step) for i in range(count)]))
            blocks.append(got[-1][:size])
            sources.append(me ^ step)
        low = jnp.where(odd, got[0][size:], got[2][size:])
        high = jnp.where(odd, got[2][size:], got[0][size:])
    else:
        for step in range(1, count):
            parts = [block]
            if step == 1:
                parts.append(high_edge)
            if step == count - 1:
                parts.append(low_edge)
            got = ring(jnp.concatenate(parts, axis=0), "gy", step)
            blocks.append(got[:size])
            sources.append((me - step) % count)
            if step == 1:
                low = got[size : size + high_edge.shape[0]]
            if step == count - 1:
                high = got[got.shape[0] - low_edge.shape[0] :]
    return blocks, sources, low, high


def vmem(shape):
    return pltpu.VMEM(shape, F32)


def call(kernel, out_shapes, scratch, inputs):
    limit = 4 * 2**20
    for s in scratch:
        size = 4
        for n in s.shape:
            size *= n
        limit += size
    for a in list(inputs) + list(out_shapes):
        limit += 4 * a.size if hasattr(a, "size") else 0
    limit = min(limit + 8 * 2**20, 60 * 2**20)
    whole = pl.BlockSpec(memory_space=pltpu.VMEM)
    return pl.pallas_call(
        kernel,
        out_shape=out_shapes,
        in_specs=[pl.BlockSpec(memory_space=pltpu.SMEM)] + [whole] * (len(inputs) - 1),
        out_specs=[whole] * len(out_shapes),
        scratch_shapes=scratch,
        compiler_params=pltpu.CompilerParams(vmem_limit_bytes=limit),
    )(*inputs)


def body(conductivity, source):
    bx, by, bz = conductivity.shape
    tiles = bz // LANES
    nx, ny, nz = (lax.axis_size(a) for a in ("gx", "gy", "gz"))
    ix, iy, iz = (lax.axis_index(a) for a in ("gx", "gy", "gz"))
    yes = ix >= 0
    flags = jnp.stack([iz > 0, iz < nz - 1, iy > 0, iy < ny - 1, yes]).astype(jnp.int32)
    x_count = bx * nx

    def shape(*dims):
        return jax.ShapeDtypeStruct(dims, F32)

    def lines(*arrays):
        return jnp.concatenate([a.reshape(-1, LANES) for a in arrays], axis=0)

    mine = jnp.stack([conductivity, source]).reshape(2, bx, by, tiles, LANES).transpose(0, 2, 3, 1, 4)
    first_edge = jnp.concatenate([mine[a, y, 0, :, :EDGE] for a in (0, 1) for y in range(by)], axis=-1)
    last_edge = jnp.concatenate(
        [mine[a, y, tiles - 1, :, LANES - EDGE :] for a in (0, 1) for y in range(by)], axis=-1
    )
    own = gather_first(mine, "gx", 3)
    zown = exchange_and_gather(first_edge, last_edge)
    edge = HALO - 1
    low_rows = lines(own[0, :HALO], own[1, :edge], zown)
    high_rows = lines(own[0, by - HALO :], own[1, by - edge :], zown)
    from_low, from_high = exchange(low_rows, high_rows, "gy", "gx")
    cut = (HALO + edge) * tiles * x_count
    rows_shape = (HALO + edge, tiles, x_count, LANES)
    ylo, zlo = from_low[:cut].reshape(rows_shape), from_low[cut:].reshape(zown.shape)
    yhi, zhi = from_high[:cut].reshape(rows_shape), from_high[cut:].reshape(zown.shape)

    ext = by + 2 * HALO
    padded = x_count + 2 * PAD
    wide = (ext, tiles + 1, padded, LANES)
    plain = (ext, tiles + 1, x_count, LANES)
    each = by // 2
    xc = x_count // 2
    kap, diag, inv, xpre, rpre, coarse, to_left, to_right = call(
        before_kernel,
        [
            shape(*wide),
            shape(*plain),
            shape(*plain),
            shape(by, tiles, x_count, LANES),
            shape(by, tiles, x_count, LANES),
            shape(2 * each * xc, LANES),
            shape(2 * xc + x_count, LANES),
            shape(2 * xc + x_count, LANES),
        ],
        [vmem(wide)] * 4 + [vmem(plain)] * 2 + [vmem((2 * each * x_count, LANES))],
        [flags, own, zown, ylo, zlo, yhi, zhi],
    )

    left, right = exchange(to_left, to_right, "gz")
    coarse_z = jnp.stack([left[: 2 * xc], right[: 2 * xc]])
    lane = lax.broadcasted_iota(jnp.int32, (x_count, LANES), 1)
    fine_z = jnp.where(lane < LANES // 2, right[2 * xc :], left[2 * xc :])
    blocks, sources, low, high = gather_second(
        lines(coarse, coarse_z), lines(rpre[:edge], fine_z), lines(rpre[by - edge :], fine_z), iy, ny
    )
    cut = 2 * each * xc
    zblocks = [b[cut:].reshape(2, 2, xc, LANES) for b in blocks]
    blocks = [b[:cut].reshape(2, each, xc, LANES) for b in blocks]
    cut = edge * tiles * x_count
    rows_shape = (edge, tiles, x_count, LANES)
    rlo, zrlo = low[:cut].reshape(rows_shape), low[cut:].reshape(fine_z.shape)
    rhi, zrhi = high[:cut].reshape(rows_shape), high[cut:].reshape(fine_z.shape)

    yc = each * ny
    tiles1 = tiles // 2 + 1
    wide1 = (yc + 2 * COARSE_PAD, tiles1, xc + 2 * PAD, LANES)
    plain1 = (yc + 2 * COARSE_PAD, tiles1, xc, LANES)
    y2 = yc // 2
    x2 = max(xc // 2, 8)
    wide2 = (y2 + 2, 1, x2 + 2 * PAD, LANES)
    plain2 = (y2 + 2, 1, x2, LANES)
    flat_rows = max(y2 * xc, tiles1 * (ext // 2 + 1) * x_count)

    places = jnp.stack([jnp.int32(p) for p in (ix, iy, iz > 0, iz < nz - 1, *sources)])

    def kernel(*refs):
        after_kernel(*refs, count=len(blocks))

    sol, resid = call(
        kernel,
        [shape(bx, by, bz), shape(bx, by, bz)],
        [vmem(wide1)] + [vmem(plain1)] * 4 + [vmem(wide1)] * 4
        + [vmem(wide2)] + [vmem(plain2)] * 4 + [vmem(wide2)] * 4
        + [vmem((flat_rows, LANES))] + [vmem(wide)] * 4 + [vmem(plain)] * 2,
        [places] + blocks + zblocks
        + [kap, diag, inv, xpre, rpre, fine_z, rlo, zrlo, rhi, zrhi],
    )
    return sol, resid


def solution(mesh):
    spec = P("gx", "gy", "gz")

    return jax.shard_map(body, mesh=mesh, in_specs=(spec, spec), out_specs=(spec, spec), check_vma=False)
```

```python
import jax
import jax.numpy as jnp
from jax import lax
from jax.experimental import pallas as pl
from jax.experimental.pallas import tpu as pltpu
from jax.sharding import PartitionSpec as P


DEGREE = 4
COARSE_DEGREE = 8
smooth_low = 0.5
coarse_low = 0.03
upper_bound = 2.0

F32 = jnp.float32
LANES = 128
PAD = 8
HALO = 5
COARSE_PAD = 4
FACE = 14.0 / 3.0
CORNER = 1.0 / 3.0
TOTAL = 128.0 / 3.0
SCALE = 0.05


def chebyshev_coefs(degree, lower):
    centre = (upper_bound + lower) / 2.0
    half_width = (upper_bound - lower) / 2.0
    ratio_term = centre / half_width
    rho_prev = 1.0 / ratio_term
    weights = []
    for _ in range(1, degree):
        rho_next = 1.0 / (2.0 * ratio_term - rho_prev)
        weights.append((rho_next * rho_prev, 2.0 * rho_next / half_width))
        rho_prev = rho_next
    return centre, weights


EDGE = 8
COARSE_EDGE = 32
CHUNK = 16


def chunks(start, stop, body):
    count = stop - start
    full = count // CHUNK
    if full == 1:
        body(start, CHUNK)
    elif full > 1:

        def step(i, carry):
            body(start + i * CHUNK, CHUNK)
            return carry

        lax.fori_loop(0, full, step, 0)
    if count % CHUNK:
        body(start + full * CHUNK, count % CHUNK)


def loop(start, stop, body):
    def group(first, rows):
        for i in range(rows):
            body(first + i)

    chunks(start, stop, group)


def third_pairs(values):
    tiles, rows, _ = values.shape
    flat = values.reshape(tiles * rows, LANES)
    up = pltpu.roll(flat, 1, 1).reshape(tiles, rows, LANES)
    down = pltpu.roll(flat, LANES - 1, 1).reshape(tiles, rows, LANES)
    if tiles > 1:
        lane = lax.broadcasted_iota(jnp.int32, (tiles, rows, LANES), 2)
        up_other = jnp.concatenate([up[tiles - 1 :], up[: tiles - 1]], axis=0)
        down_other = jnp.concatenate([down[1:], down[:1]], axis=0)
        up = jnp.where(lane == 0, up_other, up)
        down = jnp.where(lane == LANES - 1, down_other, down)
    return up + down


def neighbour_sums(ref, first, rows, row):
    at = range(first - 1, first + rows + 1) if isinstance(first, int) else [first + i for i in range(-1, rows + 1)]
    centre = [ref[y, :, row : row + 8, :] for y in at]
    side = [ref[y, :, row - 1 : row + 7, :] + ref[y, :, row + 1 : row + 9, :] for y in at]
    out = []
    for i in range(1, rows + 1):
        corner = side[i - 1] + side[i + 1]
        face = (centre[i - 1] + centre[i + 1]) + side[i]
        plane = FACE * face + corner
        beside = FACE * centre[i] + face + CORNER * corner
        out.append((plane + third_pairs(beside), centre[i]))
    return out


def zero_pads(refs):
    for ref in refs:
        count, tiles, rows, _ = ref.shape
        zero = jnp.zeros((tiles, PAD, LANES), F32)

        def body(y, ref=ref, rows=rows, zero=zero):
            ref[y, :, 0:PAD, :] = zero
            ref[y, :, rows - PAD : rows, :] = zero

        loop(0, count, body)


def zero_rows(ref, rows):
    zero = jnp.zeros(ref.shape[1:], F32)
    for y in rows:
        ref[y] = zero


def tiles_of(ref):
    return range(0, ref.shape[2], 8)


def make_diagonal(kap, diag, inv, lo, hi):
    def body(first, rows):
        for x in tiles_of(diag):
            for i, (total, centre) in enumerate(neighbour_sums(kap, first, rows, PAD + x)):
                value = TOTAL * centre + total
                diag[first + i, :, x : x + 8, :] = value
                inv[first + i, :, x : x + 8, :] = jnp.where(centre > 0.0, 1.0 / value, 0.0)

    chunks(lo, hi, body)


def accumulate(acc, y, x, step, add, own):
    tiles = step.shape[0]
    if own is not None:
        if isinstance(y, int) and not own[0] <= y < own[1]:
            return
        tiles = own[2]
    step = step[0:tiles]
    acc[y, 0:tiles, x : x + 8, :] = acc[y, 0:tiles, x : x + 8, :] + step if add else step


def first_update(kap, inv, res, v, w, acc, lo, hi, scale, add, own=None):
    def body(y):
        for x in tiles_of(inv):
            step = (inv[y, :, x : x + 8, :] * scale) * res[y, :, x : x + 8, :]
            v[y, :, PAD + x : PAD + x + 8, :] = step
            w[y, :, PAD + x : PAD + x + 8, :] = kap[y, :, PAD + x : PAD + x + 8, :] * step
            accumulate(acc, y, x, step, add, own)

    loop(lo, hi, body)


def times(kap, v, w, lo, hi):
    def body(y):
        w[y] = kap[y] * v[y]

    loop(lo, hi, body)


def new_residuals(kap, diag, res, v, w, first, rows, x):
    total = neighbour_sums(v, first, rows, PAD + x)
    weighted = neighbour_sums(w, first, rows, PAD + x)
    for i in range(rows):
        y = first + i
        k = kap[y, :, PAD + x : PAD + x + 8, :]
        centre = total[i][1]
        value = (
            res[y, :, x : x + 8, :]
            - diag[y, :, x : x + 8, :] * centre
            + (k * total[i][0] + weighted[i][0])
        )
        yield y, k, centre, value


def residual_only(kap, diag, res, v, w, lo, hi):
    def body(first, rows):
        for x in tiles_of(diag):
            for y, _, _, value in new_residuals(kap, diag, res, v, w, first, rows, x):
                res[y, :, x : x + 8, :] = value

    chunks(lo, hi, body)


def smoothing_step(kap, diag, inv, res, old, new, acc, lo, hi, pair, own=None):
    def body(first, rows):
        for x in tiles_of(diag):
            for y, k, centre, value in new_residuals(kap, diag, res, old[0], old[1], first, rows, x):
                res[y, :, x : x + 8, :] = value
                step = pair[0] * centre + (pair[1] * inv[y, :, x : x + 8, :]) * value
                new[0][y, :, PAD + x : PAD + x + 8, :] = step
                new[1][y, :, PAD + x : PAD + x + 8, :] = k * step
                accumulate(acc, y, x, step, True, own)

    chunks(lo, hi, body)


def lanes_of(values):
    return lax.broadcasted_iota(jnp.int32, values.shape, 1)


def take(values, index):
    return jnp.take_along_axis(values, index, axis=1, mode="promise_in_bounds")


def halve(first, second):
    lane = lanes_of(first)
    even = (2 * lane) % LANES
    low = take(first + pltpu.roll(first, LANES - 1, 1), even)
    high = take(second + pltpu.roll(second, LANES - 1, 1), even)
    return jnp.where(lane < LANES // 2, low, high) * 0.125


def double(values):
    half = lanes_of(values) // 2
    return take(values, half), take(values, half + LANES // 2)


def double_halo(values):
    lane = lanes_of(values)
    return take(values, lane // 2 + jnp.where(lane < LANES // 2, 0, LANES // 2))


def pack(pieces, width, from_end, start=0):
    lane = lax.broadcasted_iota(jnp.int32, pieces[0].shape, 1)
    out = jnp.zeros(pieces[0].shape, F32)
    for i, piece in enumerate(pieces, start):
        shift = (width * i + (width if from_end else 0)) % LANES
        moved = pltpu.roll(piece, shift, 1) if shift else piece
        out = jnp.where((lane >= width * i) & (lane < width * (i + 1)), moved, out)
    return out


def unpack(left, right, i, width, start=0):
    lane = lax.broadcasted_iota(jnp.int32, left.shape, 1)
    back = (LANES - width * i) % LANES
    end = (LANES - width - width * (i + start)) % LANES
    first = pltpu.roll(right, back, 1) if back else right
    last = pltpu.roll(left, end, 1) if end else left
    return jnp.where(lane < width, first, jnp.where(lane >= LANES - width, last, 0.0))


def before_kernel(flags, own, zown, ylo, zlo, yhi, zhi, kap, diag, inv, xout, rout, coarse, to_left, to_right, va, wa, vb, wb, res, acc, flat):
    rows = own.shape[1]
    tiles = own.shape[2]
    x_count = own.shape[3]
    inner = slice(PAD, PAD + x_count)
    last = HALO + rows
    zero_pads((kap, va, wa, vb, wb))

    def fill(j, k, b, z, y, there):
        left = jnp.where((flags[0] > 0) & there, z[0], 0.0)
        right = jnp.where((flags[1] > 0) & there, z[1], 0.0)
        kap[j, 0:tiles, inner, :] = jnp.where(there, SCALE * k, 0.0)
        kap[j, tiles, inner, :] = SCALE * unpack(left, right, y, EDGE)
        if b is not None:
            res[j, 0:tiles] = b
            res[j, tiles] = unpack(z[0], z[1], rows + y, EDGE)

    for y in range(rows):
        fill(HALO + y, own[0, y], own[1, y], zown, y, flags[4] > 0)
    for j in range(HALO):
        b = ylo[HALO + j - 1] if j else None
        fill(j, ylo[j], b, zlo, rows - HALO + j, flags[2] > 0)
        b = yhi[HALO + j] if j < HALO - 1 else None
        fill(last + j, yhi[j], b, zhi, j, flags[3] > 0)
    make_diagonal(kap, diag, inv, 1, last + HALO - 1)
    centre, weights = chebyshev_coefs(DEGREE, smooth_low)
    first_update(kap, inv, res, va, wa, acc, 1, last + HALO - 1, 1.0 / centre, False, (HALO, last, tiles))
    old, new = (va, wa), (vb, wb)
    lo, hi = 2, last + HALO - 2
    for pair in weights:
        smoothing_step(kap, diag, inv, res, old, new, acc, lo, hi, pair, (HALO, last, tiles))
        old, new = new, old
        lo, hi = lo + 1, hi - 1
    residual_only(kap, diag, res, old[0], old[1], HALO, last)
    at = 0
    for y in range(rows):
        xout[y] = acc[HALO + y, 0:tiles]
        rout[y] = res[HALO + y, 0:tiles]
    for source, offset in ((kap, PAD), (res, 0)):
        for y in range(0, rows, 2):
            both = (
                source[HALO + y, 0:tiles, offset : offset + x_count, :]
                + source[HALO + y + 1, 0:tiles, offset : offset + x_count, :]
            )
            flat[at : at + x_count, :] = halve(both[0], both[1])
            at += x_count
    total = flat.shape[0]
    coarse[...] = flat[pl.ds(0, total // 2, stride=2), :] + flat[pl.ds(1, total // 2, stride=2), :]
    each, xc = rows // 2, x_count // 2
    for out, from_end in ((to_left, False), (to_right, True)):
        for i in range(2):
            value = [coarse[(i * each + y) * xc : (i * each + y + 1) * xc, :] for y in range(each)]
            out[i * xc : (i + 1) * xc, :] = pack(value, COARSE_EDGE, from_end)
        value = [res[HALO + y, tiles - 1 if from_end else 0] for y in range(rows)]
        out[2 * xc : 2 * xc + x_count, :] = pack(value, EDGE, from_end, rows if from_end else 0)


def after_kernel(places, *refs, count):
    blocks, zblocks = refs[:count], refs[count : 2 * count]
    refs = refs[2 * count :]
    (kap, diag, inv, xpre, rown, zown, rlo, zlo, rhi, zhi, sol, resid) = refs[:12]
    (k1, d1, i1, r1, x1, va1, wa1, vb1, wb1, k2, d2, i2, r2, x2, va2, wa2, vb2, wb2, flat, va, wa, vb, wb, res, acc) = refs[12:]
    me_x, me_y = places[0], places[1]
    zero_pads((k1, va1, wa1, vb1, wb1, k2, va2, wa2, vb2, wb2, va, wa, vb, wb))
    each = blocks[0].shape[1]
    xc = blocks[0].shape[2]
    tiles = xpre.shape[1]
    yc = each * count
    lo1, hi1 = COARSE_PAD, COARSE_PAD + yc
    edge = [lo1 - 1, hi1]
    for ref in (k1, va1, wa1, vb1, wb1):
        zero_rows(ref, edge)
    zero_rows(x1, list(range(lo1)) + list(range(hi1, hi1 + COARSE_PAD)))
    for number, (block, z) in enumerate(zip(blocks, zblocks)):
        at = places[4 + number] * each + COARSE_PAD
        left = jnp.where(places[2] > 0, z[0, 0], 0.0)
        right = jnp.where(places[3] > 0, z[1, 0], 0.0)
        for y in range(each):
            k1[at + y, 0, PAD : PAD + xc, :] = block[0, y] * 0.25
            k1[at + y, 1, PAD : PAD + xc, :] = unpack(left, right, y, COARSE_EDGE) * 0.25
            r1[at + y, 0] = block[1, y]
            r1[at + y, 1] = unpack(z[0, 1], z[1, 1], y, COARSE_EDGE)
    make_diagonal(k1, d1, i1, lo1, hi1)
    centre, weights = chebyshev_coefs(DEGREE, smooth_low)
    first_update(k1, i1, r1, va1, wa1, x1, lo1, hi1, 1.0 / centre, False)
    old, new = (va1, wa1), (vb1, wb1)
    for pair in weights:
        smoothing_step(k1, d1, i1, r1, old, new, x1, lo1, hi1, pair)
        old, new = new, old
    residual_only(k1, d1, r1, old[0], old[1], lo1, hi1)
    tiles1 = k1.shape[1]
    y2 = yc // 2
    half = xc // 2
    for target, source, offset, factor in ((k2, k1, PAD, 0.25), (r2, r1, 0, 1.0)):
        for y in range(y2):
            a = lo1 + 2 * y
            both = source[a, :, offset : offset + xc, :] + source[a + 1, :, offset : offset + xc, :]
            flat[y * xc : (y + 1) * xc, :] = halve(both[0], both[1])
        if target is k2:
            zero_rows(k2, range(y2 + 2))
        for y in range(y2):
            value = flat[pl.ds(y * xc, half, stride=2), :] + flat[pl.ds(y * xc + 1, half, stride=2), :]
            if target is k2:
                k2[1 + y, 0, PAD : PAD + half, :] = value * factor
            else:
                r2[1 + y] = jnp.zeros(r2.shape[1:], F32)
                r2[1 + y, 0, 0:half, :] = value
    for ref in (va2, wa2, vb2, wb2):
        zero_rows(ref, [0, y2 + 1])
    make_diagonal(k2, d2, i2, 1, 1 + y2)
    centre, weights = chebyshev_coefs(COARSE_DEGREE, coarse_low)
    first_update(k2, i2, r2, va2, wa2, x2, 1, 1 + y2, 1.0 / centre, False)
    old, new = (va2, wa2), (vb2, wb2)
    for pair in weights:
        smoothing_step(k2, d2, i2, r2, old, new, x2, 1, 1 + y2, pair)
        old, new = new, old
    for y in range(y2):
        value = x2[1 + y, 0, 0:half, :]
        flat[pl.ds(y * xc, half, stride=2), :] = value
        flat[pl.ds(y * xc + 1, half, stride=2), :] = value
    for y in range(y2):
        for t, value in enumerate(double(flat[y * xc : (y + 1) * xc, :])):
            for s in (0, 1):
                at = lo1 + 2 * y + s
                va1[at, t, PAD : PAD + xc, :] = value
                x1[at, t] = x1[at, t] + value
    times(k1, va1, wa1, lo1, hi1)
    centre, weights = chebyshev_coefs(DEGREE, smooth_low)
    residual_only(k1, d1, r1, va1, wa1, lo1, hi1)
    first_update(k1, i1, r1, va1, wa1, x1, lo1, hi1, 1.0 / centre, True)
    old, new = (va1, wa1), (vb1, wb1)
    for pair in weights:
        smoothing_step(k1, d1, i1, r1, old, new, x1, lo1, hi1, pair)
        old, new = new, old
    rows = rown.shape[0]
    last = HALO + rows
    x_count = rown.shape[2]
    wide_rows = (rows + 2 * HALO) // 2 + 1
    start = COARSE_PAD - (HALO + 1) // 2 + each * me_y
    for t in range(tiles1):
        for y in range(wide_rows):
            value = x1[start + y, t]
            base = (t * wide_rows + y) * x_count
            flat[pl.ds(base, xc, stride=2), :] = value
            flat[pl.ds(base + 1, xc, stride=2), :] = value
    inner = slice(PAD, PAD + x_count)
    for y in range(wide_rows):
        parts = []
        for t in range(tiles1):
            at = (t * wide_rows + y) * x_count
            value = flat[at : at + x_count, :]
            parts += double(value) if t < tiles1 - 1 else [double_halo(value)]
        for j in (2 * y - 1, 2 * y):
            if not 0 <= j < rows + 2 * HALO:
                continue
            for t, value in enumerate(parts):
                va[j, t, inner, :] = value
                wa[j, t, inner, :] = kap[j, t, inner, :] * value
                if HALO <= j < last and t < tiles:
                    acc[j, t] = xpre[j - HALO, t] + value

    edge = HALO - 1
    for j in range(-edge, rows + edge):
        if j < 0:
            source, z, i, y = rlo, zlo, edge + j, rows + j
        elif j < rows:
            source, z, i, y = rown, zown, j, j
        else:
            source, z, i, y = rhi, zhi, j - rows, j - rows
        res[HALO + j, 0:tiles] = source[i]
        packed = z[...]
        res[HALO + j, tiles] = unpack(packed, packed, y, EDGE, rows)
    residual_only(kap, diag, res, va, wa, 1, last + HALO - 1)
    first_update(kap, inv, res, va, wa, acc, 1, last + HALO - 1, 1.0 / centre, True, (HALO, last, tiles))
    old, new = (va, wa), (vb, wb)
    lo, hi = 2, last + HALO - 2
    for pair in weights:
        smoothing_step(kap, diag, inv, res, old, new, acc, lo, hi, pair, (HALO, last, tiles))
        old, new = new, old
        lo, hi = lo + 1, hi - 1
    block_x = sol.shape[0]
    for x in range(0, x_count, 8):

        @pl.when(me_x == x // block_x)
        def _(x=x):
            values = new_residuals(kap, diag, res, old[0], old[1], HALO, rows, x)
            for y, (_, _, _, value) in enumerate(values):
                for t in range(tiles):
                    lanes = slice(t * LANES, (t + 1) * LANES)
                    at = slice(x % block_x, x % block_x + 8)
                    sol[at, y, lanes] = acc[HALO + y, t, x : x + 8, :]
                    resid[at, y, lanes] = value[t]


def ring(values, axis, step):
    count = lax.axis_size(axis)
    return lax.ppermute(values, axis, [(i, (i + step) % count) for i in range(count)])


def exchange(to_low, to_high, axis, across=None):
    count = lax.axis_size(axis)
    if count % 2:
        return ring(to_high, axis, 1), ring(to_low, axis, -1)
    odd = lax.axis_index(axis) % 2 == 1
    inner = [i + 1 if i % 2 else i - 1 for i in range(count)]
    one = lax.ppermute(jnp.where(odd, to_low, to_high), axis, [(i, i ^ 1) for i in range(count)])
    names, pairs = axis, [(i, t % count) for i, t in enumerate(inner)]
    if across is not None and lax.axis_size(across) % 2 == 0:
        names = (across, axis)
        pairs = [
            (x * count + i, x * count + t if 0 <= t < count else (x ^ 1) * count + i)
            for x in range(lax.axis_size(across))
            for i, t in enumerate(inner)
        ]
    two = lax.ppermute(jnp.where(odd, to_high, to_low), names, pairs)
    return jnp.where(odd, one, two), jnp.where(odd, two, one)


def exchange_and_gather(to_low, to_high):
    nx, nz = lax.axis_size("gx"), lax.axis_size("gz")
    if nx != 2 or nz % 2:
        return gather_first(jnp.stack(exchange(to_low, to_high, "gz")), "gx", 1)
    odd = lax.axis_index("gz") % 2 == 1
    out = []
    for payload, step in (
        (jnp.where(odd, to_low, to_high), [i ^ 1 for i in range(nz)]),
        (jnp.where(odd, to_high, to_low), [(i + 1 if i % 2 else i - 1) % nz for i in range(nz)]),
    ):
        same = lax.ppermute(payload, "gz", list(enumerate(step)))
        pairs = [(x * nz + i, (1 - x) * nz + t) for x in (0, 1) for i, t in enumerate(step)]
        cross = lax.ppermute(payload, ("gx", "gz"), pairs)
        first = lax.axis_index("gx") == 0
        out.append(jnp.concatenate([jnp.where(first, same, cross), jnp.where(first, cross, same)], axis=0))
    one, two = out
    return jnp.stack([jnp.where(odd, one, two), jnp.where(odd, two, one)])


def gather_first(values, axis, dim):
    count = lax.axis_size(axis)
    if count == 1:
        return values
    if count == 2:
        other = lax.ppermute(values, axis, [(0, 1), (1, 0)])
        first = lax.axis_index(axis) == 0
        return jnp.concatenate(
            [jnp.where(first, values, other), jnp.where(first, other, values)], axis=dim
        )
    every = lax.all_gather(values, axis)
    return jnp.concatenate([every[i] for i in range(count)], axis=dim)


def gather_second(block, low_edge, high_edge, me, count):
    size = block.shape[0]
    blocks, sources = [block], [me]
    low = high = low_edge
    if count == 4:
        odd = me % 2 == 1
        near = jnp.where(odd, low_edge, high_edge)
        far = jnp.where(odd, high_edge, low_edge)
        nx = lax.axis_size("gx")
        pairs = [(x * 4 + i, x * 4 + 3 - i if i in (1, 2) else (x ^ 1) * 4 + i) for x in range(nx) for i in range(4)]
        if nx % 2:
            pairs = [(x * 4 + i, x * 4 + 3 - i) for x in range(nx) for i in range(4)]
        got = []
        for step in (1, 2, 3):
            payload = jnp.concatenate([block, near], axis=0) if step == 1 else block
            got.append(lax.ppermute(payload, "gy", [(i, i ^ step) for i in range(count)]))
            blocks.append(got[-1][:size])
            sources.append(me ^ step)
        far = lax.ppermute(far, ("gx", "gy"), pairs)
        near = got[0][size:]
        low, high = jnp.where(odd, near, far), jnp.where(odd, far, near)
    else:
        for step in range(1, count):
            parts = [block]
            if step == 1:
                parts.append(high_edge)
            if step == count - 1:
                parts.append(low_edge)
            got = ring(jnp.concatenate(parts, axis=0), "gy", step)
            blocks.append(got[:size])
            sources.append((me - step) % count)
            if step == 1:
                low = got[size : size + high_edge.shape[0]]
            if step == count - 1:
                high = got[got.shape[0] - low_edge.shape[0] :]
    return blocks, sources, low, high


def vmem(shape):
    return pltpu.VMEM(shape, F32)


def call(kernel, out_shapes, scratch, inputs):
    limit = 4 * 2**20
    for s in scratch:
        size = 4
        for n in s.shape:
            size *= n
        limit += size
    for a in list(inputs) + list(out_shapes):
        limit += 4 * a.size if hasattr(a, "size") else 0
    limit = min(limit + 8 * 2**20, 60 * 2**20)
    whole = pl.BlockSpec(memory_space=pltpu.VMEM)
    return pl.pallas_call(
        kernel,
        out_shape=out_shapes,
        in_specs=[pl.BlockSpec(memory_space=pltpu.SMEM)] + [whole] * (len(inputs) - 1),
        out_specs=[whole] * len(out_shapes),
        scratch_shapes=scratch,
        compiler_params=pltpu.CompilerParams(vmem_limit_bytes=limit),
    )(*inputs)


def body(conductivity, source):
    bx, by, bz = conductivity.shape
    tiles = bz // LANES
    nx, ny, nz = (lax.axis_size(a) for a in ("gx", "gy", "gz"))
    ix, iy, iz = (lax.axis_index(a) for a in ("gx", "gy", "gz"))
    yes = ix >= 0
    flags = jnp.stack([iz > 0, iz < nz - 1, iy > 0, iy < ny - 1, yes]).astype(jnp.int32)
    x_count = bx * nx

    def shape(*dims):
        return jax.ShapeDtypeStruct(dims, F32)

    def lines(*arrays):
        return jnp.concatenate([a.reshape(-1, LANES) for a in arrays], axis=0)

    mine = jnp.stack([conductivity, source]).reshape(2, bx, by, tiles, LANES).transpose(0, 2, 3, 1, 4)
    first_edge = jnp.concatenate([mine[a, y, 0, :, :EDGE] for a in (0, 1) for y in range(by)], axis=-1)
    last_edge = jnp.concatenate(
        [mine[a, y, tiles - 1, :, LANES - EDGE :] for a in (0, 1) for y in range(by)], axis=-1
    )
    own = gather_first(mine, "gx", 3)
    zown = exchange_and_gather(first_edge, last_edge)
    edge = HALO - 1
    low_rows = lines(own[0, :HALO], own[1, :edge], zown)
    high_rows = lines(own[0, by - HALO :], own[1, by - edge :], zown)
    from_low, from_high = exchange(low_rows, high_rows, "gy", "gx")
    cut = (HALO + edge) * tiles * x_count
    rows_shape = (HALO + edge, tiles, x_count, LANES)
    ylo, zlo = from_low[:cut].reshape(rows_shape), from_low[cut:].reshape(zown.shape)
    yhi, zhi = from_high[:cut].reshape(rows_shape), from_high[cut:].reshape(zown.shape)

    ext = by + 2 * HALO
    padded = x_count + 2 * PAD
    wide = (ext, tiles + 1, padded, LANES)
    plain = (ext, tiles + 1, x_count, LANES)
    each = by // 2
    xc = x_count // 2
    kap, diag, inv, xpre, rpre, coarse, to_left, to_right = call(
        before_kernel,
        [
            shape(*wide),
            shape(*plain),
            shape(*plain),
            shape(by, tiles, x_count, LANES),
            shape(by, tiles, x_count, LANES),
            shape(2 * each * xc, LANES),
            shape(2 * xc + x_count, LANES),
            shape(2 * xc + x_count, LANES),
        ],
        [vmem(wide)] * 4 + [vmem(plain)] * 2 + [vmem((2 * each * x_count, LANES))],
        [flags, own, zown, ylo, zlo, yhi, zhi],
    )

    left, right = exchange(to_left, to_right, "gz")
    coarse_z = jnp.stack([left[: 2 * xc], right[: 2 * xc]])
    lane = lax.broadcasted_iota(jnp.int32, (x_count, LANES), 1)
    fine_z = jnp.where(lane < LANES // 2, right[2 * xc :], left[2 * xc :])
    blocks, sources, low, high = gather_second(
        lines(coarse, coarse_z), lines(rpre[:edge], fine_z), lines(rpre[by - edge :], fine_z), iy, ny
    )
    cut = 2 * each * xc
    zblocks = [b[cut:].reshape(2, 2, xc, LANES) for b in blocks]
    blocks = [b[:cut].reshape(2, each, xc, LANES) for b in blocks]
    cut = edge * tiles * x_count
    rows_shape = (edge, tiles, x_count, LANES)
    rlo, zrlo = low[:cut].reshape(rows_shape), low[cut:].reshape(fine_z.shape)
    rhi, zrhi = high[:cut].reshape(rows_shape), high[cut:].reshape(fine_z.shape)

    yc = each * ny
    tiles1 = tiles // 2 + 1
    wide1 = (yc + 2 * COARSE_PAD, tiles1, xc + 2 * PAD, LANES)
    plain1 = (yc + 2 * COARSE_PAD, tiles1, xc, LANES)
    y2 = yc // 2
    x2 = max(xc // 2, 8)
    wide2 = (y2 + 2, 1, x2 + 2 * PAD, LANES)
    plain2 = (y2 + 2, 1, x2, LANES)
    flat_rows = max(y2 * xc, tiles1 * (ext // 2 + 1) * x_count)

    places = jnp.stack([jnp.int32(p) for p in (ix, iy, iz > 0, iz < nz - 1, *sources)])

    def kernel(*refs):
        after_kernel(*refs, count=len(blocks))

    sol, resid = call(
        kernel,
        [shape(bx, by, bz), shape(bx, by, bz)],
        [vmem(wide1)] + [vmem(plain1)] * 4 + [vmem(wide1)] * 4
        + [vmem(wide2)] + [vmem(plain2)] * 4 + [vmem(wide2)] * 4
        + [vmem((flat_rows, LANES))] + [vmem(wide)] * 4 + [vmem(plain)] * 2,
        [places] + blocks + zblocks
        + [kap, diag, inv, xpre, rpre, fine_z, rlo, zrlo, rhi, zrhi],
    )
    return sol, resid


def solution(mesh):
    spec = P("gx", "gy", "gz")

    return jax.shard_map(body, mesh=mesh, in_specs=(spec, spec), out_specs=(spec, spec), check_vma=False)
```

```python
import jax
import jax.numpy as jnp
from jax import lax
from jax.experimental import pallas as pl
from jax.experimental.pallas import tpu as pltpu
from jax.sharding import PartitionSpec as P


DEGREE = 4
COARSE_DEGREE = 8
smooth_low = 0.5
coarse_low = 0.03
upper_bound = 2.0

F32 = jnp.float32
LANES = 128
PAD = 8
HALO = 5
COARSE_PAD = 4
FACE = 14.0 / 3.0
CORNER = 1.0 / 3.0
TOTAL = 128.0 / 3.0
SCALE = 0.05


def chebyshev_coefs(degree, lower):
    centre = (upper_bound + lower) / 2.0
    half_width = (upper_bound - lower) / 2.0
    ratio_term = centre / half_width
    rho_prev = 1.0 / ratio_term
    weights = []
    for _ in range(1, degree):
        rho_next = 1.0 / (2.0 * ratio_term - rho_prev)
        weights.append((rho_next * rho_prev, 2.0 * rho_next / half_width))
        rho_prev = rho_next
    return centre, weights


EDGE = 8
COARSE_EDGE = 32
CHUNK = 16


def chunks(start, stop, body):
    count = stop - start
    full = count // CHUNK
    if full == 1:
        body(start, CHUNK)
    elif full > 1:

        def step(i, carry):
            body(start + i * CHUNK, CHUNK)
            return carry

        lax.fori_loop(0, full, step, 0)
    if count % CHUNK:
        body(start + full * CHUNK, count % CHUNK)


def loop(start, stop, body):
    def group(first, rows):
        for i in range(rows):
            body(first + i)

    chunks(start, stop, group)


def third_pairs(values):
    tiles, rows, _ = values.shape
    flat = values.reshape(tiles * rows, LANES)
    up = pltpu.roll(flat, 1, 1).reshape(tiles, rows, LANES)
    down = pltpu.roll(flat, LANES - 1, 1).reshape(tiles, rows, LANES)
    if tiles > 1:
        lane = lax.broadcasted_iota(jnp.int32, (tiles, rows, LANES), 2)
        up_other = jnp.concatenate([up[tiles - 1 :], up[: tiles - 1]], axis=0)
        down_other = jnp.concatenate([down[1:], down[:1]], axis=0)
        up = jnp.where(lane == 0, up_other, up)
        down = jnp.where(lane == LANES - 1, down_other, down)
    return up + down


def neighbour_sums(ref, first, rows, row):
    at = range(first - 1, first + rows + 1) if isinstance(first, int) else [first + i for i in range(-1, rows + 1)]
    centre = [ref[y, :, row : row + 8, :] for y in at]
    side = [ref[y, :, row - 1 : row + 7, :] + ref[y, :, row + 1 : row + 9, :] for y in at]
    out = []
    for i in range(1, rows + 1):
        corner = side[i - 1] + side[i + 1]
        face = (centre[i - 1] + centre[i + 1]) + side[i]
        plane = FACE * face + corner
        beside = FACE * centre[i] + face + CORNER * corner
        out.append((plane + third_pairs(beside), centre[i]))
    return out


def zero_pads(refs):
    for ref in refs:
        count, tiles, rows, _ = ref.shape
        zero = jnp.zeros((tiles, PAD, LANES), F32)

        def body(y, ref=ref, rows=rows, zero=zero):
            ref[y, :, 0:PAD, :] = zero
            ref[y, :, rows - PAD : rows, :] = zero

        loop(0, count, body)


def zero_rows(ref, rows):
    zero = jnp.zeros(ref.shape[1:], F32)
    for y in rows:
        ref[y] = zero


def tiles_of(ref):
    return range(0, ref.shape[2], 8)


def make_diagonal(kap, diag, inv, lo, hi):
    def body(first, rows):
        for x in tiles_of(diag):
            for i, (total, centre) in enumerate(neighbour_sums(kap, first, rows, PAD + x)):
                value = TOTAL * centre + total
                diag[first + i, :, x : x + 8, :] = value
                inv[first + i, :, x : x + 8, :] = jnp.where(centre > 0.0, 1.0 / value, 0.0)

    chunks(lo, hi, body)


def accumulate(acc, y, x, step, add, own):
    tiles = step.shape[0]
    if own is not None:
        if isinstance(y, int) and not own[0] <= y < own[1]:
            return
        tiles = own[2]
    step = step[0:tiles]
    acc[y, 0:tiles, x : x + 8, :] = acc[y, 0:tiles, x : x + 8, :] + step if add else step


def first_update(kap, inv, res, v, w, acc, lo, hi, scale, add, own=None):
    def body(y):
        for x in tiles_of(inv):
            step = (inv[y, :, x : x + 8, :] * scale) * res[y, :, x : x + 8, :]
            v[y, :, PAD + x : PAD + x + 8, :] = step
            w[y, :, PAD + x : PAD + x + 8, :] = kap[y, :, PAD + x : PAD + x + 8, :] * step
            accumulate(acc, y, x, step, add, own)

    loop(lo, hi, body)


def times(kap, v, w, lo, hi):
    def body(y):
        w[y] = kap[y] * v[y]

    loop(lo, hi, body)


def new_residuals(kap, diag, res, v, w, first, rows, x):
    total = neighbour_sums(v, first, rows, PAD + x)
    weighted = neighbour_sums(w, first, rows, PAD + x)
    for i in range(rows):
        y = first + i
        k = kap[y, :, PAD + x : PAD + x + 8, :]
        centre = total[i][1]
        value = (
            res[y, :, x : x + 8, :]
            - diag[y, :, x : x + 8, :] * centre
            + (k * total[i][0] + weighted[i][0])
        )
        yield y, k, centre, value


def residual_only(kap, diag, res, v, w, lo, hi):
    def body(first, rows):
        for x in tiles_of(diag):
            for y, _, _, value in new_residuals(kap, diag, res, v, w, first, rows, x):
                res[y, :, x : x + 8, :] = value

    chunks(lo, hi, body)


def smoothing_step(kap, diag, inv, res, old, new, acc, lo, hi, pair, own=None):
    def body(first, rows):
        for x in tiles_of(diag):
            for y, k, centre, value in new_residuals(kap, diag, res, old[0], old[1], first, rows, x):
                res[y, :, x : x + 8, :] = value
                step = pair[0] * centre + (pair[1] * inv[y, :, x : x + 8, :]) * value
                new[0][y, :, PAD + x : PAD + x + 8, :] = step
                new[1][y, :, PAD + x : PAD + x + 8, :] = k * step
                accumulate(acc, y, x, step, True, own)

    chunks(lo, hi, body)


def lanes_of(values):
    return lax.broadcasted_iota(jnp.int32, values.shape, 1)


def take(values, index):
    return jnp.take_along_axis(values, index, axis=1, mode="promise_in_bounds")


def halve(first, second):
    lane = lanes_of(first)
    even = (2 * lane) % LANES
    low = take(first + pltpu.roll(first, LANES - 1, 1), even)
    high = take(second + pltpu.roll(second, LANES - 1, 1), even)
    return jnp.where(lane < LANES // 2, low, high) * 0.125


def double(values):
    half = lanes_of(values) // 2
    return take(values, half), take(values, half + LANES // 2)


def double_halo(values):
    lane = lanes_of(values)
    return take(values, lane // 2 + jnp.where(lane < LANES // 2, 0, LANES // 2))


def pack(pieces, width, from_end, start=0):
    lane = lax.broadcasted_iota(jnp.int32, pieces[0].shape, 1)
    out = jnp.zeros(pieces[0].shape, F32)
    for i, piece in enumerate(pieces, start):
        shift = (width * i + (width if from_end else 0)) % LANES
        moved = pltpu.roll(piece, shift, 1) if shift else piece
        out = jnp.where((lane >= width * i) & (lane < width * (i + 1)), moved, out)
    return out


def unpack(left, right, i, width, start=0):
    lane = lax.broadcasted_iota(jnp.int32, left.shape, 1)
    back = (LANES - width * i) % LANES
    end = (LANES - width - width * (i + start)) % LANES
    first = pltpu.roll(right, back, 1) if back else right
    last = pltpu.roll(left, end, 1) if end else left
    return jnp.where(lane < width, first, jnp.where(lane >= LANES - width, last, 0.0))


def before_kernel(own, zown, ylo, zlo, yhi, zhi, kap, diag, inv, xout, rout, coarse, to_left, to_right, va, wa, vb, wb, res, acc, flat):
    rows = own.shape[1]
    tiles = own.shape[2]
    x_count = own.shape[3]
    inner = slice(PAD, PAD + x_count)
    last = HALO + rows
    iy, iz = lax.axis_index("gy"), lax.axis_index("gz")
    ny, nz = lax.axis_size("gy"), lax.axis_size("gz")
    has_left, has_right = iz > 0, iz < nz - 1
    zero_pads((kap, va, wa, vb, wb))

    def fill(j, k, b, z, y, there):
        left = jnp.where(has_left & there, z[0], 0.0)
        right = jnp.where(has_right & there, z[1], 0.0)
        kap[j, 0:tiles, inner, :] = jnp.where(there, SCALE * k, 0.0)
        kap[j, tiles, inner, :] = SCALE * unpack(left, right, y, EDGE)
        if b is not None:
            res[j, 0:tiles] = b
            res[j, tiles] = unpack(z[0], z[1], rows + y, EDGE)

    for y in range(rows):
        fill(HALO + y, own[0, y], own[1, y], zown, y, iy >= 0)
    for j in range(HALO):
        b = ylo[HALO + j - 1] if j else None
        fill(j, ylo[j], b, zlo, rows - HALO + j, iy > 0)
        b = yhi[HALO + j] if j < HALO - 1 else None
        fill(last + j, yhi[j], b, zhi, j, iy < ny - 1)
    make_diagonal(kap, diag, inv, 1, last + HALO - 1)
    centre, weights = chebyshev_coefs(DEGREE, smooth_low)
    first_update(kap, inv, res, va, wa, acc, 1, last + HALO - 1, 1.0 / centre, False, (HALO, last, tiles))
    old, new = (va, wa), (vb, wb)
    lo, hi = 2, last + HALO - 2
    for pair in weights:
        smoothing_step(kap, diag, inv, res, old, new, acc, lo, hi, pair, (HALO, last, tiles))
        old, new = new, old
        lo, hi = lo + 1, hi - 1
    residual_only(kap, diag, res, old[0], old[1], HALO, last)
    at = 0
    for y in range(rows):
        xout[y] = acc[HALO + y, 0:tiles]
        rout[y] = res[HALO + y, 0:tiles]
    for source, offset in ((kap, PAD), (res, 0)):
        for y in range(0, rows, 2):
            both = (
                source[HALO + y, 0:tiles, offset : offset + x_count, :]
                + source[HALO + y + 1, 0:tiles, offset : offset + x_count, :]
            )
            flat[at : at + x_count, :] = halve(both[0], both[1])
            at += x_count
    total = flat.shape[0]
    coarse[...] = flat[pl.ds(0, total // 2, stride=2), :] + flat[pl.ds(1, total // 2, stride=2), :]
    each, xc = rows // 2, x_count // 2
    for out, from_end in ((to_left, False), (to_right, True)):
        for i in range(2):
            value = [coarse[(i * each + y) * xc : (i * each + y + 1) * xc, :] for y in range(each)]
            out[i * xc : (i + 1) * xc, :] = pack(value, COARSE_EDGE, from_end)
        value = [res[HALO + y, tiles - 1 if from_end else 0] for y in range(rows)]
        out[2 * xc : 2 * xc + x_count, :] = pack(value, EDGE, from_end, rows if from_end else 0)


def sources_of(me, count):
    if count == 4:
        return [me] + [jnp.bitwise_xor(me, step) for step in (1, 2, 3)]
    return [me] + [lax.rem(me - step + count, count) for step in range(1, count)]


def after_kernel(*refs, count):
    blocks, zblocks = refs[:count], refs[count : 2 * count]
    refs = refs[2 * count :]
    (kap, diag, inv, xpre, rown, zown, rlo, zlo, rhi, zhi, sol, resid) = refs[:12]
    (k1, d1, i1, r1, x1, va1, wa1, vb1, wb1, k2, d2, i2, r2, x2, va2, wa2, vb2, wb2, flat, va, wa, vb, wb, res, acc) = refs[12:]
    me_x, me_y, me_z = (lax.axis_index(a) for a in ("gx", "gy", "gz"))
    has_left, has_right = me_z > 0, me_z < lax.axis_size("gz") - 1
    sources = sources_of(me_y, count)
    zero_pads((k1, va1, wa1, vb1, wb1, k2, va2, wa2, vb2, wb2, va, wa, vb, wb))
    each = blocks[0].shape[1]
    xc = blocks[0].shape[2]
    tiles = xpre.shape[1]
    yc = each * count
    lo1, hi1 = COARSE_PAD, COARSE_PAD + yc
    edge = [lo1 - 1, hi1]
    for ref in (k1, va1, wa1, vb1, wb1):
        zero_rows(ref, edge)
    zero_rows(x1, list(range(lo1)) + list(range(hi1, hi1 + COARSE_PAD)))
    for number, (block, z) in enumerate(zip(blocks, zblocks)):
        at = sources[number] * each + COARSE_PAD
        left = jnp.where(has_left, z[0, 0], 0.0)
        right = jnp.where(has_right, z[1, 0], 0.0)
        for y in range(each):
            k1[at + y, 0, PAD : PAD + xc, :] = block[0, y] * 0.25
            k1[at + y, 1, PAD : PAD + xc, :] = unpack(left, right, y, COARSE_EDGE) * 0.25
            r1[at + y, 0] = block[1, y]
            r1[at + y, 1] = unpack(z[0, 1], z[1, 1], y, COARSE_EDGE)
    make_diagonal(k1, d1, i1, lo1, hi1)
    centre, weights = chebyshev_coefs(DEGREE, smooth_low)
    first_update(k1, i1, r1, va1, wa1, x1, lo1, hi1, 1.0 / centre, False)
    old, new = (va1, wa1), (vb1, wb1)
    for pair in weights:
        smoothing_step(k1, d1, i1, r1, old, new, x1, lo1, hi1, pair)
        old, new = new, old
    residual_only(k1, d1, r1, old[0], old[1], lo1, hi1)
    tiles1 = k1.shape[1]
    y2 = yc // 2
    half = xc // 2
    for target, source, offset, factor in ((k2, k1, PAD, 0.25), (r2, r1, 0, 1.0)):
        for y in range(y2):
            a = lo1 + 2 * y
            both = source[a, :, offset : offset + xc, :] + source[a + 1, :, offset : offset + xc, :]
            flat[y * xc : (y + 1) * xc, :] = halve(both[0], both[1])
        if target is k2:
            zero_rows(k2, range(y2 + 2))
        for y in range(y2):
            value = flat[pl.ds(y * xc, half, stride=2), :] + flat[pl.ds(y * xc + 1, half, stride=2), :]
            if target is k2:
                k2[1 + y, 0, PAD : PAD + half, :] = value * factor
            else:
                r2[1 + y] = jnp.zeros(r2.shape[1:], F32)
                r2[1 + y, 0, 0:half, :] = value
    for ref in (va2, wa2, vb2, wb2):
        zero_rows(ref, [0, y2 + 1])
    make_diagonal(k2, d2, i2, 1, 1 + y2)
    centre, weights = chebyshev_coefs(COARSE_DEGREE, coarse_low)
    first_update(k2, i2, r2, va2, wa2, x2, 1, 1 + y2, 1.0 / centre, False)
    old, new = (va2, wa2), (vb2, wb2)
    for pair in weights:
        smoothing_step(k2, d2, i2, r2, old, new, x2, 1, 1 + y2, pair)
        old, new = new, old
    for y in range(y2):
        value = x2[1 + y, 0, 0:half, :]
        flat[pl.ds(y * xc, half, stride=2), :] = value
        flat[pl.ds(y * xc + 1, half, stride=2), :] = value
    for y in range(y2):
        for t, value in enumerate(double(flat[y * xc : (y + 1) * xc, :])):
            for s in (0, 1):
                at = lo1 + 2 * y + s
                va1[at, t, PAD : PAD + xc, :] = value
                x1[at, t] = x1[at, t] + value
    times(k1, va1, wa1, lo1, hi1)
    centre, weights = chebyshev_coefs(DEGREE, smooth_low)
    residual_only(k1, d1, r1, va1, wa1, lo1, hi1)
    first_update(k1, i1, r1, va1, wa1, x1, lo1, hi1, 1.0 / centre, True)
    old, new = (va1, wa1), (vb1, wb1)
    for pair in weights:
        smoothing_step(k1, d1, i1, r1, old, new, x1, lo1, hi1, pair)
        old, new = new, old
    rows = rown.shape[0]
    last = HALO + rows
    x_count = rown.shape[2]
    wide_rows = (rows + 2 * HALO) // 2 + 1
    start = COARSE_PAD - (HALO + 1) // 2 + each * me_y
    for t in range(tiles1):
        for y in range(wide_rows):
            value = x1[start + y, t]
            base = (t * wide_rows + y) * x_count
            flat[pl.ds(base, xc, stride=2), :] = value
            flat[pl.ds(base + 1, xc, stride=2), :] = value
    inner = slice(PAD, PAD + x_count)
    for y in range(wide_rows):
        parts = []
        for t in range(tiles1):
            at = (t * wide_rows + y) * x_count
            value = flat[at : at + x_count, :]
            parts += double(value) if t < tiles1 - 1 else [double_halo(value)]
        for j in (2 * y - 1, 2 * y):
            if not 0 <= j < rows + 2 * HALO:
                continue
            for t, value in enumerate(parts):
                va[j, t, inner, :] = value
                wa[j, t, inner, :] = kap[j, t, inner, :] * value
                if HALO <= j < last and t < tiles:
                    acc[j, t] = xpre[j - HALO, t] + value

    edge = HALO - 1
    for j in range(-edge, rows + edge):
        if j < 0:
            source, z, i, y = rlo, zlo, edge + j, rows + j
        elif j < rows:
            source, z, i, y = rown, zown, j, j
        else:
            source, z, i, y = rhi, zhi, j - rows, j - rows
        res[HALO + j, 0:tiles] = source[i]
        packed = z[...]
        res[HALO + j, tiles] = unpack(packed, packed, y, EDGE, rows)
    residual_only(kap, diag, res, va, wa, 1, last + HALO - 1)
    first_update(kap, inv, res, va, wa, acc, 1, last + HALO - 1, 1.0 / centre, True, (HALO, last, tiles))
    old, new = (va, wa), (vb, wb)
    lo, hi = 2, last + HALO - 2
    for pair in weights:
        smoothing_step(kap, diag, inv, res, old, new, acc, lo, hi, pair, (HALO, last, tiles))
        old, new = new, old
        lo, hi = lo + 1, hi - 1
    block_x = sol.shape[0]
    for x in range(0, x_count, 8):

        @pl.when(me_x == x // block_x)
        def _(x=x):
            values = new_residuals(kap, diag, res, old[0], old[1], HALO, rows, x)
            for y, (_, _, _, value) in enumerate(values):
                for t in range(tiles):
                    lanes = slice(t * LANES, (t + 1) * LANES)
                    at = slice(x % block_x, x % block_x + 8)
                    sol[at, y, lanes] = acc[HALO + y, t, x : x + 8, :]
                    resid[at, y, lanes] = value[t]


def ring(values, axis, step):
    count = lax.axis_size(axis)
    return lax.ppermute(values, axis, [(i, (i + step) % count) for i in range(count)])


def exchange(to_low, to_high, axis, across=None):
    count = lax.axis_size(axis)
    if count % 2:
        return ring(to_high, axis, 1), ring(to_low, axis, -1)
    odd = lax.axis_index(axis) % 2 == 1
    inner = [i + 1 if i % 2 else i - 1 for i in range(count)]
    one = lax.ppermute(jnp.where(odd, to_low, to_high), axis, [(i, i ^ 1) for i in range(count)])
    names, pairs = axis, [(i, t % count) for i, t in enumerate(inner)]
    if across is not None and lax.axis_size(across) % 2 == 0:
        names = (across, axis)
        pairs = [
            (x * count + i, x * count + t if 0 <= t < count else (x ^ 1) * count + i)
            for x in range(lax.axis_size(across))
            for i, t in enumerate(inner)
        ]
    two = lax.ppermute(jnp.where(odd, to_high, to_low), names, pairs)
    return jnp.where(odd, one, two), jnp.where(odd, two, one)


def exchange_and_gather(to_low, to_high):
    nx, nz = lax.axis_size("gx"), lax.axis_size("gz")
    if nx != 2 or nz % 2:
        return gather_first(jnp.stack(exchange(to_low, to_high, "gz")), "gx", 1)
    odd = lax.axis_index("gz") % 2 == 1
    out = []
    for payload, step in (
        (jnp.where(odd, to_low, to_high), [i ^ 1 for i in range(nz)]),
        (jnp.where(odd, to_high, to_low), [(i + 1 if i % 2 else i - 1) % nz for i in range(nz)]),
    ):
        same = lax.ppermute(payload, "gz", list(enumerate(step)))
        pairs = [(x * nz + i, (1 - x) * nz + t) for x in (0, 1) for i, t in enumerate(step)]
        cross = lax.ppermute(payload, ("gx", "gz"), pairs)
        first = lax.axis_index("gx") == 0
        out.append(jnp.concatenate([jnp.where(first, same, cross), jnp.where(first, cross, same)], axis=0))
    one, two = out
    return jnp.stack([jnp.where(odd, one, two), jnp.where(odd, two, one)])


def gather_first(values, axis, dim):
    count = lax.axis_size(axis)
    if count == 1:
        return values
    if count == 2:
        other = lax.ppermute(values, axis, [(0, 1), (1, 0)])
        first = lax.axis_index(axis) == 0
        return jnp.concatenate(
            [jnp.where(first, values, other), jnp.where(first, other, values)], axis=dim
        )
    every = lax.all_gather(values, axis)
    return jnp.concatenate([every[i] for i in range(count)], axis=dim)


def gather_second(block, low_edge, high_edge, me, count):
    size = block.shape[0]
    blocks = [block]
    low = high = low_edge
    if count == 4:
        odd = me % 2 == 1
        near = jnp.where(odd, low_edge, high_edge)
        far = jnp.where(odd, high_edge, low_edge)
        nx = lax.axis_size("gx")
        pairs = [(x * 4 + i, x * 4 + 3 - i if i in (1, 2) else (x ^ 1) * 4 + i) for x in range(nx) for i in range(4)]
        if nx % 2:
            pairs = [(x * 4 + i, x * 4 + 3 - i) for x in range(nx) for i in range(4)]
        got = []
        for step in (1, 2, 3):
            payload = jnp.concatenate([block, near], axis=0) if step == 1 else block
            got.append(lax.ppermute(payload, "gy", [(i, i ^ step) for i in range(count)]))
            blocks.append(got[-1][:size])
        far = lax.ppermute(far, ("gx", "gy"), pairs)
        near = got[0][size:]
        low, high = jnp.where(odd, near, far), jnp.where(odd, far, near)
    else:
        for step in range(1, count):
            parts = [block]
            if step == 1:
                parts.append(high_edge)
            if step == count - 1:
                parts.append(low_edge)
            got = ring(jnp.concatenate(parts, axis=0), "gy", step)
            blocks.append(got[:size])
            if step == 1:
                low = got[size : size + high_edge.shape[0]]
            if step == count - 1:
                high = got[got.shape[0] - low_edge.shape[0] :]
    return blocks, low, high


def vmem(shape):
    return pltpu.VMEM(shape, F32)


def call(kernel, out_shapes, scratch, inputs):
    limit = 4 * 2**20
    for s in scratch:
        size = 4
        for n in s.shape:
            size *= n
        limit += size
    for a in list(inputs) + list(out_shapes):
        limit += 4 * a.size if hasattr(a, "size") else 0
    limit = min(limit + 8 * 2**20, 60 * 2**20)
    whole = pl.BlockSpec(memory_space=pltpu.VMEM)
    return pl.pallas_call(
        kernel,
        out_shape=out_shapes,
        in_specs=[whole] * len(inputs),
        out_specs=[whole] * len(out_shapes),
        scratch_shapes=scratch,
        compiler_params=pltpu.CompilerParams(vmem_limit_bytes=limit),
    )(*inputs)


def body(conductivity, source):
    bx, by, bz = conductivity.shape
    tiles = bz // LANES
    nx, ny, _ = (lax.axis_size(a) for a in ("gx", "gy", "gz"))
    iy = lax.axis_index("gy")
    x_count = bx * nx

    def shape(*dims):
        return jax.ShapeDtypeStruct(dims, F32)

    def lines(*arrays):
        return jnp.concatenate([a.reshape(-1, LANES) for a in arrays], axis=0)

    mine = jnp.stack([conductivity, source]).reshape(2, bx, by, tiles, LANES).transpose(0, 2, 3, 1, 4)
    first_edge = jnp.concatenate([mine[a, y, 0, :, :EDGE] for a in (0, 1) for y in range(by)], axis=-1)
    last_edge = jnp.concatenate(
        [mine[a, y, tiles - 1, :, LANES - EDGE :] for a in (0, 1) for y in range(by)], axis=-1
    )
    own = gather_first(mine, "gx", 3)
    zown = exchange_and_gather(first_edge, last_edge)
    edge = HALO - 1
    low_rows = lines(own[0, :HALO], own[1, :edge], zown)
    high_rows = lines(own[0, by - HALO :], own[1, by - edge :], zown)
    from_low, from_high = exchange(low_rows, high_rows, "gy", "gx")
    cut = (HALO + edge) * tiles * x_count
    rows_shape = (HALO + edge, tiles, x_count, LANES)
    ylo, zlo = from_low[:cut].reshape(rows_shape), from_low[cut:].reshape(zown.shape)
    yhi, zhi = from_high[:cut].reshape(rows_shape), from_high[cut:].reshape(zown.shape)

    ext = by + 2 * HALO
    padded = x_count + 2 * PAD
    wide = (ext, tiles + 1, padded, LANES)
    plain = (ext, tiles + 1, x_count, LANES)
    each = by // 2
    xc = x_count // 2
    kap, diag, inv, xpre, rpre, coarse, to_left, to_right = call(
        before_kernel,
        [
            shape(*wide),
            shape(*plain),
            shape(*plain),
            shape(by, tiles, x_count, LANES),
            shape(by, tiles, x_count, LANES),
            shape(2 * each * xc, LANES),
            shape(2 * xc + x_count, LANES),
            shape(2 * xc + x_count, LANES),
        ],
        [vmem(wide)] * 4 + [vmem(plain)] * 2 + [vmem((2 * each * x_count, LANES))],
        [own, zown, ylo, zlo, yhi, zhi],
    )

    left, right = exchange(to_left, to_right, "gz")
    coarse_z = jnp.stack([left[: 2 * xc], right[: 2 * xc]])
    lane = lax.broadcasted_iota(jnp.int32, (x_count, LANES), 1)
    fine_z = jnp.where(lane < LANES // 2, right[2 * xc :], left[2 * xc :])
    blocks, low, high = gather_second(
        lines(coarse, coarse_z), lines(rpre[:edge], fine_z), lines(rpre[by - edge :], fine_z), iy, ny
    )
    cut = 2 * each * xc
    zblocks = [b[cut:].reshape(2, 2, xc, LANES) for b in blocks]
    blocks = [b[:cut].reshape(2, each, xc, LANES) for b in blocks]
    cut = edge * tiles * x_count
    rows_shape = (edge, tiles, x_count, LANES)
    rlo, zrlo = low[:cut].reshape(rows_shape), low[cut:].reshape(fine_z.shape)
    rhi, zrhi = high[:cut].reshape(rows_shape), high[cut:].reshape(fine_z.shape)

    yc = each * ny
    tiles1 = tiles // 2 + 1
    wide1 = (yc + 2 * COARSE_PAD, tiles1, xc + 2 * PAD, LANES)
    plain1 = (yc + 2 * COARSE_PAD, tiles1, xc, LANES)
    y2 = yc // 2
    x2 = max(xc // 2, 8)
    wide2 = (y2 + 2, 1, x2 + 2 * PAD, LANES)
    plain2 = (y2 + 2, 1, x2, LANES)
    flat_rows = max(y2 * xc, tiles1 * (ext // 2 + 1) * x_count)


    def kernel(*refs):
        after_kernel(*refs, count=len(blocks))

    sol, resid = call(
        kernel,
        [shape(bx, by, bz), shape(bx, by, bz)],
        [vmem(wide1)] + [vmem(plain1)] * 4 + [vmem(wide1)] * 4
        + [vmem(wide2)] + [vmem(plain2)] * 4 + [vmem(wide2)] * 4
        + [vmem((flat_rows, LANES))] + [vmem(wide)] * 4 + [vmem(plain)] * 2,
        blocks + zblocks
        + [kap, diag, inv, xpre, rpre, fine_z, rlo, zrlo, rhi, zrhi],
    )
    return sol, resid


def solution(mesh):
    spec = P("gx", "gy", "gz")

    return jax.shard_map(body, mesh=mesh, in_specs=(spec, spec), out_specs=(spec, spec), check_vma=False)
```

```python
import jax
import jax.numpy as jnp
from jax import lax
from jax.experimental import pallas as pl
from jax.experimental.pallas import tpu as pltpu
from jax.sharding import PartitionSpec as P


DEGREE = 4
COARSE_DEGREE = 8
smooth_low = 0.5
coarse_low = 0.03
upper_bound = 2.0

F32 = jnp.float32
LANES = 128
PAD = 8
HALO = 5
COARSE_PAD = 4
FACE = 14.0 / 3.0
CORNER = 1.0 / 3.0
TOTAL = 128.0 / 3.0
SCALE = 0.05


def chebyshev_coefs(degree, lower):
    centre = (upper_bound + lower) / 2.0
    half_width = (upper_bound - lower) / 2.0
    ratio_term = centre / half_width
    rho_prev = 1.0 / ratio_term
    weights = []
    for _ in range(1, degree):
        rho_next = 1.0 / (2.0 * ratio_term - rho_prev)
        weights.append((rho_next * rho_prev, 2.0 * rho_next / half_width))
        rho_prev = rho_next
    return centre, weights


EDGE = 8
COARSE_EDGE = 32
CHUNK = 16


def chunks(start, stop, body):
    count = stop - start
    full = count // CHUNK
    if full == 1:
        body(start, CHUNK)
    elif full > 1:

        def step(i, carry):
            body(start + i * CHUNK, CHUNK)
            return carry

        lax.fori_loop(0, full, step, 0)
    if count % CHUNK:
        body(start + full * CHUNK, count % CHUNK)


def loop(start, stop, body):
    def group(first, rows):
        for i in range(rows):
            body(first + i)

    chunks(start, stop, group)


def third_pairs(values):
    tiles, rows, _ = values.shape
    flat = values.reshape(tiles * rows, LANES)
    up = pltpu.roll(flat, 1, 1).reshape(tiles, rows, LANES)
    down = pltpu.roll(flat, LANES - 1, 1).reshape(tiles, rows, LANES)
    if tiles > 1:
        lane = lax.broadcasted_iota(jnp.int32, (tiles, rows, LANES), 2)
        up_other = jnp.concatenate([up[tiles - 1 :], up[: tiles - 1]], axis=0)
        down_other = jnp.concatenate([down[1:], down[:1]], axis=0)
        up = jnp.where(lane == 0, up_other, up)
        down = jnp.where(lane == LANES - 1, down_other, down)
    return up + down


def neighbour_sums(ref, first, rows, row):
    at = range(first - 1, first + rows + 1) if isinstance(first, int) else [first + i for i in range(-1, rows + 1)]
    centre = [ref[y, :, row : row + 8, :] for y in at]
    side = [ref[y, :, row - 1 : row + 7, :] + ref[y, :, row + 1 : row + 9, :] for y in at]
    out = []
    for i in range(1, rows + 1):
        corner = side[i - 1] + side[i + 1]
        face = (centre[i - 1] + centre[i + 1]) + side[i]
        plane = FACE * face + corner
        beside = FACE * centre[i] + face + CORNER * corner
        out.append((plane + third_pairs(beside), centre[i]))
    return out


def zero_pads(refs):
    for ref in refs:
        count, tiles, rows, _ = ref.shape
        zero = jnp.zeros((tiles, PAD, LANES), F32)

        def body(y, ref=ref, rows=rows, zero=zero):
            ref[y, :, 0:PAD, :] = zero
            ref[y, :, rows - PAD : rows, :] = zero

        loop(0, count, body)


def zero_rows(ref, rows):
    zero = jnp.zeros(ref.shape[1:], F32)
    for y in rows:
        ref[y] = zero


def tiles_of(ref):
    return range(0, ref.shape[2], 8)


def make_diagonal(kap, diag, inv, lo, hi):
    def body(first, rows):
        for x in tiles_of(diag):
            for i, (total, centre) in enumerate(neighbour_sums(kap, first, rows, PAD + x)):
                value = TOTAL * centre + total
                diag[first + i, :, x : x + 8, :] = value
                inv[first + i, :, x : x + 8, :] = jnp.where(centre > 0.0, 1.0 / value, 0.0)

    chunks(lo, hi, body)


def accumulate(acc, y, x, step, add, own):
    tiles = step.shape[0]
    if own is not None:
        if isinstance(y, int) and not own[0] <= y < own[1]:
            return
        tiles = own[2]
    step = step[0:tiles]
    acc[y, 0:tiles, x : x + 8, :] = acc[y, 0:tiles, x : x + 8, :] + step if add else step


def first_update(kap, inv, res, v, w, acc, lo, hi, scale, add, own=None):
    def body(y):
        for x in tiles_of(inv):
            step = (inv[y, :, x : x + 8, :] * scale) * res[y, :, x : x + 8, :]
            v[y, :, PAD + x : PAD + x + 8, :] = step
            w[y, :, PAD + x : PAD + x + 8, :] = kap[y, :, PAD + x : PAD + x + 8, :] * step
            accumulate(acc, y, x, step, add, own)

    loop(lo, hi, body)


def times(kap, v, w, lo, hi):
    def body(y):
        w[y] = kap[y] * v[y]

    loop(lo, hi, body)


def new_residuals(kap, diag, res, v, w, first, rows, x):
    total = neighbour_sums(v, first, rows, PAD + x)
    weighted = neighbour_sums(w, first, rows, PAD + x)
    for i in range(rows):
        y = first + i
        k = kap[y, :, PAD + x : PAD + x + 8, :]
        centre = total[i][1]
        value = (
            res[y, :, x : x + 8, :]
            - diag[y, :, x : x + 8, :] * centre
            + (k * total[i][0] + weighted[i][0])
        )
        yield y, k, centre, value


def residual_only(kap, diag, res, v, w, lo, hi):
    def body(first, rows):
        for x in tiles_of(diag):
            for y, _, _, value in new_residuals(kap, diag, res, v, w, first, rows, x):
                res[y, :, x : x + 8, :] = value

    chunks(lo, hi, body)


def smoothing_step(kap, diag, inv, res, old, new, acc, lo, hi, pair, own=None):
    def body(first, rows):
        for x in tiles_of(diag):
            for y, k, centre, value in new_residuals(kap, diag, res, old[0], old[1], first, rows, x):
                res[y, :, x : x + 8, :] = value
                step = pair[0] * centre + (pair[1] * inv[y, :, x : x + 8, :]) * value
                new[0][y, :, PAD + x : PAD + x + 8, :] = step
                new[1][y, :, PAD + x : PAD + x + 8, :] = k * step
                accumulate(acc, y, x, step, True, own)

    chunks(lo, hi, body)


def lanes_of(values):
    return lax.broadcasted_iota(jnp.int32, values.shape, 1)


def take(values, index):
    return jnp.take_along_axis(values, index, axis=1, mode="promise_in_bounds")


def halve(first, second):
    lane = lanes_of(first)
    even = (2 * lane) % LANES
    low = take(first + pltpu.roll(first, LANES - 1, 1), even)
    high = take(second + pltpu.roll(second, LANES - 1, 1), even)
    return jnp.where(lane < LANES // 2, low, high) * 0.125


def double(values):
    half = lanes_of(values) // 2
    return take(values, half), take(values, half + LANES // 2)


def double_halo(values):
    lane = lanes_of(values)
    return take(values, lane // 2 + jnp.where(lane < LANES // 2, 0, LANES // 2))


def pack(pieces, width, from_end, start=0):
    lane = lax.broadcasted_iota(jnp.int32, pieces[0].shape, 1)
    out = jnp.zeros(pieces[0].shape, F32)
    for i, piece in enumerate(pieces, start):
        shift = (width * i + (width if from_end else 0)) % LANES
        moved = pltpu.roll(piece, shift, 1) if shift else piece
        out = jnp.where((lane >= width * i) & (lane < width * (i + 1)), moved, out)
    return out


def unpack(left, right, i, width, start=0):
    lane = lax.broadcasted_iota(jnp.int32, left.shape, 1)
    back = (LANES - width * i) % LANES
    end = (LANES - width - width * (i + start)) % LANES
    first = pltpu.roll(right, back, 1) if back else right
    last = pltpu.roll(left, end, 1) if end else left
    return jnp.where(lane < width, first, jnp.where(lane >= LANES - width, last, 0.0))


def before_kernel(own, zown, ylo, zlo, yhi, zhi, kap, diag, inv, xout, rout, coarse, to_left, to_right, va, wa, vb, wb, res, acc, flat):
    rows = own.shape[1]
    tiles = own.shape[2]
    x_count = own.shape[3]
    inner = slice(PAD, PAD + x_count)
    last = HALO + rows
    iy, iz = lax.axis_index("gy"), lax.axis_index("gz")
    ny, nz = lax.axis_size("gy"), lax.axis_size("gz")
    has_left, has_right = iz > 0, iz < nz - 1
    zero_pads((kap, va, wa, vb, wb))

    def fill(j, k, b, z, y, there):
        left = jnp.where(has_left & there, z[0], 0.0)
        right = jnp.where(has_right & there, z[1], 0.0)
        kap[j, 0:tiles, inner, :] = jnp.where(there, SCALE * k, 0.0)
        kap[j, tiles, inner, :] = SCALE * unpack(left, right, y, EDGE)
        if b is not None:
            res[j, 0:tiles] = b
            res[j, tiles] = unpack(z[0], z[1], rows + y, EDGE)

    for y in range(rows):
        fill(HALO + y, own[0, y], own[1, y], zown, y, iy >= 0)
    for j in range(HALO):
        b = ylo[HALO + j - 1] if j else None
        fill(j, ylo[j], b, zlo, rows - HALO + j, iy > 0)
        b = yhi[HALO + j] if j < HALO - 1 else None
        fill(last + j, yhi[j], b, zhi, j, iy < ny - 1)
    make_diagonal(kap, diag, inv, 1, last + HALO - 1)
    centre, weights = chebyshev_coefs(DEGREE, smooth_low)
    first_update(kap, inv, res, va, wa, acc, 1, last + HALO - 1, 1.0 / centre, False, (HALO, last, tiles))
    old, new = (va, wa), (vb, wb)
    lo, hi = 2, last + HALO - 2
    for pair in weights:
        smoothing_step(kap, diag, inv, res, old, new, acc, lo, hi, pair, (HALO, last, tiles))
        old, new = new, old
        lo, hi = lo + 1, hi - 1
    residual_only(kap, diag, res, old[0], old[1], HALO, last)
    at = 0
    for y in range(rows):
        xout[y] = acc[HALO + y, 0:tiles]
        rout[y] = res[HALO + y, 0:tiles]
    for source, offset in ((kap, PAD), (res, 0)):
        for y in range(0, rows, 2):
            both = (
                source[HALO + y, 0:tiles, offset : offset + x_count, :]
                + source[HALO + y + 1, 0:tiles, offset : offset + x_count, :]
            )
            flat[at : at + x_count, :] = halve(both[0], both[1])
            at += x_count
    total = flat.shape[0]
    coarse[...] = flat[pl.ds(0, total // 2, stride=2), :] + flat[pl.ds(1, total // 2, stride=2), :]
    each, xc = rows // 2, x_count // 2
    for out, from_end in ((to_left, False), (to_right, True)):
        for i in range(2):
            value = [coarse[(i * each + y) * xc : (i * each + y + 1) * xc, :] for y in range(each)]
            out[i * xc : (i + 1) * xc, :] = pack(value, COARSE_EDGE, from_end)
        value = [res[HALO + y, tiles - 1 if from_end else 0] for y in range(rows)]
        out[2 * xc : 2 * xc + x_count, :] = pack(value, EDGE, from_end, rows if from_end else 0)


def sources_of(me, count):
    if count == 4:
        return [me] + [jnp.bitwise_xor(me, step) for step in (1, 2, 3)]
    return [me] + [lax.rem(me - step + count, count) for step in range(1, count)]


def coarse_kernel(*refs, count):
    blocks, zblocks = refs[:count], refs[count : 2 * count]
    refs = refs[2 * count :]
    window = refs[0]
    (k1, d1, i1, r1, x1, va1, wa1, vb1, wb1, k2, d2, i2, r2, x2, va2, wa2, vb2, wb2, flat) = refs[1:]
    me_y, me_z = lax.axis_index("gy"), lax.axis_index("gz")
    has_left, has_right = me_z > 0, me_z < lax.axis_size("gz") - 1
    sources = sources_of(me_y, count)
    zero_pads((k1, va1, wa1, vb1, wb1, k2, va2, wa2, vb2, wb2))
    each = blocks[0].shape[1]
    xc = blocks[0].shape[2]
    yc = each * count
    lo1, hi1 = COARSE_PAD, COARSE_PAD + yc
    edge = [lo1 - 1, hi1]
    for ref in (k1, va1, wa1, vb1, wb1):
        zero_rows(ref, edge)
    zero_rows(x1, list(range(lo1)) + list(range(hi1, hi1 + COARSE_PAD)))
    for number, (block, z) in enumerate(zip(blocks, zblocks)):
        at = sources[number] * each + COARSE_PAD
        left = jnp.where(has_left, z[0, 0], 0.0)
        right = jnp.where(has_right, z[1, 0], 0.0)
        for y in range(each):
            k1[at + y, 0, PAD : PAD + xc, :] = block[0, y] * 0.25
            k1[at + y, 1, PAD : PAD + xc, :] = unpack(left, right, y, COARSE_EDGE) * 0.25
            r1[at + y, 0] = block[1, y]
            r1[at + y, 1] = unpack(z[0, 1], z[1, 1], y, COARSE_EDGE)
    make_diagonal(k1, d1, i1, lo1, hi1)
    centre, weights = chebyshev_coefs(DEGREE, smooth_low)
    first_update(k1, i1, r1, va1, wa1, x1, lo1, hi1, 1.0 / centre, False)
    old, new = (va1, wa1), (vb1, wb1)
    for pair in weights:
        smoothing_step(k1, d1, i1, r1, old, new, x1, lo1, hi1, pair)
        old, new = new, old
    residual_only(k1, d1, r1, old[0], old[1], lo1, hi1)
    y2 = yc // 2
    half = xc // 2
    for target, source, offset, factor in ((k2, k1, PAD, 0.25), (r2, r1, 0, 1.0)):
        for y in range(y2):
            a = lo1 + 2 * y
            both = source[a, :, offset : offset + xc, :] + source[a + 1, :, offset : offset + xc, :]
            flat[y * xc : (y + 1) * xc, :] = halve(both[0], both[1])
        if target is k2:
            zero_rows(k2, range(y2 + 2))
        for y in range(y2):
            value = flat[pl.ds(y * xc, half, stride=2), :] + flat[pl.ds(y * xc + 1, half, stride=2), :]
            if target is k2:
                k2[1 + y, 0, PAD : PAD + half, :] = value * factor
            else:
                r2[1 + y] = jnp.zeros(r2.shape[1:], F32)
                r2[1 + y, 0, 0:half, :] = value
    for ref in (va2, wa2, vb2, wb2):
        zero_rows(ref, [0, y2 + 1])
    make_diagonal(k2, d2, i2, 1, 1 + y2)
    centre, weights = chebyshev_coefs(COARSE_DEGREE, coarse_low)
    first_update(k2, i2, r2, va2, wa2, x2, 1, 1 + y2, 1.0 / centre, False)
    old, new = (va2, wa2), (vb2, wb2)
    for pair in weights:
        smoothing_step(k2, d2, i2, r2, old, new, x2, 1, 1 + y2, pair)
        old, new = new, old
    for y in range(y2):
        value = x2[1 + y, 0, 0:half, :]
        flat[pl.ds(y * xc, half, stride=2), :] = value
        flat[pl.ds(y * xc + 1, half, stride=2), :] = value
    for y in range(y2):
        for t, value in enumerate(double(flat[y * xc : (y + 1) * xc, :])):
            for s in (0, 1):
                at = lo1 + 2 * y + s
                va1[at, t, PAD : PAD + xc, :] = value
                x1[at, t] = x1[at, t] + value
    times(k1, va1, wa1, lo1, hi1)
    centre, weights = chebyshev_coefs(DEGREE, smooth_low)
    residual_only(k1, d1, r1, va1, wa1, lo1, hi1)
    first_update(k1, i1, r1, va1, wa1, x1, lo1, hi1, 1.0 / centre, True)
    old, new = (va1, wa1), (vb1, wb1)
    for pair in weights:
        smoothing_step(k1, d1, i1, r1, old, new, x1, lo1, hi1, pair)
        old, new = new, old
    wide_rows = window.shape[0]
    start = COARSE_PAD - (HALO + 1) // 2 + each * me_y
    for y in range(wide_rows):
        window[y] = x1[start + y]


def after_kernel(window, kap, diag, inv, xpre, rown, zown, rlo, zlo, rhi, zhi, sol, resid, flat, va, wa, vb, wb, res, acc):
    me_x = lax.axis_index("gx")
    zero_pads((va, wa, vb, wb))
    rows, tiles, x_count, _ = rown.shape
    last = HALO + rows
    wide_rows, tiles1, xc, _ = window.shape
    centre, weights = chebyshev_coefs(DEGREE, smooth_low)
    for t in range(tiles1):
        for y in range(wide_rows):
            value = window[y, t]
            base = (t * wide_rows + y) * x_count
            flat[pl.ds(base, xc, stride=2), :] = value
            flat[pl.ds(base + 1, xc, stride=2), :] = value
    inner = slice(PAD, PAD + x_count)
    for y in range(wide_rows):
        parts = []
        for t in range(tiles1):
            at = (t * wide_rows + y) * x_count
            value = flat[at : at + x_count, :]
            parts += double(value) if t < tiles1 - 1 else [double_halo(value)]
        for j in (2 * y - 1, 2 * y):
            if not 0 <= j < rows + 2 * HALO:
                continue
            for t, value in enumerate(parts):
                va[j, t, inner, :] = value
                wa[j, t, inner, :] = kap[j, t, inner, :] * value
                if HALO <= j < last and t < tiles:
                    acc[j, t] = xpre[j - HALO, t] + value

    edge = HALO - 1
    for j in range(-edge, rows + edge):
        if j < 0:
            source, z, i, y = rlo, zlo, edge + j, rows + j
        elif j < rows:
            source, z, i, y = rown, zown, j, j
        else:
            source, z, i, y = rhi, zhi, j - rows, j - rows
        res[HALO + j, 0:tiles] = source[i]
        packed = z[...]
        res[HALO + j, tiles] = unpack(packed, packed, y, EDGE, rows)
    residual_only(kap, diag, res, va, wa, 1, last + HALO - 1)
    first_update(kap, inv, res, va, wa, acc, 1, last + HALO - 1, 1.0 / centre, True, (HALO, last, tiles))
    old, new = (va, wa), (vb, wb)
    lo, hi = 2, last + HALO - 2
    for pair in weights:
        smoothing_step(kap, diag, inv, res, old, new, acc, lo, hi, pair, (HALO, last, tiles))
        old, new = new, old
        lo, hi = lo + 1, hi - 1
    block_x = sol.shape[0]
    for x in range(0, x_count, 8):

        @pl.when(me_x == x // block_x)
        def _(x=x):
            values = new_residuals(kap, diag, res, old[0], old[1], HALO, rows, x)
            for y, (_, _, _, value) in enumerate(values):
                for t in range(tiles):
                    lanes = slice(t * LANES, (t + 1) * LANES)
                    at = slice(x % block_x, x % block_x + 8)
                    sol[at, y, lanes] = acc[HALO + y, t, x : x + 8, :]
                    resid[at, y, lanes] = value[t]


def ring(values, axis, step):
    count = lax.axis_size(axis)
    return lax.ppermute(values, axis, [(i, (i + step) % count) for i in range(count)])


def exchange(to_low, to_high, axis, across=None):
    count = lax.axis_size(axis)
    if count % 2:
        return ring(to_high, axis, 1), ring(to_low, axis, -1)
    odd = lax.axis_index(axis) % 2 == 1
    inner = [i + 1 if i % 2 else i - 1 for i in range(count)]
    one = lax.ppermute(jnp.where(odd, to_low, to_high), axis, [(i, i ^ 1) for i in range(count)])
    names, pairs = axis, [(i, t % count) for i, t in enumerate(inner)]
    if across is not None and lax.axis_size(across) % 2 == 0:
        names = (across, axis)
        pairs = [
            (x * count + i, x * count + t if 0 <= t < count else (x ^ 1) * count + i)
            for x in range(lax.axis_size(across))
            for i, t in enumerate(inner)
        ]
    two = lax.ppermute(jnp.where(odd, to_high, to_low), names, pairs)
    return jnp.where(odd, one, two), jnp.where(odd, two, one)


def exchange_and_gather(to_low, to_high):
    nx, nz = lax.axis_size("gx"), lax.axis_size("gz")
    if nx != 2 or nz % 2:
        return gather_first(jnp.stack(exchange(to_low, to_high, "gz")), "gx", 1)
    odd = lax.axis_index("gz") % 2 == 1
    out = []
    for payload, step in (
        (jnp.where(odd, to_low, to_high), [i ^ 1 for i in range(nz)]),
        (jnp.where(odd, to_high, to_low), [(i + 1 if i % 2 else i - 1) % nz for i in range(nz)]),
    ):
        same = lax.ppermute(payload, "gz", list(enumerate(step)))
        pairs = [(x * nz + i, (1 - x) * nz + t) for x in (0, 1) for i, t in enumerate(step)]
        cross = lax.ppermute(payload, ("gx", "gz"), pairs)
        first = lax.axis_index("gx") == 0
        out.append(jnp.concatenate([jnp.where(first, same, cross), jnp.where(first, cross, same)], axis=0))
    one, two = out
    return jnp.stack([jnp.where(odd, one, two), jnp.where(odd, two, one)])


def gather_first(values, axis, dim):
    count = lax.axis_size(axis)
    if count == 1:
        return values
    if count == 2:
        other = lax.ppermute(values, axis, [(0, 1), (1, 0)])
        first = lax.axis_index(axis) == 0
        return jnp.concatenate(
            [jnp.where(first, values, other), jnp.where(first, other, values)], axis=dim
        )
    every = lax.all_gather(values, axis)
    return jnp.concatenate([every[i] for i in range(count)], axis=dim)


def gather_second(block, low_edge, high_edge, me, count):
    size = block.shape[0]
    blocks = [block]
    low = high = low_edge
    if count == 4:
        odd = me % 2 == 1
        near = jnp.where(odd, low_edge, high_edge)
        far = jnp.where(odd, high_edge, low_edge)
        nx = lax.axis_size("gx")
        pairs = [(x * 4 + i, x * 4 + 3 - i if i in (1, 2) else (x ^ 1) * 4 + i) for x in range(nx) for i in range(4)]
        if nx % 2:
            pairs = [(x * 4 + i, x * 4 + 3 - i) for x in range(nx) for i in range(4)]
        got = []
        for step in (1, 2, 3):
            got.append(lax.ppermute(block, "gy", [(i, i ^ step) for i in range(count)]))
            blocks.append(got[-1][:size])
        far = lax.ppermute(far, ("gx", "gy"), pairs)
        near = lax.ppermute(near, "gy", [(i, i ^ 1) for i in range(count)])
        low, high = jnp.where(odd, near, far), jnp.where(odd, far, near)
    else:
        for step in range(1, count):
            parts = [block]
            if step == 1:
                parts.append(high_edge)
            if step == count - 1:
                parts.append(low_edge)
            got = ring(jnp.concatenate(parts, axis=0), "gy", step)
            blocks.append(got[:size])
            if step == 1:
                low = got[size : size + high_edge.shape[0]]
            if step == count - 1:
                high = got[got.shape[0] - low_edge.shape[0] :]
    return blocks, low, high


def vmem(shape):
    return pltpu.VMEM(shape, F32)


def call(kernel, out_shapes, scratch, inputs):
    limit = 4 * 2**20
    for s in scratch:
        size = 4
        for n in s.shape:
            size *= n
        limit += size
    for a in list(inputs) + list(out_shapes):
        limit += 4 * a.size if hasattr(a, "size") else 0
    limit = min(limit + 8 * 2**20, 60 * 2**20)
    whole = pl.BlockSpec(memory_space=pltpu.VMEM)
    return pl.pallas_call(
        kernel,
        out_shape=out_shapes,
        in_specs=[whole] * len(inputs),
        out_specs=[whole] * len(out_shapes),
        scratch_shapes=scratch,
        compiler_params=pltpu.CompilerParams(vmem_limit_bytes=limit),
    )(*inputs)


def body(conductivity, source):
    bx, by, bz = conductivity.shape
    tiles = bz // LANES
    nx, ny, _ = (lax.axis_size(a) for a in ("gx", "gy", "gz"))
    iy = lax.axis_index("gy")
    x_count = bx * nx

    def shape(*dims):
        return jax.ShapeDtypeStruct(dims, F32)

    def lines(*arrays):
        return jnp.concatenate([a.reshape(-1, LANES) for a in arrays], axis=0)

    mine = jnp.stack([conductivity, source]).reshape(2, bx, by, tiles, LANES).transpose(0, 2, 3, 1, 4)
    first_edge = jnp.concatenate([mine[a, y, 0, :, :EDGE] for a in (0, 1) for y in range(by)], axis=-1)
    last_edge = jnp.concatenate(
        [mine[a, y, tiles - 1, :, LANES - EDGE :] for a in (0, 1) for y in range(by)], axis=-1
    )
    own = gather_first(mine, "gx", 3)
    zown = exchange_and_gather(first_edge, last_edge)
    edge = HALO - 1
    low_rows = lines(own[0, :HALO], own[1, :edge], zown)
    high_rows = lines(own[0, by - HALO :], own[1, by - edge :], zown)
    from_low, from_high = exchange(low_rows, high_rows, "gy", "gx")
    cut = (HALO + edge) * tiles * x_count
    rows_shape = (HALO + edge, tiles, x_count, LANES)
    ylo, zlo = from_low[:cut].reshape(rows_shape), from_low[cut:].reshape(zown.shape)
    yhi, zhi = from_high[:cut].reshape(rows_shape), from_high[cut:].reshape(zown.shape)

    ext = by + 2 * HALO
    padded = x_count + 2 * PAD
    wide = (ext, tiles + 1, padded, LANES)
    plain = (ext, tiles + 1, x_count, LANES)
    each = by // 2
    xc = x_count // 2
    kap, diag, inv, xpre, rpre, coarse, to_left, to_right = call(
        before_kernel,
        [
            shape(*wide),
            shape(*plain),
            shape(*plain),
            shape(by, tiles, x_count, LANES),
            shape(by, tiles, x_count, LANES),
            shape(2 * each * xc, LANES),
            shape(2 * xc + x_count, LANES),
            shape(2 * xc + x_count, LANES),
        ],
        [vmem(wide)] * 4 + [vmem(plain)] * 2 + [vmem((2 * each * x_count, LANES))],
        [own, zown, ylo, zlo, yhi, zhi],
    )

    left, right = exchange(to_left, to_right, "gz")
    coarse_z = jnp.stack([left[: 2 * xc], right[: 2 * xc]])
    lane = lax.broadcasted_iota(jnp.int32, (x_count, LANES), 1)
    fine_z = jnp.where(lane < LANES // 2, right[2 * xc :], left[2 * xc :])
    blocks, low, high = gather_second(
        lines(coarse, coarse_z), lines(rpre[:edge], fine_z), lines(rpre[by - edge :], fine_z), iy, ny
    )
    cut = 2 * each * xc
    zblocks = [b[cut:].reshape(2, 2, xc, LANES) for b in blocks]
    blocks = [b[:cut].reshape(2, each, xc, LANES) for b in blocks]
    cut = edge * tiles * x_count
    rows_shape = (edge, tiles, x_count, LANES)
    rlo, zrlo = low[:cut].reshape(rows_shape), low[cut:].reshape(fine_z.shape)
    rhi, zrhi = high[:cut].reshape(rows_shape), high[cut:].reshape(fine_z.shape)

    yc = each * ny
    tiles1 = tiles // 2 + 1
    wide1 = (yc + 2 * COARSE_PAD, tiles1, xc + 2 * PAD, LANES)
    plain1 = (yc + 2 * COARSE_PAD, tiles1, xc, LANES)
    y2 = yc // 2
    x2 = max(xc // 2, 8)
    wide2 = (y2 + 2, 1, x2 + 2 * PAD, LANES)
    plain2 = (y2 + 2, 1, x2, LANES)
    wide_rows = ext // 2 + 1

    def kernel(*refs):
        coarse_kernel(*refs, count=len(blocks))

    (window,) = call(
        kernel,
        [shape(wide_rows, tiles1, xc, LANES)],
        [vmem(wide1)] + [vmem(plain1)] * 4 + [vmem(wide1)] * 4
        + [vmem(wide2)] + [vmem(plain2)] * 4 + [vmem(wide2)] * 4
        + [vmem((y2 * xc, LANES))],
        blocks + zblocks,
    )
    sol, resid = call(
        after_kernel,
        [shape(bx, by, bz), shape(bx, by, bz)],
        [vmem((tiles1 * wide_rows * x_count, LANES))] + [vmem(wide)] * 4 + [vmem(plain)] * 2,
        [window, kap, diag, inv, xpre, rpre, fine_z, rlo, zrlo, rhi, zrhi],
    )
    return sol, resid


def solution(mesh):
    spec = P("gx", "gy", "gz")

    return jax.shard_map(body, mesh=mesh, in_specs=(spec, spec), out_specs=(spec, spec), check_vma=False)
```
